32 devices in a mesh: gx: 4 (over y, x), gy: 2 (over core), gz: 4 (over z).
Axes of the slice: x: 2, y: 2, z: 4, core: 2. Of those that a mesh axis runs over, the one named last changes fastest.
Arguments:
- positions: float32 [3, 4, 2, 4, 128], P(None, 'gx', 'gy', 'gz'), may hold values from 0 to 1
- basis: float32 [30, 3, 4, 2, 4, 128], P(None, None, 'gx', 'gy', 'gz'), may hold values from -10 to 10, as said below
- neighbours: int32 [4, 2, 4, 128, 128], P('gx', 'gy', 'gz'), may hold values from 0 to 511
- used_count: int32 [4, 2, 4, 128], P('gx', 'gy', 'gz'), may hold values from 42 to 128
- kinds: int32 [4, 2, 4, 128], P('gx', 'gy', 'gz'), may hold values from 0 to 1
- map_x: int32 [4, 2, 4, 2, 64], P('gx', 'gy', 'gz'), may hold values from 0 to 127
- map_y: int32 [4, 2, 4, 2, 64], P('gx', 'gy', 'gz'), may hold values from 0 to 255
- map_z: int32 [4, 2, 4, 2, 64], P('gx', 'gy', 'gz'), may hold values from 0 to 383
- table: float32 [2, 16, 100], replicated, may hold values from -6 to 6
- fit_w1: float32 [1600, 240], replicated, may hold values from -0.15625 to 0.15625
- fit_b1: float32 [240], replicated, may hold values from -3 to 3
- fit_w2: float32 [240, 240], replicated, may hold values from -0.375 to 0.375
- fit_b2: float32 [240], replicated, may hold values from -3 to 3
- fit_out: float32 [240], replicated, may hold values from -0.375 to 0.375
Outputs:
- next_vector: float32 [3, 4, 2, 4, 128], P(None, 'gx', 'gy', 'gz')
- correlations: float32 [30], replicated
- vector_norm: float32 [], replicated
The draws below stay inside these ranges and needn't reach their ends.
Inputs may be any that keep to these rules, and one draw needn't show every extreme that they name: `basis`: entries of order one; the stored vectors' magnitude varies from brick to brick.
All inputs are finite; a program needn't handle non-finite values.
Results may differ from the reference program's by a relative error of at most 0.0003.
Values sent between devices are 32-bit elements; how exact they have to be, the bound alone decides.
A program may use at most 64 MiB of HBM per device.

```python
import jax
import jax.numpy as jnp
from jax import lax

ATOMS_DEV = 128
NNEI = 128
NBASIS = 16
M1 = 100
M2 = 16
FIT = 240
NTYPES = 2
KVEC = 30
GRID_X = 4
GRID_Y = 2
GRID_Z = 4
GHOST = 64
EXT = 512


def draw_basis(key, part):
    first_key, second_key, third_key = jax.random.split(jax.random.fold_in(key, 17), 3)
    shape = (KVEC, 3, GRID_X, GRID_Y, GRID_Z, ATOMS_DEV)
    bricks = GRID_X * GRID_Y * GRID_Z
    order = jnp.arange(bricks, dtype=jnp.float32).reshape(1, 1, GRID_X, GRID_Y, GRID_Z, 1)
    fraction = order / max(bricks - 1, 1)
    private = jax.random.truncated_normal(first_key, -3.0, 3.0, shape, jnp.float32)
    shared = jax.random.truncated_normal(second_key, -3.0, 3.0, shape[1:], jnp.float32)
    magnitude = 0.5 * jnp.exp(fraction * jnp.log(4.0))
    mixing = jax.random.uniform(third_key, (KVEC,), jnp.float32, 0.3, 0.9).reshape(KVEC, 1, 1, 1, 1, 1)
    values = (private * jnp.sqrt(1.0 - mixing * mixing) + mixing * shared[None]) * magnitude
    return values.astype(jnp.float32)


def touch_ends(values, key, least, top_value):
    dims = values.shape
    place = [jax.random.randint(jax.random.fold_in(key, axis), (), 0, dims[axis]) for axis in range(len(dims))]
    values = values.at[tuple(place)].set(least)
    longest = dims.index(max(dims))
    place[longest] = (place[longest] + 1) % dims[longest]
    return values.at[tuple(place)].set(top_value)


def block_levels(rng, extent, pieces, smallest, largest):
    gain = 1.0
    for axis_at, shards_of in pieces:
        heights = jax.random.uniform(jax.random.fold_in(jax.random.fold_in(rng, 6), axis_at), (shards_of,), jnp.float32, smallest / len(pieces), largest / len(pieces))
        gain = gain * jnp.repeat(jnp.exp(heights), extent[axis_at] // shards_of).reshape((-1,) + (1,) * (len(extent) - 1 - axis_at))
    return gain


def normal_values(rng, shape, width, reach, kind=jnp.bfloat16):
    return jnp.clip(width * jax.random.normal(rng, shape, jnp.float32), -reach, reach).astype(kind)


def setup_inputs(seed: int = 0) -> dict:
    streams_of = jax.random.split(jax.random.key(seed), 15)
    return {
        "positions": jnp.clip(1.0 * jax.random.uniform(streams_of[0], (3, GRID_X, GRID_Y, GRID_Z, ATOMS_DEV), jnp.float32) ** block_levels(streams_of[0], (3, GRID_X, GRID_Y, GRID_Z, ATOMS_DEV), ((1, 4), (2, 2), (3, 4)), -0.2, 0.2), 0.0, 1.0),
        "basis": draw_basis(jax.random.fold_in(streams_of[14], 71), 0),
        "neighbours": touch_ends(jax.random.randint(streams_of[2], (GRID_X, GRID_Y, GRID_Z, ATOMS_DEV, NNEI), 0, EXT), jax.random.fold_in(streams_of[2], 1), 0, EXT - 1).astype(jnp.int32),
        "used_count": touch_ends(jax.random.randint(streams_of[3], (GRID_X, GRID_Y, GRID_Z, ATOMS_DEV), NNEI // 3, NNEI + 1), jax.random.fold_in(streams_of[3], 1), NNEI // 3, NNEI).astype(jnp.int32),
        "kinds": touch_ends(jax.random.randint(streams_of[4], (GRID_X, GRID_Y, GRID_Z, ATOMS_DEV), 0, NTYPES), jax.random.fold_in(streams_of[4], 1), 0, NTYPES - 1).astype(jnp.int32),
        "map_x": touch_ends(jax.random.randint(streams_of[5], (GRID_X, GRID_Y, GRID_Z, 2, GHOST), 0, ATOMS_DEV), jax.random.fold_in(streams_of[5], 1), 0, ATOMS_DEV - 1).astype(jnp.int32),
        "map_y": touch_ends(jax.random.randint(streams_of[6], (GRID_X, GRID_Y, GRID_Z, 2, GHOST), 0, ATOMS_DEV + 2 * GHOST), jax.random.fold_in(streams_of[6], 1), 0, (ATOMS_DEV + 2 * GHOST) - 1).astype(jnp.int32),
        "map_z": touch_ends(jax.random.randint(streams_of[7], (GRID_X, GRID_Y, GRID_Z, 2, GHOST), 0, ATOMS_DEV + 4 * GHOST), jax.random.fold_in(streams_of[7], 1), 0, (ATOMS_DEV + 4 * GHOST) - 1).astype(jnp.int32),
        "table": normal_values(streams_of[8], (NTYPES, NBASIS, M1), 1.0, 6.0, jnp.float32),
        "fit_w1": normal_values(streams_of[9], (M1 * M2, FIT), (M1 * M2) ** -0.5, 0.15625, jnp.float32),
        "fit_b1": normal_values(streams_of[10], (FIT,), 0.5, 3.0, jnp.float32),
        "fit_w2": normal_values(streams_of[11], (FIT, FIT), FIT ** -0.5, 0.375, jnp.float32),
        "fit_b2": normal_values(streams_of[12], (FIT,), 0.5, 3.0, jnp.float32),
        "fit_out": normal_values(streams_of[13], (FIT,), FIT ** -0.5, 0.375, jnp.float32),
    }


def site_energy(centre, around, filled, onehot, table, fit_w1, fit_b1, fit_w2, fit_b2, fit_out):
    highest = lax.Precision.HIGHEST
    offsets = around - centre[:, :, None]
    square = lax.optimization_barrier(jnp.sum(offsets * offsets, axis=0))
    radius = jnp.sqrt(square + 0.01)
    smooth = jnp.exp(-square) / radius * filled
    radial = jnp.concatenate([smooth[None], smooth[None] * offsets / radius[None]], axis=0)
    scaled = smooth / (1.0 + smooth)
    levels = table.shape[1]
    centres = jnp.arange(levels, dtype=jnp.float32) / (levels - 1)
    spread = (scaled[:, None, :] - centres[None, :, None]) * (levels - 1)
    profile = jnp.exp(-spread * spread)
    pooled = jnp.einsum('bkn,abn->bka', profile, radial, precision=highest) / around.shape[2]
    tables = jnp.einsum('bt,tkm->bkm', onehot, table, precision=highest)
    environment = jnp.einsum('bkm,bka->bma', tables, pooled, precision=highest)
    descriptor = jnp.einsum('bma,bna->bmn', environment, environment[:, :M2], precision=highest)
    descriptor = descriptor.reshape(descriptor.shape[0], -1)
    first_layer = jnp.tanh(jnp.dot(descriptor, fit_w1, precision=highest) + fit_b1)
    second_layer = jnp.tanh(jnp.dot(first_layer, fit_w2, precision=highest) + fit_b2) + first_layer
    return jnp.sum(jnp.dot(second_layer, fit_out, precision=highest))

def device_hvp(ext_places, ext_tangent, neighbour_ids, counts, species, weights):
    atom_count = neighbour_ids.shape[0]
    block_rows = min(atom_count, 128)
    slots = jnp.arange(neighbour_ids.shape[1], dtype=jnp.int32)
    type_ids = jnp.arange(weights[0].shape[0], dtype=jnp.int32)

    def one_block(counter, summed):
        offset = (counter * block_rows).astype(jnp.int32)
        block_ids = lax.dynamic_slice_in_dim(neighbour_ids, offset, block_rows, 0)
        block_counts = lax.dynamic_slice_in_dim(counts, offset, block_rows, 0)
        block_species = lax.dynamic_slice_in_dim(species, offset, block_rows, 0)
        filled = (slots[None, :] < block_counts[:, None]).astype(jnp.float32)
        onehot = (block_species[:, None] == type_ids[None, :]).astype(jnp.float32)

        def energy(places):
            centre = lax.dynamic_slice_in_dim(places, offset, block_rows, 1)
            return site_energy(centre, places[:, block_ids], filled, onehot, *weights)
        return summed + jax.jvp(jax.grad(energy), (ext_places,), (ext_tangent,))[1]
    zeros = jnp.zeros(ext_places.shape, jnp.float32)
    return lax.fori_loop(0, atom_count // block_rows, one_block, zeros)

def take_rows(values, indices):
    wide = jnp.broadcast_to(indices[None], (values.shape[0],) + indices.shape)
    return jnp.take_along_axis(values, wide, axis=-1)

def extend(places, tangent, maps, axis, coord):
    displace = (jnp.arange(3) == coord).astype(jnp.float32).reshape(3, 1, 1, 1, 1)
    down_places = take_rows(places, maps[..., 0, :])
    up_places = take_rows(places, maps[..., 1, :])
    down_tangent = take_rows(tangent, maps[..., 0, :])
    up_tangent = take_rows(tangent, maps[..., 1, :])
    places = jnp.concatenate([places, jnp.roll(up_places, 1, axis) - displace, jnp.roll(down_places, -1, axis) + displace], axis=-1)
    tangent = jnp.concatenate([tangent, jnp.roll(up_tangent, 1, axis), jnp.roll(down_tangent, -1, axis)], axis=-1)
    return (places, tangent)

def add_one(target, indices, values):
    return target.at[:, indices].add(values)

def add_rows(target, indices, values):
    return jax.vmap(add_one, in_axes=(1, 0, 1), out_axes=1)(target, indices, values)

def reverse_section(contributions, maps, axis, current):
    ghosts = maps.shape[-1]
    bricks = GRID_X * GRID_Y * GRID_Z
    holder = contributions[..., :current]
    lower_part = contributions[..., current:current + ghosts]
    upper_part = contributions[..., current + ghosts:]
    from_below = jnp.roll(upper_part, 1, axis).reshape(3, bricks, ghosts)
    from_above = jnp.roll(lower_part, -1, axis).reshape(3, bricks, ghosts)
    flat = holder.reshape(3, bricks, current)
    flat = add_rows(flat, maps[..., 0, :].reshape(bricks, ghosts), from_below)
    flat = add_rows(flat, maps[..., 1, :].reshape(bricks, ghosts), from_above)
    return flat.reshape(holder.shape)

def reference(positions, basis, neighbours, used_count, kinds, map_x, map_y, map_z, table, fit_w1, fit_b1, fit_w2, fit_b2, fit_out):
    highest = lax.Precision.HIGHEST
    places = positions
    tangent = basis[KVEC - 1]
    places, tangent = extend(places, tangent, map_x, 1, 0)
    places, tangent = extend(places, tangent, map_y, 2, 1)
    places, tangent = extend(places, tangent, map_z, 3, 2)
    bricks = GRID_X * GRID_Y * GRID_Z
    extended = places.shape[-1]
    flat_places = jnp.transpose(places.reshape(3, bricks, extended), (1, 0, 2))
    flat_tangent = jnp.transpose(tangent.reshape(3, bricks, extended), (1, 0, 2))
    flat_ids = neighbours.reshape(bricks, ATOMS_DEV, NNEI)
    flat_counts = used_count.reshape(bricks, ATOMS_DEV)
    flat_species = kinds.reshape(bricks, ATOMS_DEV)
    weights = (table, fit_w1, fit_b1, fit_w2, fit_b2, fit_out)

    def per_brick(packed):
        return device_hvp(packed[0], packed[1], packed[2], packed[3], packed[4], weights)
    products = lax.map(per_brick, (flat_places, flat_tangent, flat_ids, flat_counts, flat_species))
    products = jnp.transpose(products, (1, 0, 2)).reshape(3, GRID_X, GRID_Y, GRID_Z, extended)
    products = reverse_section(products, map_z, 3, ATOMS_DEV + 4 * GHOST)
    products = reverse_section(products, map_y, 2, ATOMS_DEV + 2 * GHOST)
    products = reverse_section(products, map_x, 1, ATOMS_DEV)
    entries = 3 * ATOMS_DEV * bricks
    stored = basis.reshape(KVEC, -1)
    hessian_vec = products.reshape(-1)
    correlations = jnp.dot(stored, hessian_vec, precision=highest) / entries
    residual = hessian_vec - jnp.dot(correlations, stored, precision=highest)
    vector_norm = jnp.sqrt(jnp.sum(residual * residual) / entries + 1e-06)
    next_vector = (residual / vector_norm).reshape(positions.shape)
    return (next_vector, correlations, vector_norm)
```

```python
import functools

import jax
import jax.numpy as jnp
from jax import lax
from jax.experimental import pallas as pl
from jax.experimental.pallas import tpu as pltpu
from jax.sharding import PartitionSpec as P

F32, BF16 = jnp.float32, jnp.bfloat16
HIGHEST = lax.Precision.HIGHEST


def split(x):
    high = x.astype(BF16)
    return high, (x - high.astype(F32)).astype(BF16)


def dot_parts(left, right, dims):
    def one(a, b):
        return lax.dot_general(a, b, (dims, ((), ())), preferred_element_type=F32)

    return one(left[0], right[0]) + (one(left[0], right[1]) + one(left[1], right[0]))


def dot_full(a, b, dims):
    return lax.dot_general(a, b, (dims, ((), ())), precision=HIGHEST, preferred_element_type=F32)


def radial_parts(d, v, mask):
    q = d[0] * d[0] + d[1] * d[1] + d[2] * d[2]
    qd = 2.0 * (d[0] * v[0] + d[1] * v[1] + d[2] * v[2])
    w = 1.0 / (q + 0.01)
    decay = jnp.exp(-q) * mask
    s = decay * jnp.sqrt(w)
    u = decay * w
    s_q = -s * (1.0 + 0.5 * w)
    u_q = -u * (1.0 + w)
    shrink = 1.0 / (1.0 + s)
    t_s = shrink * shrink
    t_q = t_s * s_q
    return q, qd, w, s, u, s_q, u_q, shrink, t_s, t_q


def hessian_product(ext_ref, idt, counts_ref, kinds_ref, table_ref, w1_ref, w2_ref, b1_ref, b2_ref, fo_ref, out_ref,
                    dv, pool, env, dhi, dlo, gd, genv, gp):
    width, atoms = idt.shape
    types, levels, m1 = table_ref.shape
    m2 = w1_ref.shape[1] // m1
    ext = ext_ref.shape[1]
    banks = ext // 128
    top = float(levels - 1)
    pool[...] = jnp.zeros_like(pool)
    counts = counts_ref[...]
    kinds = kinds_ref[...]

    def used(first, rows):
        slot = lax.broadcasted_iota(jnp.int32, (rows, atoms), 0) + first
        return jnp.where(slot < counts, 1.0, 0.0).astype(F32)

    def forward(c, carry):
        first = pl.multiple_of(c * 8, 8)
        idx = idt[pl.ds(first, 8), :]
        lane = jnp.bitwise_and(idx, 127)
        bank = jnp.right_shift(idx, 7)
        fields = []
        for f in range(6):
            got = None
            for b in range(banks):
                row = jnp.broadcast_to(ext_ref[f : f + 1, b * 128 : (b + 1) * 128], (8, 128))
                part = jnp.take_along_axis(row, lane, axis=1, mode="promise_in_bounds")
                got = part if got is None else jnp.where(bank == b, part, got)
            got = got - ext_ref[f : f + 1, :atoms]
            dv[f, pl.ds(first, 8), :] = got
            fields.append(got)
        d, v = fields[:3], fields[3:]
        _, qd, _, s, u, s_q, u_q, shrink, _, t_q = radial_parts(d, v, used(first, 8))
        scaled = s * shrink * top
        r = [s] + [u * e for e in d]
        dr = [s_q * qd] + [u_q * qd * d[e] + u * v[e] for e in range(3)]
        slope = -2.0 * top * t_q * qd
        tr = [slope * e for e in r]
        for k in range(levels):
            y = scaled - float(k)
            phi = jnp.exp(-(y * y))
            psi = y * phi
            for a in range(4):
                pool[a, k] += phi * r[a]
                pool[4 + a, k] += phi * dr[a] + psi * tr[a]
        return carry

    lax.fori_loop(0, width // 8, forward, 0)
    pooled = jnp.concatenate([jnp.sum(pool[a], axis=1) for a in range(8)], axis=1) / width
    kinds8 = jnp.concatenate([kinds] * 8, axis=1)
    chosen = None
    for t in range(types):
        part = dot_full(table_ref[t], pooled, ((0,), (0,)))
        chosen = part if t == 0 else jnp.where(kinds8 == t, part, chosen)
    for a in range(8):
        env[a] = chosen[:, a * atoms : (a + 1) * atoms]
    lead = [env[a, :m2, :] for a in range(8)]

    def describe(m, carry):
        rows = [env[a, pl.ds(m, 1), :] for a in range(8)]
        plain = rows[0] * lead[0]
        moved = rows[4] * lead[0] + rows[0] * lead[4]
        for a in range(1, 4):
            plain += rows[a] * lead[a]
            moved += rows[4 + a] * lead[a] + rows[a] * lead[4 + a]
        place = pl.ds(pl.multiple_of(m * m2, m2), m2)
        for at, value in ((0, plain), (1, moved)):
            high, low = split(value)
            dhi[place, at * atoms : (at + 1) * atoms] = high
            dlo[place, at * atoms : (at + 1) * atoms] = low
        return carry

    lax.fori_loop(0, m1, describe, 0, unroll=4)
    w1 = split(w1_ref[...])
    z1 = dot_parts(w1, (dhi[...], dlo[...]), ((1,), (0,)))
    fit = b1_ref.shape[1]
    lines = jnp.concatenate([b1_ref[...], b2_ref[...], fo_ref[...], jnp.zeros((5, fit), F32)], axis=0)
    same = lax.broadcasted_iota(jnp.int32, (8, 8), 0) == lax.broadcasted_iota(jnp.int32, (8, 8), 1)
    cols = dot_full(lines, jnp.where(same, 1.0, 0.0).astype(F32), ((0,), (0,)))
    b1, b2, fo = cols[:, 0:1], cols[:, 1:2], cols[:, 2:3]
    h1 = jnp.tanh(z1[:, :atoms] + b1)
    gate1 = 1.0 - h1 * h1
    dh1 = gate1 * z1[:, atoms:]
    w2 = w2_ref[...]
    z2 = dot_full(w2, jnp.concatenate([h1, dh1], axis=1), ((0,), (0,)))
    t2 = jnp.tanh(z2[:, :atoms] + b2)
    gate2 = 1.0 - t2 * t2
    dt2 = gate2 * z2[:, atoms:]
    gz2 = jnp.concatenate([fo * gate2, fo * (-2.0 * t2 * dt2)], axis=1)
    gh = dot_full(w2, gz2, ((1,), (0,)))
    gh1 = gh[:, :atoms] + fo
    gz1 = jnp.concatenate([gh1 * gate1, gh[:, atoms:] * gate1 - 2.0 * gh1 * h1 * dh1], axis=1)
    gd[...] = dot_parts(w1, split(gz1), ((0,), (0,)))

    def describe_back(m, acc):
        place = pl.ds(pl.multiple_of(m * m2, m2), m2)
        g = gd[place, :atoms]
        dg = gd[place, atoms:]
        out = []
        for a in range(4):
            genv[a, pl.ds(m, 1), :] = jnp.sum(g * lead[a], axis=0, keepdims=True)
            genv[4 + a, pl.ds(m, 1), :] = jnp.sum(
                dg * lead[a] + g * lead[4 + a], axis=0, keepdims=True
            )
        for a in range(4):
            out.append(acc[a] + g * env[a, pl.ds(m, 1), :])
        for a in range(4):
            out.append(
                acc[4 + a]
                + dg * env[a, pl.ds(m, 1), :]
                + g * env[4 + a, pl.ds(m, 1), :]
            )
        return tuple(out)

    acc = lax.fori_loop(0, m1, describe_back, tuple(jnp.zeros((m2, atoms), F32) for _ in range(8)), unroll=2)
    for a in range(8):
        genv[a, :m2, :] += acc[a]
    total = None
    pulled = jnp.concatenate([genv[a] for a in range(8)], axis=1)
    for t in range(types):
        part = dot_full(table_ref[t], jnp.where(kinds8 == t, pulled, 0.0), ((1,), (0,)))
        total = part if total is None else total + part
    total = total / width
    for a in range(8):
        gp[a] = total[:, a * atoms : (a + 1) * atoms]
    low_iota = lax.broadcasted_iota(jnp.int32, (128, atoms), 0)

    def backward(c, carry):
        acc, centre = carry
        first = pl.multiple_of(c * 8, 8)
        d = [dv[f, pl.ds(first, 8), :] for f in range(3)]
        v = [dv[f, pl.ds(first, 8), :] for f in range(3, 6)]
        q, qd, w, s, u, s_q, u_q, shrink, t_s, t_q = radial_parts(d, v, used(first, 8))
        s_qq = -s_q * (1.0 + 0.5 * w) + 0.5 * s * w * w
        u_qq = -u_q * (1.0 + w) + u * w * w
        t_qq = -2.0 * t_s * shrink * s_q * s_q + t_s * s_qq
        scaled = s * shrink * top
        zero = jnp.zeros((8, atoms), F32)
        s0, s1, s2, e0, e1 = ([zero] * 4 for _ in range(5))
        for k in range(levels):
            y = scaled - float(k)
            phi = jnp.exp(-(y * y))
            psi = y * phi
            chi = y * psi
            for a in range(4):
                g = gp[a, k : k + 1, :]
                h = gp[4 + a, k : k + 1, :]
                s0[a] = s0[a] + g * phi
                s1[a] = s1[a] + g * psi
                s2[a] = s2[a] + g * chi
                e0[a] = e0[a] + h * phi
                e1[a] = e1[a] + h * psi
        step = t_q * qd
        val = s0
        val_t = [-2.0 * top * e for e in s1]
        val_tt = [top * top * (4.0 * s2[a] - 2.0 * s0[a]) for a in range(4)]
        dval = [e0[a] + val_t[a] * step for a in range(4)]
        dval_t = [-2.0 * top * e1[a] + val_tt[a] * step for a in range(4)]
        big = val[1] * d[0] + val[2] * d[1] + val[3] * d[2]
        big_t = val_t[1] * d[0] + val_t[2] * d[1] + val_t[3] * d[2]
        dbig = sum(dval[1 + e] * d[e] + val[1 + e] * v[e] for e in range(3))
        dbig_t = sum(dval_t[1 + e] * d[e] + val_t[1 + e] * v[e] for e in range(3))
        kern = t_q * (val_t[0] * s + big_t * u) + val[0] * s_q + big * u_q
        dkern = (
            t_q * (dval_t[0] * s + dbig_t * u)
            + dval[0] * s_q
            + dbig * u_q
            + qd * (
                t_qq * (val_t[0] * s + big_t * u)
                + t_q * (val_t[0] * s_q + big_t * u_q)
                + val[0] * s_qq
                + big * u_qq
            )
        )
        du = u_q * qd
        force = [2.0 * (v[e] * kern + d[e] * dkern) + du * val[1 + e] + u * dval[1 + e] for e in range(3)]
        centre = tuple(centre[e] - force[e] for e in range(3))
        idx = idt[pl.ds(first, 8), :]
        lane = jnp.bitwise_and(idx, 127)
        bank = jnp.right_shift(idx, 7)
        rows = []
        for e in range(3):
            high = force[e].astype(BF16).astype(F32)
            for part in (high, force[e] - high):
                for b in range(banks):
                    rows.append(jnp.where(bank == b, part, 0.0))
        lefts, rights = [], []
        for r in range(8):
            lefts.append(jnp.concatenate([x[r : r + 1, :] for x in rows], axis=0).astype(BF16))
            rights.append(jnp.where(lane[r : r + 1, :] == low_iota, 1.0, 0.0).astype(BF16))
        acc = acc + lax.dot_general(
            jnp.concatenate(lefts, axis=1),
            jnp.concatenate(rights, axis=1),
            (((1,), (1,)), ((), ())),
            preferred_element_type=F32,
        )
        return acc, centre

    out_ref[...] = jnp.zeros_like(out_ref)
    start = (jnp.zeros((6 * banks, 128), F32), tuple(jnp.zeros((8, atoms), F32) for _ in range(3)))
    acc, centre = lax.fori_loop(0, width // 8, backward, start)
    for e in range(3):
        base = 2 * banks * e
        for b in range(banks):
            row = acc[base + b : base + b + 1] + acc[base + banks + b : base + banks + b + 1]
            if b == 0:
                row = row + jnp.sum(centre[e], axis=0, keepdims=True)
            out_ref[e : e + 1, b * 128 : (b + 1) * 128] = row


AXES = ("gx", "gy", "gz")
MESH = pl.DeviceIdType.MESH
GROUP_LIMIT = 32


def sizes_of():
    return [lax.axis_size(axis) for axis in AXES]


def plane_offsets():
    def along(size):
        return (0, 1) if size == 2 else (0, 1, -1)

    _, ny, nz = sizes_of()
    return [(dy, dz) for dz in along(nz) for dy in along(ny)]


def device_at(shift):
    return {
        axis: lax.rem(lax.axis_index(axis) + (step + peers) % peers, peers)
        for axis, step, peers in zip(AXES, shift, sizes_of())
    }


def reduction_groups():
    sizes = sizes_of()
    groups = []
    for at in range(3):
        if groups and groups[-1][1] * sizes[at] <= GROUP_LIMIT:
            groups[-1] = (groups[-1][0] + [at], groups[-1][1] * sizes[at])
        else:
            groups.append(([at], sizes[at]))
    out = []
    for members, count in groups:
        shifts = [[0, 0, 0]]
        for at in members:
            shifts = [s[:at] + [step] + s[at + 1 :] for s in shifts for step in range(sizes[at])]
        out.append((members, count, [tuple(s) for s in shifts if any(s)]))
    return out


def place_in(members):
    sizes = sizes_of()
    me = 0
    for at in members:
        me = me * sizes[at] + lax.axis_index(AXES[at])
    return me


def three_parts(x):
    high = x.astype(BF16)
    rest = x - high.astype(F32)
    middle = rest.astype(BF16)
    low = (rest - middle.astype(F32)).astype(BF16)
    return jnp.concatenate([high.astype(F32), middle.astype(F32), low.astype(F32)], axis=0).astype(BF16)


def select_dot(x, onehot, dims):
    n = x.shape[0]
    out = lax.dot_general(three_parts(x), onehot, (dims, ((), ())), preferred_element_type=F32)
    return (out[:n] + out[n : 2 * n]) + out[2 * n :]


def chosen_columns(map_row, columns):
    rows = lax.broadcasted_iota(jnp.int32, (columns, map_row.shape[1]), 0).astype(F32)
    return jnp.where(rows == map_row, 1.0, 0.0).astype(BF16)


def sides(parts, early):
    if -1 in parts:
        return jnp.where(early, parts[-1], parts[1])
    return parts[1]


def one_side(x, step, distinct, early):
    if not distinct:
        return x
    return jnp.where(early, x, 0.0) if step == -1 else jnp.where(early, 0.0, x)


class Sender:
    def __init__(self, send_sem, recv_sem):
        self.send_sem, self.recv_sem, self.used, self.started = send_sem, recv_sem, 0, []

    def send(self, source, target, shift):
        copy = pltpu.make_async_remote_copy(
            src_ref=source,
            dst_ref=target,
            send_sem=self.send_sem.at[self.used],
            recv_sem=self.recv_sem.at[self.used],
            device_id=device_at(shift),
            device_id_type=MESH,
        )
        copy.start()
        self.used += 1
        self.started.append(copy)
        return copy


def lanczos_kernel(*refs, inputs, copies):
    hbm, (next_ref, corr_ref, norm_ref) = refs[:inputs], refs[inputs : inputs + 3]
    local = refs[inputs + 3 : 2 * inputs + 3]
    (idt, load_sem, send_sem, recv_sem, ext, work, mine, face, raw_land, low_land, up_land, back_raw, back_face,
     raw_back, low_back, up_back, stack, gram_tile, gram_land, row_tile, row_land, *hvp_scratch) = refs[2 * inputs + 3 :]
    places, basis, ids, counts, kinds, map_x, map_y, map_z, table, w1, w2, b1, b2, fo = local
    atoms = places.shape[2]
    stored = basis.shape[0]
    rows = stack.shape[0]
    pair = 2 * map_x.shape[1]
    sizes = sizes_of()
    entries = 3 * atoms * sizes[0] * sizes[1] * sizes[2]
    planes = plane_offsets()
    groups = reduction_groups()
    faces = ((1, low_land, up_back), (-1, up_land, low_back))

    partners = set()
    for dy, dz in planes:
        for dx in (-1, 0, 1):
            partners.add(tuple(step % peers for step, peers in zip((dx, dy, dz), sizes)))
    for _, _, shifts in groups:
        partners.update(shifts)
    partners = sorted(partners - {(0, 0, 0)})
    opposite = {tuple(-step % peers for step, peers in zip(shift, sizes)) for shift in partners}
    assert opposite == set(partners)
    barrier = pltpu.get_barrier_semaphore()
    for shift in partners:
        pl.semaphore_signal(barrier, inc=1, device_id=device_at(shift), device_id_type=MESH)
    loads = [pltpu.make_async_copy(a, b, load_sem.at[at]) for at, (a, b) in enumerate(zip(hbm, local))]
    for at in (0, 1, 5, 6, 7, 2, 3, 4, 8, 9, 10, 11, 12, 13):
        loads[at].start()
    early = lax.broadcasted_iota(jnp.int32, (8, pair), 1) < pair // 2
    line = lax.broadcasted_iota(jnp.int32, (8, pair), 0)
    for at in (0, 1, 5, 6, 7):
        loads[at].wait()
    for c in range(3):
        mine[c : c + 1, :] = places[c]
        mine[3 + c : 4 + c, :] = basis[stored - 1, c]
    map_rows = [jnp.concatenate([m[1:2, :], m[0:1, :]], axis=1).astype(F32) for m in (map_x, map_y, map_z)]
    mine[6:7, :] = map_rows[1]
    mine[7:8, :] = map_rows[2]
    pick_x = chosen_columns(map_rows[0], atoms)
    face[...] = select_dot(mine[...], pick_x, ((1,), (0,)))
    pl.semaphore_wait(barrier, len(partners))

    sender = Sender(send_sem, recv_sem)
    arriving = []
    for at, (dy, dz) in reversed(list(enumerate(planes))):
        for dx, land, _ in faces:
            arriving.append(sender.send(face, land.at[at], (dx, -dy, -dz)))
        if at:
            arriving.append(sender.send(mine, raw_land.at[at], (0, -dy, -dz)))

    stack[rows - 8 :, :] = jnp.zeros((8, 3 * atoms), F32)
    for k in range(stored):
        for c in range(3):
            stack[k : k + 1, c * atoms : (c + 1) * atoms] = basis[k, c]
    gram = dot_full(stack[...], stack[...], ((1,), (1,)))
    gram_tile[...] = jnp.concatenate([gram[r : r + 8] for r in range(0, rows, 8)], axis=1)
    for at in (2, 3, 4, 8, 9, 10, 11, 12, 13):
        loads[at].wait()
    idt[...] = ids[...].T
    for copy in arriving:
        copy.wait_recv()

    def shifted(x, row):
        return x + jnp.where(line == row, jnp.where(early, -1.0, 1.0), 0.0)

    raw = {plane: mine[...] if at == 0 else raw_land[at] for at, plane in enumerate(planes)}
    wide = {
        plane: jnp.concatenate([raw[plane], shifted(jnp.where(early, low_land[at], up_land[at]), 0)], axis=1)
        for at, plane in enumerate(planes)
    }
    pick_y, pick_z, wider = {}, {}, {}
    for dz in sorted({dz for _, dz in planes}):
        got = {}
        for dy in (1, -1):
            if (dy, dz) in raw:
                pick_y[dy, dz] = chosen_columns(raw[dy, dz][6:7, :], atoms + pair)
                got[dy] = select_dot(wide[dy, dz], pick_y[dy, dz], ((1,), (0,)))
        wider[dz] = jnp.concatenate([wide[0, dz], shifted(sides(got, early), 1)], axis=1)
    got = {}
    for dz in (1, -1):
        if dz in wider:
            pick_z[dz] = chosen_columns(raw[0, dz][7:8, :], atoms + 2 * pair)
            got[dz] = select_dot(wider[dz], pick_z[dz], ((1,), (0,)))
    ext[:, : atoms + 2 * pair] = wider[0]
    ext[:, atoms + 2 * pair :] = shifted(sides(got, early), 2)

    started = []
    members, _, shifts = groups[0]
    me = place_in(members)
    gram_land[me] = gram_tile[...]
    for shift in shifts:
        started.append(sender.send(gram_land.at[me], gram_land.at[me], shift))

    hessian_product(ext, idt, counts, kinds, table, w1, w2, b1, b2, fo, work, *hvp_scratch)

    many_y, many_z = -1 in {dy for dy, _ in planes}, -1 in wider
    back = {0: work[:, : atoms + 2 * pair]}
    for dz in pick_z:
        part = one_side(work[:, atoms + 2 * pair :], dz, many_z, early)
        back[dz] = select_dot(part, pick_z[dz], ((1,), (1,)))
    terms = {(0, dz): x[:, : atoms + pair] for dz, x in back.items()}
    for dy, dz in pick_y:
        part = one_side(back[dz][:, atoms + pair :], dy, many_y, early)
        terms[dy, dz] = select_dot(part, pick_y[dy, dz], ((1,), (1,)))
    arriving = []
    for at, (dy, dz) in reversed(list(enumerate(planes))):
        back_raw[at] = terms[dy, dz][:, :atoms]
        back_face[at] = terms[dy, dz][:, atoms:]
        for dx, _, land in faces:
            arriving.append(sender.send(back_face.at[at], land.at[at], (-dx, dy, dz)))
        if at:
            arriving.append(sender.send(back_raw.at[at], raw_back.at[at], (0, dy, dz)))

    for copy in started:
        copy.wait_recv()
    total = gram_land[0]
    for other in range(1, groups[0][1]):
        total = total + gram_land[other]
    base = groups[0][1]
    for members, count, shifts in groups[1:]:
        me = base + place_in(members)
        gram_land[me] = total
        started = [sender.send(gram_land.at[me], gram_land.at[me], shift) for shift in shifts]
        for copy in started:
            copy.wait_recv()
        total = gram_land[base]
        for other in range(1, count):
            total = total + gram_land[base + other]
        base += count
    gram = jnp.concatenate([total[:, r : r + rows] for r in range(0, rows * rows // 8, rows)], axis=0) / entries

    for copy in arriving:
        copy.wait_recv()
    own = back_raw[0]
    low, up = low_back[0], up_back[0]
    for at in range(1, len(planes)):
        own = own + raw_back[at]
        low = low + low_back[at]
        up = up + up_back[at]
    own = own + select_dot(jnp.where(early, up, low), pick_x, ((1,), (1,)))
    hv = jnp.concatenate([own[c : c + 1, :] for c in range(3)], axis=1)
    stack[stored : stored + 1, :] = hv
    sums = dot_full(jnp.broadcast_to(hv, (8, 3 * atoms)), stack[...], ((1,), (1,)))
    sums = jnp.concatenate([sums[0:1], jnp.zeros((1, row_tile.shape[1] - rows), F32)], axis=1)
    base = 0
    for members, count, shifts in groups:
        me = base + place_in(members)
        row_land[me] = sums
        started = [sender.send(row_land.at[me], row_land.at[me], shift) for shift in shifts]
        for copy in started:
            copy.wait_recv()
        sums = row_land[base]
        for other in range(1, count):
            sums = sums + row_land[base + other]
        base += count
    for copy in sender.started:
        copy.wait_send()
    assert sender.used == copies
    lane = lax.broadcasted_iota(jnp.int32, (1, rows), 1)
    sums = sums[:, :rows] / entries
    kept = jnp.where(lane < stored, sums, 0.0)
    both = jnp.concatenate([gram, stack[...]], axis=1)
    mixed = dot_full(jnp.broadcast_to(kept, (8, rows)), both, ((1,), (0,)))[0:1]
    plain = sums[:, stored : stored + 1]
    cross = jnp.sum(mixed[:, :rows] * kept - 2.0 * kept * kept, axis=1, keepdims=True)
    norm = jnp.sqrt(plain + cross + 1e-06)
    norm_ref[...] = norm
    corr_ref[...] = sums[:, :stored]
    for c in range(3):
        part = slice(c * atoms, (c + 1) * atoms)
        next_ref[c] = (hv[:, part] - mixed[:, rows:][:, part]) / norm


def on_device(positions, basis, neighbours, used_count, kinds, map_x, map_y, map_z,
              table, fit_w1, fit_b1, fit_w2, fit_b2, fit_out):
    atoms = positions.shape[-1]
    width = neighbours.shape[-1]
    stored = basis.shape[0]
    types, levels, m1 = table.shape
    m2 = fit_w1.shape[0] // m1
    pair = 2 * map_x.shape[-1]
    ext = atoms + 3 * pair
    args = [
        positions.reshape(3, 1, atoms),
        basis.reshape(stored, 3, 1, atoms),
        neighbours.reshape(atoms, width),
        used_count.reshape(1, atoms),
        kinds.reshape(1, atoms),
        map_x.reshape(2, -1),
        map_y.reshape(2, -1),
        map_z.reshape(2, -1),
        table,
        fit_w1.T,
        fit_w2,
        fit_b1[None],
        fit_b2[None],
        fit_out[None],
    ]
    rows = (stored + 8) // 8 * 8
    planes = len(plane_offsets())
    groups = reduction_groups()
    slots = sum(count for _, count, _ in groups)
    copies = 2 * (3 * planes - 1) + 2 * sum(len(shifts) for _, _, shifts in groups)
    any_space = pl.BlockSpec(memory_space=pl.ANY)
    vmem = pl.BlockSpec(memory_space=pltpu.VMEM)
    tile = pltpu.VMEM((planes, 8, pair), F32)
    next_vector, correlations, norm = pl.pallas_call(
        functools.partial(lanczos_kernel, inputs=len(args), copies=copies),
        out_shape=(
            jax.ShapeDtypeStruct((3, 1, atoms), F32),
            jax.ShapeDtypeStruct((1, stored), F32),
            jax.ShapeDtypeStruct((1, 1), F32),
        ),
        in_specs=[any_space] * len(args),
        out_specs=(vmem,) * 3,
        scratch_shapes=[pltpu.VMEM(x.shape, x.dtype) for x in args] + [
            pltpu.VMEM((width, atoms), jnp.int32),
            pltpu.SemaphoreType.DMA((len(args),)),
            pltpu.SemaphoreType.DMA((copies,)),
            pltpu.SemaphoreType.DMA((copies,)),
            pltpu.VMEM((8, ext), F32),
            pltpu.VMEM((8, ext), F32),
            pltpu.VMEM((8, pair), F32),
            pltpu.VMEM((8, pair), F32),
            tile, tile, tile, tile, tile, tile, tile, tile,
            pltpu.VMEM((rows, 3 * atoms), F32),
            pltpu.VMEM((8, rows * rows // 8), F32),
            pltpu.VMEM((slots, 8, rows * rows // 8), F32),
            pltpu.VMEM((1, 128), F32),
            pltpu.VMEM((slots, 1, 128), F32),
            pltpu.VMEM((6, width, atoms), F32),
            pltpu.VMEM((8, levels, 8, atoms), F32),
            pltpu.VMEM((8, m1, atoms), F32),
            pltpu.VMEM((m1 * m2, 2 * atoms), BF16),
            pltpu.VMEM((m1 * m2, 2 * atoms), BF16),
            pltpu.VMEM((m1 * m2, 2 * atoms), F32),
            pltpu.VMEM((8, m1, atoms), F32),
            pltpu.VMEM((8, levels, atoms), F32),
        ],
        compiler_params=pltpu.CompilerParams(
            collective_id=0, has_side_effects=True, vmem_limit_bytes=60 << 20
        ),
        name="lanczos",
    )(*args)
    return next_vector.reshape(positions.shape), correlations.reshape(stored), norm.reshape(())


def solution(mesh):
    placed = (
        P(None, "gx", "gy", "gz", None),
        P(None, None, "gx", "gy", "gz", None),
        P("gx", "gy", "gz", None, None),
        P("gx", "gy", "gz", None),
        P("gx", "gy", "gz", None),
        P("gx", "gy", "gz", None, None),
        P("gx", "gy", "gz", None, None),
        P("gx", "gy", "gz", None, None),
        P(),
        P(),
        P(),
        P(),
        P(),
        P(),
    )
    return jax.shard_map(
        on_device,
        mesh=mesh,
        in_specs=placed,
        out_specs=(P(None, "gx", "gy", "gz", None), P(), P()),
        check_vma=False,
    )
```

```python
import functools

import jax
import jax.numpy as jnp
from jax import lax
from jax.experimental import pallas as pl
from jax.experimental.pallas import tpu as pltpu
from jax.sharding import PartitionSpec as P

F32, BF16 = jnp.float32, jnp.bfloat16
HIGHEST = lax.Precision.HIGHEST
CHUNK = 8


def split(x):
    high = x.astype(BF16)
    return high, (x - high.astype(F32)).astype(BF16)


def left_parts(x):
    high, low = split(x)
    return jnp.concatenate([high, low, high], axis=1)


def right_parts(x):
    high, low = split(x)
    return jnp.concatenate([high, high, low], axis=0)


def matmul(a, b):
    return lax.dot_general(a, b, (((1,), (0,)), ((), ())), preferred_element_type=F32)


def dot_full(a, b, dims):
    return lax.dot_general(a, b, (dims, ((), ())), precision=HIGHEST, preferred_element_type=F32)


def padded(x, rows, columns):
    if columns > x.shape[1]:
        x = jnp.concatenate([x, jnp.zeros((x.shape[0], columns - x.shape[1]), x.dtype)], axis=1)
    if rows > x.shape[0]:
        x = jnp.concatenate([x, jnp.zeros((rows - x.shape[0], x.shape[1]), x.dtype)], axis=0)
    return x


def up_to(n, step):
    return (n + step - 1) // step * step


def hvp_shapes(atoms, width, types, levels, m1, m2, fit):
    fit_wide, m1_wide = up_to(fit, 128), up_to(m1, 128)
    return dict(
        idt=((width, atoms), jnp.int32),
        onehot=((width // CHUNK, 128, CHUNK * atoms), BF16),
        w1_right=((2 * fit, m1 * m2), BF16),
        w1_left=((m1 * m2, 3 * fit_wide), BF16),
        w2_right=((fit, 3 * fit_wide), BF16),
        w2_left=((fit, 3 * fit_wide), BF16),
        columns=((fit, 8), F32),
        table_up=((types * up_to(m1, 8), 3 * levels * CHUNK), BF16),
        table_down=((types * levels, 3 * m1_wide), BF16),
        dv=((6, width, atoms), F32),
        radial=((5, width, atoms), F32),
        mix=((9, width, atoms), F32),
        gauss=((3, levels, width, atoms), F32),
        pool=((levels * CHUNK, 8 * atoms), F32),
        env=((8, up_to(m1, 8), atoms), F32),
        dhi=((m1 * m2, 2 * atoms), BF16),
        dlo=((m1 * m2, 2 * atoms), BF16),
        gd=((m1 * m2, 2 * atoms), F32),
        genv=((8, m1_wide, atoms), F32),
        gp=((levels, 8 * atoms), F32),
        forces=((width * 8, atoms), F32),
    )


def prepare_matrices(h, table_ref, w1_ref, w2_ref, b1_ref, b2_ref, fo_ref):
    types, levels, m1 = table_ref.shape
    width = h.idt.shape[0]
    fit = w1_ref.shape[0]
    fit_wide = h.w1_left.shape[1] // 3
    m1_wide = h.table_down.shape[1] // 3
    high, low = split(w1_ref[...])
    h.w1_right[:fit, :] = high
    h.w1_right[fit:, :] = low
    h.w1_left[...] = left_parts(padded(w1_ref[...], fit_wide, 0).T)
    w2 = padded(w2_ref[...], fit_wide, fit_wide)
    h.w2_left[...] = left_parts(w2[:fit])
    h.w2_right[...] = left_parts(w2.T[:fit])
    lines = jnp.concatenate([b1_ref[...], b2_ref[...], fo_ref[...], jnp.zeros((5, fit), F32)], axis=0)
    same = lax.broadcasted_iota(jnp.int32, (8, 8), 0) == lax.broadcasted_iota(jnp.int32, (8, 8), 1)
    h.columns[...] = dot_full(lines, jnp.where(same, 1.0, 0.0).astype(F32), ((0,), (0,)))
    m1_rows = h.table_up.shape[0] // types
    level = lax.broadcasted_iota(jnp.int32, (levels, levels * CHUNK), 0)
    slot = lax.broadcasted_iota(jnp.int32, (levels, levels * CHUNK), 1)
    spread = jnp.where(jnp.right_shift(slot, CHUNK.bit_length() - 1) == level, 1.0 / width, 0.0).astype(F32)
    for t in range(types):
        up = padded(dot_full(table_ref[t], spread, ((0,), (0,))), m1_rows, 0)
        h.table_up[t * m1_rows : (t + 1) * m1_rows, :] = left_parts(up)
        h.table_down[t * levels : (t + 1) * levels, :] = left_parts(padded(table_ref[t] / width, 0, m1_wide))
    tail = m1 // 8 * 8
    h.genv[:, tail:, :] = jnp.zeros((8, m1_wide - tail, h.genv.shape[2]), F32)
    h.forces[...] = jnp.zeros_like(h.forces)


def prepare_scatter(h, ids_ref):
    width, atoms = h.idt.shape
    h.idt[...] = ids_ref[...].T
    column = lax.broadcasted_iota(jnp.int32, (128, atoms), 0)

    def one(c, carry):
        lane = jnp.bitwise_and(h.idt[pl.ds(pl.multiple_of(c * CHUNK, CHUNK), CHUNK), :], 127)
        for r in range(CHUNK):
            hit = jnp.where(lane[r : r + 1, :] == column, 1.0, 0.0)
            h.onehot[c, :, r * atoms : (r + 1) * atoms] = hit.astype(BF16)
        return carry

    lax.fori_loop(0, width // CHUNK, one, 0)


def pair_terms(h, ext_ref, counts):
    width, atoms = h.idt.shape
    levels = h.gauss.shape[1]
    banks = ext_ref.shape[1] // 128
    top = float(levels - 1)

    def one(c, carry):
        first = pl.multiple_of(c * CHUNK, CHUNK)
        here = pl.ds(first, CHUNK)
        idx = h.idt[here, :]
        lane = jnp.bitwise_and(idx, 127)
        bank = jnp.right_shift(idx, 7)
        fields = []
        for f in range(6):
            got = None
            for b in range(banks):
                row = jnp.broadcast_to(ext_ref[f : f + 1, b * 128 : (b + 1) * 128], (CHUNK, 128))
                part = jnp.take_along_axis(row, lane, axis=1, mode="promise_in_bounds")
                got = part if got is None else jnp.where(bank == b, part, got)
            got = got - ext_ref[f : f + 1, :atoms]
            h.dv[f, here, :] = got
            fields.append(got)
        d, v = fields[:3], fields[3:]
        slot = lax.broadcasted_iota(jnp.int32, (CHUNK, atoms), 0) + first
        q = d[0] * d[0] + d[1] * d[1] + d[2] * d[2]
        qd = 2.0 * (d[0] * v[0] + d[1] * v[1] + d[2] * v[2])
        w = 1.0 / (q + 0.01)
        decay = jnp.where(slot < counts, jnp.exp(-q), 0.0)
        s = decay * jnp.sqrt(w)
        u = decay * w
        s_q = -s * (1.0 + 0.5 * w)
        u_q = -u * (1.0 + w)
        shrink = 1.0 / (1.0 + s)
        for at, value in enumerate((qd, w, s, u, shrink)):
            h.radial[at, here, :] = value
        step = s_q * qd
        for at, value in enumerate(
            [-2.0 * top * shrink * shrink * step]
            + [s] + [u * e for e in d]
            + [step] + [u_q * qd * d[e] + u * v[e] for e in range(3)]
        ):
            h.mix[at, here, :] = value
        scaled = s * shrink * top
        for k in range(levels):
            y = scaled - float(k)
            phi = jnp.exp(-(y * y))
            psi = y * phi
            h.gauss[0, k, here, :] = phi
            h.gauss[1, k, here, :] = psi
            h.gauss[2, k, here, :] = y * psi
        return carry

    lax.fori_loop(0, width // CHUNK, one, 0, unroll=2)


def pooled_terms(h):
    width, atoms = h.idt.shape
    levels = h.gauss.shape[1]
    together = 4
    zero = jnp.zeros((CHUNK, atoms), F32)
    for k0 in range(0, levels, together):

        def one(c, acc):
            here = pl.ds(pl.multiple_of(c * CHUNK, CHUNK), CHUNK)
            slope = h.mix[0, here, :]
            r = [h.mix[1 + a, here, :] for a in range(4)]
            dr = [h.mix[5 + a, here, :] for a in range(4)]
            out = []
            for k in range(together):
                phi = h.gauss[0, k0 + k, here, :]
                psi = h.gauss[1, k0 + k, here, :] * slope
                out += [acc[8 * k + a] + phi * r[a] for a in range(4)]
                out += [acc[8 * k + 4 + a] + (phi * dr[a] + psi * r[a]) for a in range(4)]
            return tuple(out)

        acc = lax.fori_loop(0, width // CHUNK, one, (zero,) * (8 * together), unroll=2)
        for k in range(together):
            for a in range(8):
                h.pool[(k0 + k) * CHUNK : (k0 + k + 1) * CHUNK, a * atoms : (a + 1) * atoms] = acc[8 * k + a]


def of_kind(kinds8, parts):
    out = parts[0]
    for t in range(1, len(parts)):
        out = jnp.where(kinds8 == t, parts[t], out)
    return out


def environment(h, kinds8, types):
    m1_rows = h.table_up.shape[0] // types
    atoms = h.idt.shape[1]
    for half in range(4):
        at = slice(half * 2 * atoms, (half + 1) * 2 * atoms)
        both = matmul(h.table_up[...], right_parts(h.pool[:, at]))
        mine = of_kind(kinds8[:, at], [both[t * m1_rows : (t + 1) * m1_rows] for t in range(types)])
        h.env[2 * half] = mine[:, :atoms]
        h.env[2 * half + 1] = mine[:, atoms:]


def fitting_net(h, m1, m2):
    fit = h.columns.shape[0]
    fit_wide = h.w2_left.shape[1] // 3
    atoms = h.idt.shape[1]
    lead = [h.env[a, :m2, :] for a in range(8)]

    def describe(m, carry):
        rows = [h.env[a, pl.ds(m, 1), :] for a in range(8)]
        plain = rows[0] * lead[0]
        moved = rows[4] * lead[0] + rows[0] * lead[4]
        for a in range(1, 4):
            plain += rows[a] * lead[a]
            moved += rows[4 + a] * lead[a] + rows[a] * lead[4 + a]
        place = pl.ds(pl.multiple_of(m * m2, m2), m2)
        for at, value in ((0, plain), (1, moved)):
            high, low = split(value)
            h.dhi[place, at * atoms : (at + 1) * atoms] = high
            h.dlo[place, at * atoms : (at + 1) * atoms] = low
        return carry

    lax.fori_loop(0, m1, describe, 0, unroll=4)
    both = matmul(h.w1_right[...], h.dhi[...])
    z1 = (both[:fit] + both[fit:]) + matmul(h.w1_right[:fit, :], h.dlo[...])
    b1, b2, fo = h.columns[:, 0:1], h.columns[:, 1:2], h.columns[:, 2:3]
    h1 = jnp.tanh(z1[:, :atoms] + b1)
    gate1 = 1.0 - h1 * h1
    dh1 = gate1 * z1[:, atoms:]
    z2 = matmul(h.w2_right[...], right_parts(padded(jnp.concatenate([h1, dh1], axis=1), fit_wide, 0)))
    t2 = jnp.tanh(z2[:, :atoms] + b2)
    gate2 = 1.0 - t2 * t2
    dt2 = gate2 * z2[:, atoms:]
    gz2 = jnp.concatenate([fo * gate2, fo * (-2.0 * t2 * dt2)], axis=1)
    gh = matmul(h.w2_left[...], right_parts(padded(gz2, fit_wide, 0)))
    gh1 = gh[:, :atoms] + fo
    gz1 = jnp.concatenate([gh1 * gate1, gh[:, atoms:] * gate1 - 2.0 * gh1 * h1 * dh1], axis=1)
    h.gd[...] = matmul(h.w1_left[...], right_parts(padded(gz1, fit_wide, 0)))

    def describe_back(m, acc):
        place = pl.ds(pl.multiple_of(m * m2, m2), m2)
        g = h.gd[place, :atoms]
        dg = h.gd[place, atoms:]
        rows = [h.env[a, pl.ds(m, 1), :] for a in range(8)]
        for a in range(4):
            h.genv[a, pl.ds(m, 1), :] = jnp.sum(g * lead[a], axis=0, keepdims=True)
            h.genv[4 + a, pl.ds(m, 1), :] = jnp.sum(
                dg * lead[a] + g * lead[4 + a], axis=0, keepdims=True
            )
        out = [acc[a] + g * rows[a] for a in range(4)]
        out += [acc[4 + a] + (dg * rows[a] + g * rows[4 + a]) for a in range(4)]
        return tuple(out)

    acc = lax.fori_loop(0, m1, describe_back, tuple(jnp.zeros((m2, atoms), F32) for _ in range(8)), unroll=2)
    for a in range(8):
        h.genv[a, :m2, :] += acc[a]


def pulled_back(h, kinds8, types):
    levels = h.gp.shape[0]
    atoms = h.idt.shape[1]
    for half in range(4):
        at = slice(half * 2 * atoms, (half + 1) * 2 * atoms)
        pulled = jnp.concatenate([h.genv[2 * half], h.genv[2 * half + 1]], axis=1)
        both = matmul(h.table_down[...], right_parts(pulled))
        h.gp[:, at] = of_kind(kinds8[:, at], [both[t * levels : (t + 1) * levels] for t in range(types)])


def pair_forces(h, out_ref):
    width, atoms = h.idt.shape
    levels = h.gauss.shape[1]
    banks = out_ref.shape[1] // 128
    top = float(levels - 1)

    def force_of(c, centre):
        first = pl.multiple_of(c * CHUNK, CHUNK)
        here = pl.ds(first, CHUNK)
        zero = jnp.zeros((CHUNK, atoms), F32)
        s0, s1, s2, e0, e1 = ([zero] * 4 for _ in range(5))
        for k in range(levels):
            phi, psi, chi = (h.gauss[p, k, here, :] for p in range(3))
            for a in range(4):
                g = h.gp[k : k + 1, a * atoms : (a + 1) * atoms]
                gd = h.gp[k : k + 1, (4 + a) * atoms : (5 + a) * atoms]
                s0[a] = s0[a] + g * phi
                s1[a] = s1[a] + g * psi
                s2[a] = s2[a] + g * chi
                e0[a] = e0[a] + gd * phi
                e1[a] = e1[a] + gd * psi
        d = [h.dv[f, here, :] for f in range(3)]
        v = [h.dv[f, here, :] for f in range(3, 6)]
        qd, w, s, u, shrink = (h.radial[at, here, :] for at in range(5))
        s_q = -s * (1.0 + 0.5 * w)
        u_q = -u * (1.0 + w)
        t_s = shrink * shrink
        t_q = t_s * s_q
        s_qq = -s_q * (1.0 + 0.5 * w) + 0.5 * s * w * w
        u_qq = -u_q * (1.0 + w) + u * w * w
        t_qq = -2.0 * t_s * shrink * s_q * s_q + t_s * s_qq
        step = t_q * qd
        val = s0
        val_t = [-2.0 * top * e for e in s1]
        val_tt = [top * top * (4.0 * s2[a] - 2.0 * s0[a]) for a in range(4)]
        dval = [e0[a] + val_t[a] * step for a in range(4)]
        dval_t = [-2.0 * top * e1[a] + val_tt[a] * step for a in range(4)]
        big = val[1] * d[0] + val[2] * d[1] + val[3] * d[2]
        big_t = val_t[1] * d[0] + val_t[2] * d[1] + val_t[3] * d[2]
        dbig = sum(dval[1 + e] * d[e] + val[1 + e] * v[e] for e in range(3))
        dbig_t = sum(dval_t[1 + e] * d[e] + val_t[1 + e] * v[e] for e in range(3))
        flow = val_t[0] * s + big_t * u
        kern = t_q * flow + val[0] * s_q + big * u_q
        dkern = (
            t_q * (dval_t[0] * s + dbig_t * u)
            + dval[0] * s_q
            + dbig * u_q
            + qd * (t_qq * flow + t_q * (val_t[0] * s_q + big_t * u_q) + val[0] * s_qq + big * u_qq)
        )
        du = u_q * qd
        out = []
        for e in range(3):
            force = 2.0 * (v[e] * kern + d[e] * dkern) + du * val[1 + e] + u * dval[1 + e]
            high = force.astype(BF16).astype(F32)
            h.forces[pl.ds(first * 8 + e, CHUNK, stride=8), :] = high
            h.forces[pl.ds(first * 8 + 3 + e, CHUNK, stride=8), :] = force - high
            out.append(centre[e] - force)
        return tuple(out)

    zero = jnp.zeros((CHUNK, atoms), F32)
    centre = lax.fori_loop(0, width // CHUNK, force_of, (zero,) * 3)

    def scatter(c, acc):
        first = pl.multiple_of(c * CHUNK, CHUNK)
        bank = jnp.right_shift(h.idt[pl.ds(first, CHUNK), :], 7)
        lefts = []
        for r in range(CHUNK):
            part = h.forces[pl.ds(pl.multiple_of((first + r) * 8, 8), 8), :]
            mine = jnp.broadcast_to(bank[r : r + 1, :], part.shape)
            lefts.append(jnp.concatenate([jnp.where(mine == b, part, 0.0) for b in range(banks)], axis=0).astype(BF16))
        return acc + lax.dot_general(
            jnp.concatenate(lefts, axis=1), h.onehot[c], (((1,), (1,)), ((), ())), preferred_element_type=F32
        )

    acc = lax.fori_loop(0, width // CHUNK, scatter, jnp.zeros((8 * banks, 128), F32))
    for b in range(banks):
        part = acc[8 * b : 8 * b + 8]
        out_ref[:, b * 128 : (b + 1) * 128] = part + jnp.concatenate([part[3:], part[:3]], axis=0)
    for e in range(3):
        out_ref[e : e + 1, :atoms] += jnp.sum(centre[e], axis=0, keepdims=True)


def hessian_product(h, ext_ref, counts_ref, kinds_ref, out_ref, types, m1, m2):
    kinds8 = jnp.concatenate([kinds_ref[...]] * 8, axis=1)
    pair_terms(h, ext_ref, counts_ref[...])
    pooled_terms(h)
    environment(h, kinds8, types)
    fitting_net(h, m1, m2)
    pulled_back(h, kinds8, types)
    pair_forces(h, out_ref)


class Scratch:
    def __init__(self, names, refs):
        for name, ref in zip(names, refs, strict=True):
            setattr(self, name, ref)


AXES = ("gx", "gy", "gz")
MESH = pl.DeviceIdType.MESH
GROUP_LIMIT = 32


def sizes_of():
    return [lax.axis_size(axis) for axis in AXES]


def plane_offsets():
    def along(size):
        return (0, 1) if size == 2 else (0, 1, -1)

    _, ny, nz = sizes_of()
    return [(dy, dz) for dz in along(nz) for dy in along(ny)]


def device_at(shift):
    return {
        axis: lax.rem(lax.axis_index(axis) + (step + peers) % peers, peers)
        for axis, step, peers in zip(AXES, shift, sizes_of())
    }


def reduction_groups():
    sizes = sizes_of()
    groups = []
    for at in range(3):
        if groups and groups[-1][1] * sizes[at] <= GROUP_LIMIT:
            groups[-1] = (groups[-1][0] + [at], groups[-1][1] * sizes[at])
        else:
            groups.append(([at], sizes[at]))
    out = []
    for members, count in groups:
        shifts = [[0, 0, 0]]
        for at in members:
            shifts = [s[:at] + [step] + s[at + 1 :] for s in shifts for step in range(sizes[at])]
        out.append((members, count, [tuple(s) for s in shifts if any(s)]))
    return out


def place_in(members):
    sizes = sizes_of()
    me = 0
    for at in members:
        me = me * sizes[at] + lax.axis_index(AXES[at])
    return me


def three_parts(x):
    high = x.astype(BF16)
    rest = x - high.astype(F32)
    middle = rest.astype(BF16)
    low = (rest - middle.astype(F32)).astype(BF16)
    return jnp.concatenate([high.astype(F32), middle.astype(F32), low.astype(F32)], axis=0).astype(BF16)


def select_dot(x, onehot, dims):
    n = x.shape[0]
    out = lax.dot_general(three_parts(x), onehot, (dims, ((), ())), preferred_element_type=F32)
    return (out[:n] + out[n : 2 * n]) + out[2 * n :]


def chosen_columns(map_row, columns):
    rows = lax.broadcasted_iota(jnp.int32, (columns, map_row.shape[1]), 0).astype(F32)
    return jnp.where(rows == map_row, 1.0, 0.0).astype(BF16)


def sides(parts, early):
    if -1 in parts:
        return jnp.where(early, parts[-1], parts[1])
    return parts[1]


def one_side(x, step, distinct, early):
    if not distinct:
        return x
    return jnp.where(early, x, 0.0) if step == -1 else jnp.where(early, 0.0, x)


class Sender:
    def __init__(self, send_sem, recv_sem):
        self.send_sem, self.recv_sem, self.used, self.started = send_sem, recv_sem, 0, []

    def send(self, source, target, shift):
        copy = pltpu.make_async_remote_copy(
            src_ref=source,
            dst_ref=target,
            send_sem=self.send_sem.at[self.used],
            recv_sem=self.recv_sem.at[self.used],
            device_id=device_at(shift),
            device_id_type=MESH,
        )
        copy.start()
        self.used += 1
        self.started.append(copy)
        return copy


def lanczos_kernel(*refs, inputs, copies, names):
    hbm, (next_ref, corr_ref, norm_ref) = refs[:inputs], refs[inputs : inputs + 3]
    local = refs[inputs + 3 : 2 * inputs + 3]
    (load_sem, send_sem, recv_sem, ext, work, mine, face, raw_land, low_land, up_land, back_raw, back_face,
     raw_back, low_back, up_back, stack, gram_tile, gram_land, row_tile, row_land, *hvp_scratch) = refs[2 * inputs + 3 :]
    places, basis, ids, counts, kinds, map_x, map_y, map_z, table, w1, w2, b1, b2, fo = local
    h = Scratch(names, hvp_scratch)
    types, _, m1 = table.shape
    m2 = w1.shape[1] // m1
    atoms = places.shape[2]
    stored = basis.shape[0]
    rows = stack.shape[0]
    pair = 2 * map_x.shape[1]
    sizes = sizes_of()
    entries = 3 * atoms * sizes[0] * sizes[1] * sizes[2]
    planes = plane_offsets()
    groups = reduction_groups()
    faces = ((1, low_land, up_back), (-1, up_land, low_back))

    partners = set()
    for dy, dz in planes:
        for dx in (-1, 0, 1):
            partners.add(tuple(step % peers for step, peers in zip((dx, dy, dz), sizes)))
    for _, _, shifts in groups:
        partners.update(shifts)
    partners = sorted(partners - {(0, 0, 0)})
    opposite = {tuple(-step % peers for step, peers in zip(shift, sizes)) for shift in partners}
    assert opposite == set(partners)
    barrier = pltpu.get_barrier_semaphore()
    for shift in partners:
        pl.semaphore_signal(barrier, inc=1, device_id=device_at(shift), device_id_type=MESH)
    loads = [pltpu.make_async_copy(a, b, load_sem.at[at]) for at, (a, b) in enumerate(zip(hbm, local))]
    for at in (0, 1, 5, 6, 7, 2, 3, 4, 8, 9, 10, 11, 12, 13):
        loads[at].start()
    early = lax.broadcasted_iota(jnp.int32, (8, pair), 1) < pair // 2
    line = lax.broadcasted_iota(jnp.int32, (8, pair), 0)
    for at in (0, 1, 5, 6, 7):
        loads[at].wait()
    for c in range(3):
        mine[c : c + 1, :] = places[c]
        mine[3 + c : 4 + c, :] = basis[stored - 1, c]
    map_rows = [jnp.concatenate([m[1:2, :], m[0:1, :]], axis=1).astype(F32) for m in (map_x, map_y, map_z)]
    mine[6:7, :] = map_rows[1]
    mine[7:8, :] = map_rows[2]
    pick_x = chosen_columns(map_rows[0], atoms)
    face[...] = select_dot(mine[...], pick_x, ((1,), (0,)))
    pl.semaphore_wait(barrier, len(partners))

    sender = Sender(send_sem, recv_sem)
    arriving = []
    for at, (dy, dz) in reversed(list(enumerate(planes))):
        for dx, land, _ in faces:
            arriving.append(sender.send(face, land.at[at], (dx, -dy, -dz)))
        if at:
            arriving.append(sender.send(mine, raw_land.at[at], (0, -dy, -dz)))

    stack[rows - 8 :, :] = jnp.zeros((8, 3 * atoms), F32)
    for k in range(stored):
        for c in range(3):
            stack[k : k + 1, c * atoms : (c + 1) * atoms] = basis[k, c]
    gram = dot_full(stack[...], stack[...], ((1,), (1,)))
    gram_tile[...] = jnp.concatenate([gram[r : r + 8] for r in range(0, rows, 8)], axis=1)
    for at in (2, 3, 4, 8, 9, 10, 11, 12, 13):
        loads[at].wait()
    prepare_scatter(h, ids)
    prepare_matrices(h, table, w1, w2, b1, b2, fo)
    for copy in arriving:
        copy.wait_recv()

    def shifted(x, row):
        return x + jnp.where(line == row, jnp.where(early, -1.0, 1.0), 0.0)

    raw = {plane: mine[...] if at == 0 else raw_land[at] for at, plane in enumerate(planes)}
    wide = {
        plane: jnp.concatenate([raw[plane], shifted(jnp.where(early, low_land[at], up_land[at]), 0)], axis=1)
        for at, plane in enumerate(planes)
    }
    pick_y, pick_z, wider = {}, {}, {}
    for dz in sorted({dz for _, dz in planes}):
        got = {}
        for dy in (1, -1):
            if (dy, dz) in raw:
                pick_y[dy, dz] = chosen_columns(raw[dy, dz][6:7, :], atoms + pair)
                got[dy] = select_dot(wide[dy, dz], pick_y[dy, dz], ((1,), (0,)))
        wider[dz] = jnp.concatenate([wide[0, dz], shifted(sides(got, early), 1)], axis=1)
    got = {}
    for dz in (1, -1):
        if dz in wider:
            pick_z[dz] = chosen_columns(raw[0, dz][7:8, :], atoms + 2 * pair)
            got[dz] = select_dot(wider[dz], pick_z[dz], ((1,), (0,)))
    ext[:, : atoms + 2 * pair] = wider[0]
    ext[:, atoms + 2 * pair :] = shifted(sides(got, early), 2)

    started = []
    members, _, shifts = groups[0]
    me = place_in(members)
    gram_land[me] = gram_tile[...]
    for shift in shifts:
        started.append(sender.send(gram_land.at[me], gram_land.at[me], shift))

    hessian_product(h, ext, counts, kinds, work, types, m1, m2)

    many_y, many_z = -1 in {dy for dy, _ in planes}, -1 in wider
    back = {0: work[:, : atoms + 2 * pair]}
    for dz in pick_z:
        part = one_side(work[:, atoms + 2 * pair :], dz, many_z, early)
        back[dz] = select_dot(part, pick_z[dz], ((1,), (1,)))
    terms = {(0, dz): x[:, : atoms + pair] for dz, x in back.items()}
    for dy, dz in pick_y:
        part = one_side(back[dz][:, atoms + pair :], dy, many_y, early)
        terms[dy, dz] = select_dot(part, pick_y[dy, dz], ((1,), (1,)))
    arriving = []
    for at, (dy, dz) in reversed(list(enumerate(planes))):
        back_raw[at] = terms[dy, dz][:, :atoms]
        back_face[at] = terms[dy, dz][:, atoms:]
        for dx, _, land in faces:
            arriving.append(sender.send(back_face.at[at], land.at[at], (-dx, dy, dz)))
        if at:
            arriving.append(sender.send(back_raw.at[at], raw_back.at[at], (0, dy, dz)))

    for copy in started:
        copy.wait_recv()
    total = gram_land[0]
    for other in range(1, groups[0][1]):
        total = total + gram_land[other]
    base = groups[0][1]
    for members, count, shifts in groups[1:]:
        me = base + place_in(members)
        gram_land[me] = total
        started = [sender.send(gram_land.at[me], gram_land.at[me], shift) for shift in shifts]
        for copy in started:
            copy.wait_recv()
        total = gram_land[base]
        for other in range(1, count):
            total = total + gram_land[base + other]
        base += count
    gram = jnp.concatenate([total[:, r : r + rows] for r in range(0, rows * rows // 8, rows)], axis=0) / entries

    for copy in arriving:
        copy.wait_recv()
    own = back_raw[0]
    low, up = low_back[0], up_back[0]
    for at in range(1, len(planes)):
        own = own + raw_back[at]
        low = low + low_back[at]
        up = up + up_back[at]
    own = own + select_dot(jnp.where(early, up, low), pick_x, ((1,), (1,)))
    hv = jnp.concatenate([own[c : c + 1, :] for c in range(3)], axis=1)
    stack[stored : stored + 1, :] = hv
    sums = dot_full(jnp.broadcast_to(hv, (8, 3 * atoms)), stack[...], ((1,), (1,)))
    sums = jnp.concatenate([sums[0:1], jnp.zeros((1, row_tile.shape[1] - rows), F32)], axis=1)
    base = 0
    for members, count, shifts in groups:
        me = base + place_in(members)
        row_land[me] = sums
        started = [sender.send(row_land.at[me], row_land.at[me], shift) for shift in shifts]
        for copy in started:
            copy.wait_recv()
        sums = row_land[base]
        for other in range(1, count):
            sums = sums + row_land[base + other]
        base += count
    for copy in sender.started:
        copy.wait_send()
    assert sender.used == copies
    lane = lax.broadcasted_iota(jnp.int32, (1, rows), 1)
    sums = sums[:, :rows] / entries
    kept = jnp.where(lane < stored, sums, 0.0)
    both = jnp.concatenate([gram, stack[...]], axis=1)
    mixed = dot_full(jnp.broadcast_to(kept, (8, rows)), both, ((1,), (0,)))[0:1]
    plain = sums[:, stored : stored + 1]
    cross = jnp.sum(mixed[:, :rows] * kept - 2.0 * kept * kept, axis=1, keepdims=True)
    norm = jnp.sqrt(plain + cross + 1e-06)
    norm_ref[...] = norm
    corr_ref[...] = sums[:, :stored]
    for c in range(3):
        part = slice(c * atoms, (c + 1) * atoms)
        next_ref[c] = (hv[:, part] - mixed[:, rows:][:, part]) / norm


def on_device(positions, basis, neighbours, used_count, kinds, map_x, map_y, map_z,
              table, fit_w1, fit_b1, fit_w2, fit_b2, fit_out):
    atoms = positions.shape[-1]
    width = neighbours.shape[-1]
    stored = basis.shape[0]
    types, levels, m1 = table.shape
    m2 = fit_w1.shape[0] // m1
    pair = 2 * map_x.shape[-1]
    ext = atoms + 3 * pair
    args = [
        positions.reshape(3, 1, atoms),
        basis.reshape(stored, 3, 1, atoms),
        neighbours.reshape(atoms, width),
        used_count.reshape(1, atoms),
        kinds.reshape(1, atoms),
        map_x.reshape(2, -1),
        map_y.reshape(2, -1),
        map_z.reshape(2, -1),
        table,
        fit_w1.T,
        fit_w2,
        fit_b1[None],
        fit_b2[None],
        fit_out[None],
    ]
    rows = (stored + 8) // 8 * 8
    planes = len(plane_offsets())
    groups = reduction_groups()
    slots = sum(count for _, count, _ in groups)
    copies = 2 * (3 * planes - 1) + 2 * sum(len(shifts) for _, _, shifts in groups)
    hvp = hvp_shapes(atoms, width, types, levels, m1, m2, fit_w2.shape[0])
    any_space = pl.BlockSpec(memory_space=pl.ANY)
    vmem = pl.BlockSpec(memory_space=pltpu.VMEM)
    tile = pltpu.VMEM((planes, 8, pair), F32)
    next_vector, correlations, norm = pl.pallas_call(
        functools.partial(lanczos_kernel, inputs=len(args), copies=copies, names=tuple(hvp)),
        out_shape=(
            jax.ShapeDtypeStruct((3, 1, atoms), F32),
            jax.ShapeDtypeStruct((1, stored), F32),
            jax.ShapeDtypeStruct((1, 1), F32),
        ),
        in_specs=[any_space] * len(args),
        out_specs=(vmem,) * 3,
        scratch_shapes=[pltpu.VMEM(x.shape, x.dtype) for x in args] + [
            pltpu.SemaphoreType.DMA((len(args),)),
            pltpu.SemaphoreType.DMA((copies,)),
            pltpu.SemaphoreType.DMA((copies,)),
            pltpu.VMEM((8, ext), F32),
            pltpu.VMEM((8, ext), F32),
            pltpu.VMEM((8, pair), F32),
            pltpu.VMEM((8, pair), F32),
            tile, tile, tile, tile, tile, tile, tile, tile,
            pltpu.VMEM((rows, 3 * atoms), F32),
            pltpu.VMEM((8, rows * rows // 8), F32),
            pltpu.VMEM((slots, 8, rows * rows // 8), F32),
            pltpu.VMEM((1, 128), F32),
            pltpu.VMEM((slots, 1, 128), F32),
        ] + [pltpu.VMEM(shape, dtype) for shape, dtype in hvp.values()],
        compiler_params=pltpu.CompilerParams(
            collective_id=0, has_side_effects=True, vmem_limit_bytes=60 << 20
        ),
        name="lanczos",
    )(*args)
    return next_vector.reshape(positions.shape), correlations.reshape(stored), norm.reshape(())


def solution(mesh):
    placed = (
        P(None, "gx", "gy", "gz", None),
        P(None, None, "gx", "gy", "gz", None),
        P("gx", "gy", "gz", None, None),
        P("gx", "gy", "gz", None),
        P("gx", "gy", "gz", None),
        P("gx", "gy", "gz", None, None),
        P("gx", "gy", "gz", None, None),
        P("gx", "gy", "gz", None, None),
        P(),
        P(),
        P(),
        P(),
        P(),
        P(),
    )
    return jax.shard_map(
        on_device,
        mesh=mesh,
        in_specs=placed,
        out_specs=(P(None, "gx", "gy", "gz", None), P(), P()),
        check_vma=False,
    )
```

```python
import functools

import jax
import jax.numpy as jnp
from jax import lax
from jax.experimental import pallas as pl
from jax.experimental.pallas import tpu as pltpu
from jax.sharding import PartitionSpec as P

F32, BF16 = jnp.float32, jnp.bfloat16
HIGHEST = lax.Precision.HIGHEST
CHUNK = 8


def split(x):
    high = x.astype(BF16)
    return high, (x - high.astype(F32)).astype(BF16)


def left_parts(x):
    high, low = split(x)
    return jnp.concatenate([high, low, high], axis=1)


def right_parts(x):
    high, low = split(x)
    return jnp.concatenate([high, high, low], axis=0)


def matmul(a, b):
    return lax.dot_general(a, b, (((1,), (0,)), ((), ())), preferred_element_type=F32)


def dot_full(a, b, dims):
    return lax.dot_general(a, b, (dims, ((), ())), precision=HIGHEST, preferred_element_type=F32)


def padded(x, rows, columns):
    if columns > x.shape[1]:
        x = jnp.concatenate([x, jnp.zeros((x.shape[0], columns - x.shape[1]), x.dtype)], axis=1)
    if rows > x.shape[0]:
        x = jnp.concatenate([x, jnp.zeros((rows - x.shape[0], x.shape[1]), x.dtype)], axis=0)
    return x


def up_to(n, step):
    return (n + step - 1) // step * step


def hvp_shapes(atoms, width, types, levels, m1, m2, fit, banks):
    fit_wide, m1_wide = up_to(fit, 128), up_to(m1, 128)
    low = levels * m2
    return dict(
        idt=((width, atoms), jnp.int32),
        onehot=((width * atoms, 128), BF16),
        in_bank=((banks, width, atoms), F32),
        w1_rows=((fit_wide // 128, m1_wide * m2, 128), F32),
        w1_low=((fit_wide // 128, types * low, 128), F32),
        low_right=((types * fit, 3 * low), BF16),
        low_left=((types * low, 3 * fit_wide), BF16),
        w2_right=((fit, 3 * fit_wide), BF16),
        w2_left=((fit, 3 * fit_wide), BF16),
        columns=((fit, 8), F32),
        lead_up=((types * m2, 3 * levels), BF16),
        lead_down=((types * levels, 3 * m2), BF16),
        dv=((6, width, atoms), F32),
        radial=((5, width, atoms), F32),
        mix=((9, width, atoms), F32),
        gauss=((3, levels, width, atoms), F32),
        pooled=((8, levels, atoms), F32),
        product=((low, 2 * atoms), F32),
        pulled=((low, 2 * atoms), F32),
        gp=((levels, 8 * atoms), F32),
        forces=((width * 8, atoms), F32),
    )


def prepare_matrices(h, table_ref, w1_ref, w2_ref, b1_ref, b2_ref, fo_ref):
    types, levels, m1 = table_ref.shape
    fit, m2 = w1_ref.shape[0], w1_ref.shape[1] // m1
    halves, rows, _ = h.w1_rows.shape
    m1_wide, low = rows // m2, levels * m2
    turned = padded(w1_ref[...], halves * 128, 0).T
    tables = jnp.concatenate([padded(table_ref[t], 0, m1_wide) for t in range(types)], axis=0)
    tables = left_parts(tables)
    for half in range(halves):
        h.w1_rows[half, : m1 * m2, :] = turned[:, half * 128 : (half + 1) * 128]
        h.w1_rows[half, m1 * m2 :, :] = jnp.zeros((rows - m1 * m2, 128), F32)
    for n in range(m2):
        part = [h.w1_rows[half, pl.ds(n, m1_wide, stride=m2), :] for half in range(halves)]
        out = matmul(tables, right_parts(jnp.concatenate(part, axis=1)))
        for half in range(halves):
            h.w1_low[half, pl.ds(n, types * levels, stride=m2), :] = out[:, half * 128 : (half + 1) * 128]
    for t in range(types):
        at = slice(t * low, (t + 1) * low)
        mine = jnp.concatenate([h.w1_low[half, at, :] for half in range(halves)], axis=1)
        h.low_left[at, :] = left_parts(mine)
        h.low_right[t * fit : (t + 1) * fit, :] = left_parts(mine.T[:fit])
    w2 = padded(w2_ref[...], halves * 128, halves * 128)
    h.w2_left[...] = left_parts(w2[:fit])
    h.w2_right[...] = left_parts(w2.T[:fit])
    lines = jnp.concatenate([b1_ref[...], b2_ref[...], fo_ref[...], jnp.zeros((5, fit), F32)], axis=0)
    h.columns[...] = dot_full(lines, identity(8), ((0,), (0,)))
    for t in range(types):
        first = table_ref[t][:, :m2]
        h.lead_down[t * levels : (t + 1) * levels, :] = left_parts(first)
        h.lead_up[t * m2 : (t + 1) * m2, :] = left_parts(dot_full(first, identity(levels), ((0,), (0,))))
    h.forces[...] = jnp.zeros_like(h.forces)


def identity(n):
    same = lax.broadcasted_iota(jnp.int32, (n, n), 0) == lax.broadcasted_iota(jnp.int32, (n, n), 1)
    return jnp.where(same, 1.0, 0.0).astype(F32)


def prepare_scatter(h, ids_ref):
    width, atoms = h.idt.shape
    h.idt[...] = ids_ref[...].T
    bank = jnp.right_shift(h.idt[...], 7)
    for b in range(h.in_bank.shape[0]):
        h.in_bank[b] = jnp.where(bank == b, 1.0, 0.0).astype(F32)
    lanes = lax.broadcasted_iota(jnp.int32, (atoms, 128), 1)

    def one(c, carry):
        first = pl.multiple_of(c * CHUNK, CHUNK)
        column = jnp.bitwise_and(h.idt[pl.ds(first, CHUNK), :], 127).T
        for r in range(CHUNK):
            hit = jnp.where(column[:, r : r + 1] == lanes, 1.0, 0.0)
            h.onehot[pl.ds(pl.multiple_of((first + r) * atoms, atoms), atoms), :] = hit.astype(BF16)
        return carry

    lax.fori_loop(0, width // CHUNK, one, 0)


def pair_terms(h, ext_ref, counts):
    width, atoms = h.idt.shape
    levels = h.gauss.shape[1]
    banks = ext_ref.shape[1] // 128
    top = float(levels - 1)

    def one(c, carry):
        first = pl.multiple_of(c * CHUNK, CHUNK)
        here = pl.ds(first, CHUNK)
        idx = h.idt[here, :]
        lane = jnp.bitwise_and(idx, 127)
        bank = jnp.right_shift(idx, 7)
        fields = []
        for f in range(6):
            got = None
            for b in range(banks):
                row = jnp.broadcast_to(ext_ref[f : f + 1, b * 128 : (b + 1) * 128], (CHUNK, 128))
                part = jnp.take_along_axis(row, lane, axis=1, mode="promise_in_bounds")
                got = part if got is None else jnp.where(bank == b, part, got)
            got = got - ext_ref[f : f + 1, :atoms]
            h.dv[f, here, :] = got
            fields.append(got)
        d, v = fields[:3], fields[3:]
        slot = lax.broadcasted_iota(jnp.int32, (CHUNK, atoms), 0) + first
        q = d[0] * d[0] + d[1] * d[1] + d[2] * d[2]
        qd = 2.0 * (d[0] * v[0] + d[1] * v[1] + d[2] * v[2])
        w = 1.0 / (q + 0.01)
        decay = jnp.where(slot < counts, jnp.exp(-q), 0.0)
        s = decay * jnp.sqrt(w)
        u = decay * w
        s_q = -s * (1.0 + 0.5 * w)
        u_q = -u * (1.0 + w)
        shrink = 1.0 / (1.0 + s)
        for at, value in enumerate((qd, w, s, u, shrink)):
            h.radial[at, here, :] = value
        step = s_q * qd
        for at, value in enumerate(
            [-2.0 * top * shrink * shrink * step]
            + [s] + [u * e for e in d]
            + [step] + [u_q * qd * d[e] + u * v[e] for e in range(3)]
        ):
            h.mix[at, here, :] = value
        scaled = s * shrink * top
        for k in range(levels):
            y = scaled - float(k)
            phi = jnp.exp(-(y * y))
            psi = y * phi
            h.gauss[0, k, here, :] = phi
            h.gauss[1, k, here, :] = psi
            h.gauss[2, k, here, :] = y * psi
        return carry

    lax.fori_loop(0, width // CHUNK, one, 0, unroll=2)


def pooled_terms(h):
    width, atoms = h.idt.shape
    levels = h.gauss.shape[1]
    together = 4
    zero = jnp.zeros((CHUNK, atoms), F32)
    for k0 in range(0, levels, together):

        def one(c, acc):
            here = pl.ds(pl.multiple_of(c * CHUNK, CHUNK), CHUNK)
            slope = h.mix[0, here, :]
            r = [h.mix[1 + a, here, :] for a in range(4)]
            dr = [h.mix[5 + a, here, :] for a in range(4)]
            out = []
            for k in range(together):
                phi = h.gauss[0, k0 + k, here, :]
                psi = h.gauss[1, k0 + k, here, :] * slope
                out += [acc[8 * k + a] + phi * r[a] for a in range(4)]
                out += [acc[8 * k + 4 + a] + (phi * dr[a] + psi * r[a]) for a in range(4)]
            return tuple(out)

        acc = lax.fori_loop(0, width // CHUNK, one, (zero,) * (8 * together), unroll=2)
        for k in range(together):
            for a in range(8):
                h.pooled[a, k0 + k : k0 + k + 1, :] = jnp.sum(acc[8 * k + a], axis=0, keepdims=True) / width


def of_kind(kinds, rows):
    types = len(kinds)
    step = rows.shape[0] // types
    out = rows[:step]
    for t in range(1, types):
        out = jnp.where(kinds[t], rows[t * step : (t + 1) * step], out)
    return out


def lanes_of(x, count, atoms):
    return [x[:, a * atoms : (a + 1) * atoms] for a in range(count)]


def fitting_net(h, kinds_ref, types):
    fit = h.columns.shape[0]
    fit_wide = h.w2_left.shape[1] // 3
    levels = h.pooled.shape[1]
    m2 = h.lead_up.shape[0] // types
    width, atoms = h.idt.shape
    kinds2 = jnp.concatenate([kinds_ref[...]] * 2, axis=1)
    kinds8 = jnp.concatenate([kinds2] * 4, axis=1)
    kinds2 = [kinds2 == t for t in range(types)]
    kinds8 = [kinds8 == t for t in range(types)]
    pooled = jnp.concatenate([h.pooled[a] for a in range(8)], axis=1)
    lead = lanes_of(of_kind(kinds8, matmul(h.lead_up[...], right_parts(pooled))), 8, atoms)
    for k in range(levels):
        rows = [h.pooled[a, k : k + 1, :] for a in range(8)]
        plain = rows[0] * lead[0]
        moved = rows[4] * lead[0] + rows[0] * lead[4]
        for a in range(1, 4):
            plain += rows[a] * lead[a]
            moved += rows[4 + a] * lead[a] + rows[a] * lead[4 + a]
        h.product[k * m2 : (k + 1) * m2, :atoms] = plain
        h.product[k * m2 : (k + 1) * m2, atoms:] = moved
    z1 = of_kind(kinds2, matmul(h.low_right[...], right_parts(h.product[...])))
    b1, b2, fo = h.columns[:, 0:1], h.columns[:, 1:2], h.columns[:, 2:3]
    h1 = jnp.tanh(z1[:, :atoms] + b1)
    gate1 = 1.0 - h1 * h1
    dh1 = gate1 * z1[:, atoms:]
    z2 = matmul(h.w2_right[...], right_parts(padded(jnp.concatenate([h1, dh1], axis=1), fit_wide, 0)))
    t2 = jnp.tanh(z2[:, :atoms] + b2)
    gate2 = 1.0 - t2 * t2
    dt2 = gate2 * z2[:, atoms:]
    gz2 = jnp.concatenate([fo * gate2, fo * (-2.0 * t2 * dt2)], axis=1)
    gh = matmul(h.w2_left[...], right_parts(padded(gz2, fit_wide, 0)))
    gh1 = gh[:, :atoms] + fo
    gz1 = jnp.concatenate([gh1 * gate1, gh[:, atoms:] * gate1 - 2.0 * gh1 * h1 * dh1], axis=1)
    h.pulled[...] = of_kind(kinds2, matmul(h.low_left[...], right_parts(padded(gz1, fit_wide, 0))))
    acc = [jnp.zeros((m2, atoms), F32) for _ in range(8)]
    for k in range(levels):
        g = h.pulled[k * m2 : (k + 1) * m2, :atoms]
        dg = h.pulled[k * m2 : (k + 1) * m2, atoms:]
        rows = [h.pooled[a, k : k + 1, :] for a in range(8)]
        for a in range(4):
            straight = jnp.sum(g * lead[a], axis=0, keepdims=True)
            turned = jnp.sum(dg * lead[a] + g * lead[4 + a], axis=0, keepdims=True)
            h.gp[k : k + 1, a * atoms : (a + 1) * atoms] = straight
            h.gp[k : k + 1, (4 + a) * atoms : (5 + a) * atoms] = turned
            acc[a] = acc[a] + g * rows[a]
            acc[4 + a] = acc[4 + a] + (dg * rows[a] + g * rows[4 + a])
    across = of_kind(kinds8, matmul(h.lead_down[...], right_parts(jnp.concatenate(acc, axis=1))))
    h.gp[...] = (h.gp[...] + across) / width


def pair_forces(h, out_ref):
    width, atoms = h.idt.shape
    levels = h.gauss.shape[1]
    banks = out_ref.shape[1] // 128
    top = float(levels - 1)

    def force_of(c, centre):
        first = pl.multiple_of(c * CHUNK, CHUNK)
        here = pl.ds(first, CHUNK)
        zero = jnp.zeros((CHUNK, atoms), F32)
        s0, s1, s2, e0, e1 = ([zero] * 4 for _ in range(5))
        for k in range(levels):
            phi, psi, chi = (h.gauss[p, k, here, :] for p in range(3))
            for a in range(4):
                g = h.gp[k : k + 1, a * atoms : (a + 1) * atoms]
                gd = h.gp[k : k + 1, (4 + a) * atoms : (5 + a) * atoms]
                s0[a] = s0[a] + g * phi
                s1[a] = s1[a] + g * psi
                s2[a] = s2[a] + g * chi
                e0[a] = e0[a] + gd * phi
                e1[a] = e1[a] + gd * psi
        d = [h.dv[f, here, :] for f in range(3)]
        v = [h.dv[f, here, :] for f in range(3, 6)]
        qd, w, s, u, shrink = (h.radial[at, here, :] for at in range(5))
        s_q = -s * (1.0 + 0.5 * w)
        u_q = -u * (1.0 + w)
        t_s = shrink * shrink
        t_q = t_s * s_q
        s_qq = -s_q * (1.0 + 0.5 * w) + 0.5 * s * w * w
        u_qq = -u_q * (1.0 + w) + u * w * w
        t_qq = -2.0 * t_s * shrink * s_q * s_q + t_s * s_qq
        step = t_q * qd
        val = s0
        val_t = [-2.0 * top * e for e in s1]
        val_tt = [top * top * (4.0 * s2[a] - 2.0 * s0[a]) for a in range(4)]
        dval = [e0[a] + val_t[a] * step for a in range(4)]
        dval_t = [-2.0 * top * e1[a] + val_tt[a] * step for a in range(4)]
        big = val[1] * d[0] + val[2] * d[1] + val[3] * d[2]
        big_t = val_t[1] * d[0] + val_t[2] * d[1] + val_t[3] * d[2]
        dbig = sum(dval[1 + e] * d[e] + val[1 + e] * v[e] for e in range(3))
        dbig_t = sum(dval_t[1 + e] * d[e] + val_t[1 + e] * v[e] for e in range(3))
        flow = val_t[0] * s + big_t * u
        kern = t_q * flow + val[0] * s_q + big * u_q
        dkern = (
            t_q * (dval_t[0] * s + dbig_t * u)
            + dval[0] * s_q
            + dbig * u_q
            + qd * (t_qq * flow + t_q * (val_t[0] * s_q + big_t * u_q) + val[0] * s_qq + big * u_qq)
        )
        du = u_q * qd
        out = []
        for e in range(3):
            force = 2.0 * (v[e] * kern + d[e] * dkern) + du * val[1 + e] + u * dval[1 + e]
            high = force.astype(BF16).astype(F32)
            h.forces[pl.ds(first * 8 + e, CHUNK, stride=8), :] = high
            h.forces[pl.ds(first * 8 + 3 + e, CHUNK, stride=8), :] = force - high
            out.append(centre[e] - force)
        return tuple(out)

    zero = jnp.zeros((CHUNK, atoms), F32)
    centre = lax.fori_loop(0, width // CHUNK, force_of, (zero,) * 3)

    together = width // 2

    def scatter(c, acc):
        lefts = []
        for r in range(together):
            n = c * together + r
            part = h.forces[pl.ds(pl.multiple_of(n * 8, 8), 8), :]
            lefts.append(
                jnp.concatenate([part * h.in_bank[b, pl.ds(n, 1), :] for b in range(banks)], axis=0).astype(BF16)
            )
        first = pl.multiple_of(c * together * atoms, together * atoms)
        return acc + matmul(jnp.concatenate(lefts, axis=1), h.onehot[pl.ds(first, together * atoms), :])

    acc = lax.fori_loop(0, width // together, scatter, jnp.zeros((8 * banks, 128), F32))
    for b in range(banks):
        part = acc[8 * b : 8 * b + 8]
        out_ref[:, b * 128 : (b + 1) * 128] = part + jnp.concatenate([part[3:], part[:3]], axis=0)
    for e in range(3):
        out_ref[e : e + 1, :atoms] += jnp.sum(centre[e], axis=0, keepdims=True)


def hessian_product(h, ext_ref, counts_ref, kinds_ref, out_ref, types):
    pair_terms(h, ext_ref, counts_ref[...])
    pooled_terms(h)
    fitting_net(h, kinds_ref, types)
    pair_forces(h, out_ref)


class Scratch:
    def __init__(self, names, refs):
        for name, ref in zip(names, refs, strict=True):
            setattr(self, name, ref)


AXES = ("gx", "gy", "gz")
MESH = pl.DeviceIdType.MESH
GROUP_LIMIT = 32


def sizes_of():
    return [lax.axis_size(axis) for axis in AXES]


def plane_offsets():
    def along(size):
        return (0, 1) if size == 2 else (0, 1, -1)

    _, ny, nz = sizes_of()
    return [(dy, dz) for dz in along(nz) for dy in along(ny)]


def device_at(shift):
    return {
        axis: lax.rem(lax.axis_index(axis) + (step + peers) % peers, peers)
        for axis, step, peers in zip(AXES, shift, sizes_of())
    }


def reduction_groups():
    sizes = sizes_of()
    groups = []
    for at in range(3):
        if groups and groups[-1][1] * sizes[at] <= GROUP_LIMIT:
            groups[-1] = (groups[-1][0] + [at], groups[-1][1] * sizes[at])
        else:
            groups.append(([at], sizes[at]))
    out = []
    for members, count in groups:
        shifts = [[0, 0, 0]]
        for at in members:
            shifts = [s[:at] + [step] + s[at + 1 :] for s in shifts for step in range(sizes[at])]
        out.append((members, count, [tuple(s) for s in shifts if any(s)]))
    return out


def place_in(members):
    sizes = sizes_of()
    me = 0
    for at in members:
        me = me * sizes[at] + lax.axis_index(AXES[at])
    return me


def three_parts(x):
    high = x.astype(BF16)
    rest = x - high.astype(F32)
    middle = rest.astype(BF16)
    low = (rest - middle.astype(F32)).astype(BF16)
    return jnp.concatenate([high.astype(F32), middle.astype(F32), low.astype(F32)], axis=0).astype(BF16)


def select_dot(x, onehot, dims):
    n = x.shape[0]
    out = lax.dot_general(three_parts(x), onehot, (dims, ((), ())), preferred_element_type=F32)
    return (out[:n] + out[n : 2 * n]) + out[2 * n :]


def chosen_columns(map_row, columns):
    rows = lax.broadcasted_iota(jnp.int32, (columns, map_row.shape[1]), 0).astype(F32)
    return jnp.where(rows == map_row, 1.0, 0.0).astype(BF16)


def sides(parts, early):
    if -1 in parts:
        return jnp.where(early, parts[-1], parts[1])
    return parts[1]


def one_side(x, step, distinct, early):
    if not distinct:
        return x
    return jnp.where(early, x, 0.0) if step == -1 else jnp.where(early, 0.0, x)


class Sender:
    def __init__(self, send_sem, recv_sem):
        self.send_sem, self.recv_sem, self.used, self.started = send_sem, recv_sem, 0, []

    def send(self, source, target, shift):
        copy = pltpu.make_async_remote_copy(
            src_ref=source,
            dst_ref=target,
            send_sem=self.send_sem.at[self.used],
            recv_sem=self.recv_sem.at[self.used],
            device_id=device_at(shift),
            device_id_type=MESH,
        )
        copy.start()
        self.used += 1
        self.started.append(copy)
        return copy


def lanczos_kernel(*refs, inputs, copies, names):
    hbm, (next_ref, corr_ref, norm_ref) = refs[:inputs], refs[inputs : inputs + 3]
    local = refs[inputs + 3 : 2 * inputs + 3]
    (load_sem, send_sem, recv_sem, ext, work, mine, face, raw_land, low_land, up_land, back_raw, back_face,
     raw_back, low_back, up_back, stack, gram_tile, gram_land, row_tile, row_land, *hvp_scratch) = refs[2 * inputs + 3 :]
    places, basis, ids, counts, kinds, map_x, map_y, map_z, table, w1, w2, b1, b2, fo = local
    h = Scratch(names, hvp_scratch)
    types = table.shape[0]
    atoms = places.shape[2]
    stored = basis.shape[0]
    rows = stack.shape[0]
    pair = 2 * map_x.shape[1]
    sizes = sizes_of()
    entries = 3 * atoms * sizes[0] * sizes[1] * sizes[2]
    planes = plane_offsets()
    groups = reduction_groups()
    faces = ((1, low_land, up_back), (-1, up_land, low_back))

    partners = set()
    for dy, dz in planes:
        for dx in (-1, 0, 1):
            partners.add(tuple(step % peers for step, peers in zip((dx, dy, dz), sizes)))
    for _, _, shifts in groups:
        partners.update(shifts)
    partners = sorted(partners - {(0, 0, 0)})
    opposite = {tuple(-step % peers for step, peers in zip(shift, sizes)) for shift in partners}
    assert opposite == set(partners)
    barrier = pltpu.get_barrier_semaphore()
    for shift in partners:
        pl.semaphore_signal(barrier, inc=1, device_id=device_at(shift), device_id_type=MESH)
    loads = [pltpu.make_async_copy(a, b, load_sem.at[at]) for at, (a, b) in enumerate(zip(hbm, local))]
    for at in (0, 1, 5, 6, 7, 2, 3, 4, 8, 9, 10, 11, 12, 13):
        loads[at].start()
    early = lax.broadcasted_iota(jnp.int32, (8, pair), 1) < pair // 2
    line = lax.broadcasted_iota(jnp.int32, (8, pair), 0)
    for at in (0, 1, 5, 6, 7):
        loads[at].wait()
    for c in range(3):
        mine[c : c + 1, :] = places[c]
        mine[3 + c : 4 + c, :] = basis[stored - 1, c]
    map_rows = [jnp.concatenate([m[1:2, :], m[0:1, :]], axis=1).astype(F32) for m in (map_x, map_y, map_z)]
    mine[6:7, :] = map_rows[1]
    mine[7:8, :] = map_rows[2]
    pick_x = chosen_columns(map_rows[0], atoms)
    face[...] = select_dot(mine[...], pick_x, ((1,), (0,)))
    pl.semaphore_wait(barrier, len(partners))

    sender = Sender(send_sem, recv_sem)
    arriving = []
    for at, (dy, dz) in reversed(list(enumerate(planes))):
        for dx, land, _ in faces:
            arriving.append(sender.send(face, land.at[at], (dx, -dy, -dz)))
        if at:
            arriving.append(sender.send(mine, raw_land.at[at], (0, -dy, -dz)))

    stack[rows - 8 :, :] = jnp.zeros((8, 3 * atoms), F32)
    for k in range(stored):
        for c in range(3):
            stack[k : k + 1, c * atoms : (c + 1) * atoms] = basis[k, c]
    gram = dot_full(stack[...], stack[...], ((1,), (1,)))
    gram_tile[...] = jnp.concatenate([gram[r : r + 8] for r in range(0, rows, 8)], axis=1)
    for at in (2, 3, 4, 8, 9, 10, 11, 12, 13):
        loads[at].wait()
    prepare_scatter(h, ids)
    prepare_matrices(h, table, w1, w2, b1, b2, fo)
    for copy in arriving:
        copy.wait_recv()

    def shifted(x, row):
        return x + jnp.where(line == row, jnp.where(early, -1.0, 1.0), 0.0)

    raw = {plane: mine[...] if at == 0 else raw_land[at] for at, plane in enumerate(planes)}
    wide = {
        plane: jnp.concatenate([raw[plane], shifted(jnp.where(early, low_land[at], up_land[at]), 0)], axis=1)
        for at, plane in enumerate(planes)
    }
    pick_y, pick_z, wider = {}, {}, {}
    for dz in sorted({dz for _, dz in planes}):
        got = {}
        for dy in (1, -1):
            if (dy, dz) in raw:
                pick_y[dy, dz] = chosen_columns(raw[dy, dz][6:7, :], atoms + pair)
                got[dy] = select_dot(wide[dy, dz], pick_y[dy, dz], ((1,), (0,)))
        wider[dz] = jnp.concatenate([wide[0, dz], shifted(sides(got, early), 1)], axis=1)
    got = {}
    for dz in (1, -1):
        if dz in wider:
            pick_z[dz] = chosen_columns(raw[0, dz][7:8, :], atoms + 2 * pair)
            got[dz] = select_dot(wider[dz], pick_z[dz], ((1,), (0,)))
    ext[:, : atoms + 2 * pair] = wider[0]
    ext[:, atoms + 2 * pair :] = shifted(sides(got, early), 2)

    started = []
    members, _, shifts = groups[0]
    me = place_in(members)
    gram_land[me] = gram_tile[...]
    for shift in shifts:
        started.append(sender.send(gram_land.at[me], gram_land.at[me], shift))

    hessian_product(h, ext, counts, kinds, work, types)

    many_y, many_z = -1 in {dy for dy, _ in planes}, -1 in wider
    back = {0: work[:, : atoms + 2 * pair]}
    for dz in pick_z:
        part = one_side(work[:, atoms + 2 * pair :], dz, many_z, early)
        back[dz] = select_dot(part, pick_z[dz], ((1,), (1,)))
    terms = {(0, dz): x[:, : atoms + pair] for dz, x in back.items()}
    for dy, dz in pick_y:
        part = one_side(back[dz][:, atoms + pair :], dy, many_y, early)
        terms[dy, dz] = select_dot(part, pick_y[dy, dz], ((1,), (1,)))
    arriving = []
    for at, (dy, dz) in reversed(list(enumerate(planes))):
        back_raw[at] = terms[dy, dz][:, :atoms]
        back_face[at] = terms[dy, dz][:, atoms:]
        for dx, _, land in faces:
            arriving.append(sender.send(back_face.at[at], land.at[at], (-dx, dy, dz)))
        if at:
            arriving.append(sender.send(back_raw.at[at], raw_back.at[at], (0, dy, dz)))

    for copy in started:
        copy.wait_recv()
    total = gram_land[0]
    for other in range(1, groups[0][1]):
        total = total + gram_land[other]
    base = groups[0][1]
    for members, count, shifts in groups[1:]:
        me = base + place_in(members)
        gram_land[me] = total
        started = [sender.send(gram_land.at[me], gram_land.at[me], shift) for shift in shifts]
        for copy in started:
            copy.wait_recv()
        total = gram_land[base]
        for other in range(1, count):
            total = total + gram_land[base + other]
        base += count
    gram = jnp.concatenate([total[:, r : r + rows] for r in range(0, rows * rows // 8, rows)], axis=0) / entries

    for copy in arriving:
        copy.wait_recv()
    own = back_raw[0]
    low, up = low_back[0], up_back[0]
    for at in range(1, len(planes)):
        own = own + raw_back[at]
        low = low + low_back[at]
        up = up + up_back[at]
    own = own + select_dot(jnp.where(early, up, low), pick_x, ((1,), (1,)))
    hv = jnp.concatenate([own[c : c + 1, :] for c in range(3)], axis=1)
    stack[stored : stored + 1, :] = hv
    sums = dot_full(jnp.broadcast_to(hv, (8, 3 * atoms)), stack[...], ((1,), (1,)))
    sums = jnp.concatenate([sums[0:1], jnp.zeros((1, row_tile.shape[1] - rows), F32)], axis=1)
    base = 0
    for members, count, shifts in groups:
        me = base + place_in(members)
        row_land[me] = sums
        started = [sender.send(row_land.at[me], row_land.at[me], shift) for shift in shifts]
        for copy in started:
            copy.wait_recv()
        sums = row_land[base]
        for other in range(1, count):
            sums = sums + row_land[base + other]
        base += count
    for copy in sender.started:
        copy.wait_send()
    assert sender.used == copies
    lane = lax.broadcasted_iota(jnp.int32, (1, rows), 1)
    sums = sums[:, :rows] / entries
    kept = jnp.where(lane < stored, sums, 0.0)
    both = jnp.concatenate([gram, stack[...]], axis=1)
    mixed = dot_full(jnp.broadcast_to(kept, (8, rows)), both, ((1,), (0,)))[0:1]
    plain = sums[:, stored : stored + 1]
    cross = jnp.sum(mixed[:, :rows] * kept - 2.0 * kept * kept, axis=1, keepdims=True)
    norm = jnp.sqrt(plain + cross + 1e-06)
    norm_ref[...] = norm
    corr_ref[...] = sums[:, :stored]
    for c in range(3):
        part = slice(c * atoms, (c + 1) * atoms)
        next_ref[c] = (hv[:, part] - mixed[:, rows:][:, part]) / norm


def on_device(positions, basis, neighbours, used_count, kinds, map_x, map_y, map_z,
              table, fit_w1, fit_b1, fit_w2, fit_b2, fit_out):
    atoms = positions.shape[-1]
    width = neighbours.shape[-1]
    stored = basis.shape[0]
    types, levels, m1 = table.shape
    m2 = fit_w1.shape[0] // m1
    pair = 2 * map_x.shape[-1]
    ext = atoms + 3 * pair
    args = [
        positions.reshape(3, 1, atoms),
        basis.reshape(stored, 3, 1, atoms),
        neighbours.reshape(atoms, width),
        used_count.reshape(1, atoms),
        kinds.reshape(1, atoms),
        map_x.reshape(2, -1),
        map_y.reshape(2, -1),
        map_z.reshape(2, -1),
        table,
        fit_w1.T,
        fit_w2,
        fit_b1[None],
        fit_b2[None],
        fit_out[None],
    ]
    rows = (stored + 8) // 8 * 8
    planes = len(plane_offsets())
    groups = reduction_groups()
    slots = sum(count for _, count, _ in groups)
    copies = 2 * (3 * planes - 1) + 2 * sum(len(shifts) for _, _, shifts in groups)
    hvp = hvp_shapes(atoms, width, types, levels, m1, m2, fit_w2.shape[0], ext // 128)
    any_space = pl.BlockSpec(memory_space=pl.ANY)
    vmem = pl.BlockSpec(memory_space=pltpu.VMEM)
    tile = pltpu.VMEM((planes, 8, pair), F32)
    next_vector, correlations, norm = pl.pallas_call(
        functools.partial(lanczos_kernel, inputs=len(args), copies=copies, names=tuple(hvp)),
        out_shape=(
            jax.ShapeDtypeStruct((3, 1, atoms), F32),
            jax.ShapeDtypeStruct((1, stored), F32),
            jax.ShapeDtypeStruct((1, 1), F32),
        ),
        in_specs=[any_space] * len(args),
        out_specs=(vmem,) * 3,
        scratch_shapes=[pltpu.VMEM(x.shape, x.dtype) for x in args] + [
            pltpu.SemaphoreType.DMA((len(args),)),
            pltpu.SemaphoreType.DMA((copies,)),
            pltpu.SemaphoreType.DMA((copies,)),
            pltpu.VMEM((8, ext), F32),
            pltpu.VMEM((8, ext), F32),
            pltpu.VMEM((8, pair), F32),
            pltpu.VMEM((8, pair), F32),
            tile, tile, tile, tile, tile, tile, tile, tile,
            pltpu.VMEM((rows, 3 * atoms), F32),
            pltpu.VMEM((8, rows * rows // 8), F32),
            pltpu.VMEM((slots, 8, rows * rows // 8), F32),
            pltpu.VMEM((1, 128), F32),
            pltpu.VMEM((slots, 1, 128), F32),
        ] + [pltpu.VMEM(shape, dtype) for shape, dtype in hvp.values()],
        compiler_params=pltpu.CompilerParams(
            collective_id=0, has_side_effects=True, vmem_limit_bytes=60 << 20
        ),
        name="lanczos",
    )(*args)
    return next_vector.reshape(positions.shape), correlations.reshape(stored), norm.reshape(())


def solution(mesh):
    placed = (
        P(None, "gx", "gy", "gz", None),
        P(None, None, "gx", "gy", "gz", None),
        P("gx", "gy", "gz", None, None),
        P("gx", "gy", "gz", None),
        P("gx", "gy", "gz", None),
        P("gx", "gy", "gz", None, None),
        P("gx", "gy", "gz", None, None),
        P("gx", "gy", "gz", None, None),
        P(),
        P(),
        P(),
        P(),
        P(),
        P(),
    )
    return jax.shard_map(
        on_device,
        mesh=mesh,
        in_specs=placed,
        out_specs=(P(None, "gx", "gy", "gz", None), P(), P()),
        check_vma=False,
    )
```

```python
import functools

import jax
import jax.numpy as jnp
from jax import lax
from jax.experimental import pallas as pl
from jax.experimental.pallas import tpu as pltpu
from jax.sharding import PartitionSpec as P

F32, BF16 = jnp.float32, jnp.bfloat16
HIGHEST = lax.Precision.HIGHEST
CHUNK = 8
DIGIT = 64


def split(x):
    high = x.astype(BF16)
    return high, (x - high.astype(F32)).astype(BF16)


def left_parts(x):
    high, low = split(x)
    return jnp.concatenate([high, low, high], axis=1)


def right_parts(x):
    high, low = split(x)
    return jnp.concatenate([high, high, low], axis=0)


def matmul(a, b):
    return lax.dot_general(a, b, (((1,), (0,)), ((), ())), preferred_element_type=F32)


def dot_full(a, b, dims):
    return lax.dot_general(a, b, (dims, ((), ())), precision=HIGHEST, preferred_element_type=F32)


def padded(x, rows, columns):
    if columns > x.shape[1]:
        x = jnp.concatenate([x, jnp.zeros((x.shape[0], columns - x.shape[1]), x.dtype)], axis=1)
    if rows > x.shape[0]:
        x = jnp.concatenate([x, jnp.zeros((rows - x.shape[0], x.shape[1]), x.dtype)], axis=0)
    return x


def up_to(n, step):
    return (n + step - 1) // step * step


def hvp_shapes(atoms, width, types, levels, m1, m2, fit, ext):
    fit_wide, m1_wide = up_to(fit, 128), up_to(m1, 128)
    low = levels * m2
    return dict(
        idt=((width, atoms), jnp.int32),
        onehot=((width // CHUNK, DIGIT, CHUNK * atoms), BF16),
        in_bank=((ext // DIGIT, width, atoms), F32),
        w1_rows=((fit_wide // 128, m1_wide * m2, 128), F32),
        w1_low=((fit_wide // 128, types * low, 128), F32),
        low_right=((types * fit, 3 * low), BF16),
        low_left=((types * low, 3 * fit_wide), BF16),
        w2_right=((fit, 3 * fit_wide), BF16),
        w2_left=((fit, 3 * fit_wide), BF16),
        columns=((fit, 8), F32),
        lead_up=((types * m2, 3 * levels), BF16),
        lead_down=((types * levels, 3 * m2), BF16),
        dv=((6, width, atoms), F32),
        radial=((5, width, atoms), F32),
        mix=((9, width, atoms), F32),
        gauss=((3, levels, width, atoms), F32),
        pooled=((8, levels, atoms), F32),
        product=((low, 2 * atoms), F32),
        pulled=((low, 2 * atoms), F32),
        gp=((levels, 8 * atoms), F32),
        forces=((width * 8, atoms), F32),
    )


def prepare_matrices(h, table_ref, w1_ref, w2_ref, b1_ref, b2_ref, fo_ref):
    types, levels, m1 = table_ref.shape
    fit, m2 = w1_ref.shape[0], w1_ref.shape[1] // m1
    halves, rows, _ = h.w1_rows.shape
    m1_wide, low = rows // m2, levels * m2
    turned = padded(w1_ref[...], halves * 128, 0).T
    tables = jnp.concatenate([padded(table_ref[t], 0, m1_wide) for t in range(types)], axis=0)
    tables = left_parts(tables)
    for half in range(halves):
        h.w1_rows[half, : m1 * m2, :] = turned[:, half * 128 : (half + 1) * 128]
        h.w1_rows[half, m1 * m2 :, :] = jnp.zeros((rows - m1 * m2, 128), F32)
    for n in range(m2):
        part = [h.w1_rows[half, pl.ds(n, m1_wide, stride=m2), :] for half in range(halves)]
        out = matmul(tables, right_parts(jnp.concatenate(part, axis=1)))
        for half in range(halves):
            h.w1_low[half, pl.ds(n, types * levels, stride=m2), :] = out[:, half * 128 : (half + 1) * 128]
    for t in range(types):
        at = slice(t * low, (t + 1) * low)
        mine = jnp.concatenate([h.w1_low[half, at, :] for half in range(halves)], axis=1)
        h.low_left[at, :] = left_parts(mine)
        h.low_right[t * fit : (t + 1) * fit, :] = left_parts(mine.T[:fit])
    w2 = padded(w2_ref[...], halves * 128, halves * 128)
    h.w2_left[...] = left_parts(w2[:fit])
    h.w2_right[...] = left_parts(w2.T[:fit])
    lines = jnp.concatenate([b1_ref[...], b2_ref[...], fo_ref[...], jnp.zeros((5, fit), F32)], axis=0)
    h.columns[...] = dot_full(lines, identity(8), ((0,), (0,)))
    for t in range(types):
        first = table_ref[t][:, :m2]
        h.lead_down[t * levels : (t + 1) * levels, :] = left_parts(first)
        h.lead_up[t * m2 : (t + 1) * m2, :] = left_parts(dot_full(first, identity(levels), ((0,), (0,))))
    h.forces[...] = jnp.zeros_like(h.forces)


def identity(n):
    same = lax.broadcasted_iota(jnp.int32, (n, n), 0) == lax.broadcasted_iota(jnp.int32, (n, n), 1)
    return jnp.where(same, 1.0, 0.0).astype(F32)


def prepare_scatter(h, ids_ref):
    width, atoms = h.idt.shape
    h.idt[...] = ids_ref[...].T
    bank = jnp.right_shift(h.idt[...], DIGIT.bit_length() - 1)
    for b in range(h.in_bank.shape[0]):
        h.in_bank[b] = jnp.where(bank == b, 1.0, 0.0).astype(F32)
    column = lax.broadcasted_iota(jnp.int32, (DIGIT, atoms), 0)

    def one(c, carry):
        digit = jnp.bitwise_and(h.idt[pl.ds(pl.multiple_of(c * CHUNK, CHUNK), CHUNK), :], DIGIT - 1)
        for r in range(CHUNK):
            hit = jnp.where(digit[r : r + 1, :] == column, 1.0, 0.0)
            h.onehot[c, :, r * atoms : (r + 1) * atoms] = hit.astype(BF16)
        return carry

    lax.fori_loop(0, width // CHUNK, one, 0)


def pair_terms(h, ext_ref, counts):
    width, atoms = h.idt.shape
    levels = h.gauss.shape[1]
    banks = ext_ref.shape[1] // 128
    top = float(levels - 1)

    def one(c, carry):
        first = pl.multiple_of(c * CHUNK, CHUNK)
        here = pl.ds(first, CHUNK)
        idx = h.idt[here, :]
        lane = jnp.bitwise_and(idx, 127)
        bank = jnp.right_shift(idx, 7)
        fields = []
        for f in range(6):
            got = None
            for b in range(banks):
                row = jnp.broadcast_to(ext_ref[f : f + 1, b * 128 : (b + 1) * 128], (CHUNK, 128))
                part = jnp.take_along_axis(row, lane, axis=1, mode="promise_in_bounds")
                got = part if got is None else jnp.where(bank == b, part, got)
            got = got - ext_ref[f : f + 1, :atoms]
            h.dv[f, here, :] = got
            fields.append(got)
        d, v = fields[:3], fields[3:]
        slot = lax.broadcasted_iota(jnp.int32, (CHUNK, atoms), 0) + first
        q = d[0] * d[0] + d[1] * d[1] + d[2] * d[2]
        qd = 2.0 * (d[0] * v[0] + d[1] * v[1] + d[2] * v[2])
        w = 1.0 / (q + 0.01)
        decay = jnp.where(slot < counts, jnp.exp(-q), 0.0)
        s = decay * jnp.sqrt(w)
        u = decay * w
        s_q = -s * (1.0 + 0.5 * w)
        u_q = -u * (1.0 + w)
        shrink = 1.0 / (1.0 + s)
        for at, value in enumerate((qd, w, s, u, shrink)):
            h.radial[at, here, :] = value
        step = s_q * qd
        for at, value in enumerate(
            [-2.0 * top * shrink * shrink * step]
            + [s] + [u * e for e in d]
            + [step] + [u_q * qd * d[e] + u * v[e] for e in range(3)]
        ):
            h.mix[at, here, :] = value
        scaled = s * shrink * top
        for k in range(levels):
            y = scaled - float(k)
            phi = jnp.exp(-(y * y))
            psi = y * phi
            h.gauss[0, k, here, :] = phi
            h.gauss[1, k, here, :] = psi
            h.gauss[2, k, here, :] = y * psi
        return carry

    lax.fori_loop(0, width // CHUNK, one, 0, unroll=2)


def pooled_terms(h):
    width, atoms = h.idt.shape
    levels = h.gauss.shape[1]
    together = 4
    zero = jnp.zeros((CHUNK, atoms), F32)
    for k0 in range(0, levels, together):

        def one(c, acc):
            here = pl.ds(pl.multiple_of(c * CHUNK, CHUNK), CHUNK)
            slope = h.mix[0, here, :]
            r = [h.mix[1 + a, here, :] for a in range(4)]
            dr = [h.mix[5 + a, here, :] for a in range(4)]
            out = []
            for k in range(together):
                phi = h.gauss[0, k0 + k, here, :]
                psi = h.gauss[1, k0 + k, here, :] * slope
                out += [acc[8 * k + a] + phi * r[a] for a in range(4)]
                out += [acc[8 * k + 4 + a] + (phi * dr[a] + psi * r[a]) for a in range(4)]
            return tuple(out)

        acc = lax.fori_loop(0, width // CHUNK, one, (zero,) * (8 * together), unroll=2)
        for k in range(together):
            for a in range(8):
                h.pooled[a, k0 + k : k0 + k + 1, :] = jnp.sum(acc[8 * k + a], axis=0, keepdims=True) / width


def of_kind(kinds, rows):
    types = len(kinds)
    step = rows.shape[0] // types
    out = rows[:step]
    for t in range(1, types):
        out = jnp.where(kinds[t], rows[t * step : (t + 1) * step], out)
    return out


def lanes_of(x, count, atoms):
    return [x[:, a * atoms : (a + 1) * atoms] for a in range(count)]


def fitting_net(h, kinds_ref, types):
    fit = h.columns.shape[0]
    fit_wide = h.w2_left.shape[1] // 3
    levels = h.pooled.shape[1]
    m2 = h.lead_up.shape[0] // types
    width, atoms = h.idt.shape
    kinds2 = jnp.concatenate([kinds_ref[...]] * 2, axis=1)
    kinds8 = jnp.concatenate([kinds2] * 4, axis=1)
    kinds2 = [kinds2 == t for t in range(types)]
    kinds8 = [kinds8 == t for t in range(types)]
    pooled = jnp.concatenate([h.pooled[a] for a in range(8)], axis=1)
    lead = lanes_of(of_kind(kinds8, matmul(h.lead_up[...], right_parts(pooled))), 8, atoms)
    for k in range(levels):
        rows = [h.pooled[a, k : k + 1, :] for a in range(8)]
        plain = rows[0] * lead[0]
        moved = rows[4] * lead[0] + rows[0] * lead[4]
        for a in range(1, 4):
            plain += rows[a] * lead[a]
            moved += rows[4 + a] * lead[a] + rows[a] * lead[4 + a]
        h.product[k * m2 : (k + 1) * m2, :atoms] = plain
        h.product[k * m2 : (k + 1) * m2, atoms:] = moved
    z1 = of_kind(kinds2, matmul(h.low_right[...], right_parts(h.product[...])))
    b1, b2, fo = h.columns[:, 0:1], h.columns[:, 1:2], h.columns[:, 2:3]
    h1 = jnp.tanh(z1[:, :atoms] + b1)
    gate1 = 1.0 - h1 * h1
    dh1 = gate1 * z1[:, atoms:]
    z2 = matmul(h.w2_right[...], right_parts(padded(jnp.concatenate([h1, dh1], axis=1), fit_wide, 0)))
    t2 = jnp.tanh(z2[:, :atoms] + b2)
    gate2 = 1.0 - t2 * t2
    dt2 = gate2 * z2[:, atoms:]
    gz2 = jnp.concatenate([fo * gate2, fo * (-2.0 * t2 * dt2)], axis=1)
    gh = matmul(h.w2_left[...], right_parts(padded(gz2, fit_wide, 0)))
    gh1 = gh[:, :atoms] + fo
    gz1 = jnp.concatenate([gh1 * gate1, gh[:, atoms:] * gate1 - 2.0 * gh1 * h1 * dh1], axis=1)
    h.pulled[...] = of_kind(kinds2, matmul(h.low_left[...], right_parts(padded(gz1, fit_wide, 0))))
    acc = [jnp.zeros((m2, atoms), F32) for _ in range(8)]
    for k in range(levels):
        g = h.pulled[k * m2 : (k + 1) * m2, :atoms]
        dg = h.pulled[k * m2 : (k + 1) * m2, atoms:]
        rows = [h.pooled[a, k : k + 1, :] for a in range(8)]
        for a in range(4):
            straight = jnp.sum(g * lead[a], axis=0, keepdims=True)
            turned = jnp.sum(dg * lead[a] + g * lead[4 + a], axis=0, keepdims=True)
            h.gp[k : k + 1, a * atoms : (a + 1) * atoms] = straight
            h.gp[k : k + 1, (4 + a) * atoms : (5 + a) * atoms] = turned
            acc[a] = acc[a] + g * rows[a]
            acc[4 + a] = acc[4 + a] + (dg * rows[a] + g * rows[4 + a])
    across = of_kind(kinds8, matmul(h.lead_down[...], right_parts(jnp.concatenate(acc, axis=1))))
    h.gp[...] = (h.gp[...] + across) / width


def pair_forces(h, out_ref):
    width, atoms = h.idt.shape
    levels = h.gauss.shape[1]
    banks = h.in_bank.shape[0]
    top = float(levels - 1)

    def force_of(c, centre):
        first = pl.multiple_of(c * CHUNK, CHUNK)
        here = pl.ds(first, CHUNK)
        zero = jnp.zeros((CHUNK, atoms), F32)
        s0, s1, s2, e0, e1 = ([zero] * 4 for _ in range(5))
        for k in range(levels):
            phi, psi, chi = (h.gauss[p, k, here, :] for p in range(3))
            for a in range(4):
                g = h.gp[k : k + 1, a * atoms : (a + 1) * atoms]
                gd = h.gp[k : k + 1, (4 + a) * atoms : (5 + a) * atoms]
                s0[a] = s0[a] + g * phi
                s1[a] = s1[a] + g * psi
                s2[a] = s2[a] + g * chi
                e0[a] = e0[a] + gd * phi
                e1[a] = e1[a] + gd * psi
        d = [h.dv[f, here, :] for f in range(3)]
        v = [h.dv[f, here, :] for f in range(3, 6)]
        qd, w, s, u, shrink = (h.radial[at, here, :] for at in range(5))
        s_q = -s * (1.0 + 0.5 * w)
        u_q = -u * (1.0 + w)
        t_s = shrink * shrink
        t_q = t_s * s_q
        s_qq = -s_q * (1.0 + 0.5 * w) + 0.5 * s * w * w
        u_qq = -u_q * (1.0 + w) + u * w * w
        t_qq = -2.0 * t_s * shrink * s_q * s_q + t_s * s_qq
        step = t_q * qd
        val = s0
        val_t = [-2.0 * top * e for e in s1]
        val_tt = [top * top * (4.0 * s2[a] - 2.0 * s0[a]) for a in range(4)]
        dval = [e0[a] + val_t[a] * step for a in range(4)]
        dval_t = [-2.0 * top * e1[a] + val_tt[a] * step for a in range(4)]
        big = val[1] * d[0] + val[2] * d[1] + val[3] * d[2]
        big_t = val_t[1] * d[0] + val_t[2] * d[1] + val_t[3] * d[2]
        dbig = sum(dval[1 + e] * d[e] + val[1 + e] * v[e] for e in range(3))
        dbig_t = sum(dval_t[1 + e] * d[e] + val_t[1 + e] * v[e] for e in range(3))
        flow = val_t[0] * s + big_t * u
        kern = t_q * flow + val[0] * s_q + big * u_q
        dkern = (
            t_q * (dval_t[0] * s + dbig_t * u)
            + dval[0] * s_q
            + dbig * u_q
            + qd * (t_qq * flow + t_q * (val_t[0] * s_q + big_t * u_q) + val[0] * s_qq + big * u_qq)
        )
        du = u_q * qd
        out = []
        for e in range(3):
            force = 2.0 * (v[e] * kern + d[e] * dkern) + du * val[1 + e] + u * dval[1 + e]
            high = force.astype(BF16).astype(F32)
            h.forces[pl.ds(first * 8 + e, CHUNK, stride=8), :] = high
            h.forces[pl.ds(first * 8 + 3 + e, CHUNK, stride=8), :] = force - high
            out.append(centre[e] - force)
        return tuple(out)

    zero = jnp.zeros((CHUNK, atoms), F32)
    centre = lax.fori_loop(0, width // CHUNK, force_of, (zero,) * 3)

    together = width // 2

    def scatter(c, acc):
        lefts = []
        for r in range(together):
            n = c * together + r
            part = h.forces[pl.ds(pl.multiple_of(n * 8, 8), 8), :]
            lefts.append(
                jnp.concatenate([part * h.in_bank[b, pl.ds(n, 1), :] for b in range(banks)], axis=0).astype(BF16)
            )
        right = jnp.concatenate([h.onehot[c * (together // CHUNK) + j] for j in range(together // CHUNK)], axis=1)
        return acc + lax.dot_general(
            jnp.concatenate(lefts, axis=1), right, (((1,), (1,)), ((), ())), preferred_element_type=F32
        )

    acc = lax.fori_loop(0, width // together, scatter, jnp.zeros((8 * banks, DIGIT), F32))
    per = 128 // DIGIT
    for b in range(0, banks, per):
        part = jnp.concatenate([acc[8 * j : 8 * j + 8] for j in range(b, b + per)], axis=1)
        out_ref[:, b * DIGIT : (b + per) * DIGIT] = part + jnp.concatenate([part[3:], part[:3]], axis=0)
    for e in range(3):
        out_ref[e : e + 1, :atoms] += jnp.sum(centre[e], axis=0, keepdims=True)


def hessian_product(h, ext_ref, counts_ref, kinds_ref, out_ref, types):
    pair_terms(h, ext_ref, counts_ref[...])
    pooled_terms(h)
    fitting_net(h, kinds_ref, types)
    pair_forces(h, out_ref)


class Scratch:
    def __init__(self, names, refs):
        for name, ref in zip(names, refs, strict=True):
            setattr(self, name, ref)


AXES = ("gx", "gy", "gz")
MESH = pl.DeviceIdType.MESH
GROUP_LIMIT = 32


def sizes_of():
    return [lax.axis_size(axis) for axis in AXES]


def plane_offsets():
    def along(size):
        return (0, 1) if size == 2 else (0, 1, -1)

    _, ny, nz = sizes_of()
    return [(dy, dz) for dz in along(nz) for dy in along(ny)]


def device_at(shift):
    return {
        axis: lax.rem(lax.axis_index(axis) + (step + peers) % peers, peers)
        for axis, step, peers in zip(AXES, shift, sizes_of())
    }


def reduction_groups():
    sizes = sizes_of()
    groups = []
    for at in range(3):
        if groups and groups[-1][1] * sizes[at] <= GROUP_LIMIT:
            groups[-1] = (groups[-1][0] + [at], groups[-1][1] * sizes[at])
        else:
            groups.append(([at], sizes[at]))
    out = []
    for members, count in groups:
        shifts = [[0, 0, 0]]
        for at in members:
            shifts = [s[:at] + [step] + s[at + 1 :] for s in shifts for step in range(sizes[at])]
        out.append((members, count, [tuple(s) for s in shifts if any(s)]))
    return out


def place_in(members):
    sizes = sizes_of()
    me = 0
    for at in members:
        me = me * sizes[at] + lax.axis_index(AXES[at])
    return me


def three_parts(x):
    high = x.astype(BF16)
    rest = x - high.astype(F32)
    middle = rest.astype(BF16)
    low = (rest - middle.astype(F32)).astype(BF16)
    return jnp.concatenate([high.astype(F32), middle.astype(F32), low.astype(F32)], axis=0).astype(BF16)


def select_dot(x, onehot, dims):
    n = x.shape[0]
    out = lax.dot_general(three_parts(x), onehot, (dims, ((), ())), preferred_element_type=F32)
    return (out[:n] + out[n : 2 * n]) + out[2 * n :]


def chosen_columns(map_row, columns):
    rows = lax.broadcasted_iota(jnp.int32, (columns, map_row.shape[1]), 0).astype(F32)
    return jnp.where(rows == map_row, 1.0, 0.0).astype(BF16)


def sides(parts, early):
    if -1 in parts:
        return jnp.where(early, parts[-1], parts[1])
    return parts[1]


def one_side(x, step, distinct, early):
    if not distinct:
        return x
    return jnp.where(early, x, 0.0) if step == -1 else jnp.where(early, 0.0, x)


class Sender:
    def __init__(self, send_sem, recv_sem):
        self.send_sem, self.recv_sem, self.used, self.started = send_sem, recv_sem, 0, []

    def send(self, source, target, shift):
        copy = pltpu.make_async_remote_copy(
            src_ref=source,
            dst_ref=target,
            send_sem=self.send_sem.at[self.used],
            recv_sem=self.recv_sem.at[self.used],
            device_id=device_at(shift),
            device_id_type=MESH,
        )
        copy.start()
        self.used += 1
        self.started.append(copy)
        return copy


def lanczos_kernel(*refs, inputs, copies, names):
    hbm, (next_ref, corr_ref, norm_ref) = refs[:inputs], refs[inputs : inputs + 3]
    local = refs[inputs + 3 : 2 * inputs + 3]
    (load_sem, send_sem, recv_sem, ext, work, mine, face, raw_land, low_land, up_land, back_raw, back_face,
     raw_back, low_back, up_back, stack, gram_tile, gram_land, row_tile, row_land, *hvp_scratch) = refs[2 * inputs + 3 :]
    places, basis, ids, counts, kinds, map_x, map_y, map_z, table, w1, w2, b1, b2, fo = local
    h = Scratch(names, hvp_scratch)
    types = table.shape[0]
    atoms = places.shape[2]
    stored = basis.shape[0]
    rows = stack.shape[0]
    pair = 2 * map_x.shape[1]
    sizes = sizes_of()
    entries = 3 * atoms * sizes[0] * sizes[1] * sizes[2]
    planes = plane_offsets()
    groups = reduction_groups()
    faces = ((1, low_land, up_back), (-1, up_land, low_back))

    partners = set()
    for dy, dz in planes:
        for dx in (-1, 0, 1):
            partners.add(tuple(step % peers for step, peers in zip((dx, dy, dz), sizes)))
    for _, _, shifts in groups:
        partners.update(shifts)
    partners = sorted(partners - {(0, 0, 0)})
    opposite = {tuple(-step % peers for step, peers in zip(shift, sizes)) for shift in partners}
    assert opposite == set(partners)
    barrier = pltpu.get_barrier_semaphore()
    for shift in partners:
        pl.semaphore_signal(barrier, inc=1, device_id=device_at(shift), device_id_type=MESH)
    loads = [pltpu.make_async_copy(a, b, load_sem.at[at]) for at, (a, b) in enumerate(zip(hbm, local))]
    for at in (0, 1, 5, 6, 7, 2, 3, 4, 8, 9, 10, 11, 12, 13):
        loads[at].start()
    early = lax.broadcasted_iota(jnp.int32, (8, pair), 1) < pair // 2
    line = lax.broadcasted_iota(jnp.int32, (8, pair), 0)
    for at in (0, 1, 5, 6, 7):
        loads[at].wait()
    for c in range(3):
        mine[c : c + 1, :] = places[c]
        mine[3 + c : 4 + c, :] = basis[stored - 1, c]
    map_rows = [jnp.concatenate([m[1:2, :], m[0:1, :]], axis=1).astype(F32) for m in (map_x, map_y, map_z)]
    mine[6:7, :] = map_rows[1]
    mine[7:8, :] = map_rows[2]
    pick_x = chosen_columns(map_rows[0], atoms)
    face[...] = select_dot(mine[...], pick_x, ((1,), (0,)))
    pl.semaphore_wait(barrier, len(partners))

    sender = Sender(send_sem, recv_sem)
    arriving = []
    for at, (dy, dz) in reversed(list(enumerate(planes))):
        for dx, land, _ in faces:
            arriving.append(sender.send(face, land.at[at], (dx, -dy, -dz)))
        if at:
            arriving.append(sender.send(mine, raw_land.at[at], (0, -dy, -dz)))

    stack[rows - 8 :, :] = jnp.zeros((8, 3 * atoms), F32)
    for k in range(stored):
        for c in range(3):
            stack[k : k + 1, c * atoms : (c + 1) * atoms] = basis[k, c]
    gram = dot_full(stack[...], stack[...], ((1,), (1,)))
    gram_tile[...] = jnp.concatenate([gram[r : r + 8] for r in range(0, rows, 8)], axis=1)
    for at in (2, 3, 4, 8, 9, 10, 11, 12, 13):
        loads[at].wait()
    prepare_scatter(h, ids)
    prepare_matrices(h, table, w1, w2, b1, b2, fo)
    for copy in arriving:
        copy.wait_recv()

    def shifted(x, row):
        return x + jnp.where(line == row, jnp.where(early, -1.0, 1.0), 0.0)

    raw = {plane: mine[...] if at == 0 else raw_land[at] for at, plane in enumerate(planes)}
    wide = {
        plane: jnp.concatenate([raw[plane], shifted(jnp.where(early, low_land[at], up_land[at]), 0)], axis=1)
        for at, plane in enumerate(planes)
    }
    pick_y, pick_z, wider = {}, {}, {}
    for dz in sorted({dz for _, dz in planes}):
        got = {}
        for dy in (1, -1):
            if (dy, dz) in raw:
                pick_y[dy, dz] = chosen_columns(raw[dy, dz][6:7, :], atoms + pair)
                got[dy] = select_dot(wide[dy, dz], pick_y[dy, dz], ((1,), (0,)))
        wider[dz] = jnp.concatenate([wide[0, dz], shifted(sides(got, early), 1)], axis=1)
    got = {}
    for dz in (1, -1):
        if dz in wider:
            pick_z[dz] = chosen_columns(raw[0, dz][7:8, :], atoms + 2 * pair)
            got[dz] = select_dot(wider[dz], pick_z[dz], ((1,), (0,)))
    ext[:, : atoms + 2 * pair] = wider[0]
    ext[:, atoms + 2 * pair :] = shifted(sides(got, early), 2)

    started = []
    members, _, shifts = groups[0]
    me = place_in(members)
    gram_land[me] = gram_tile[...]
    for shift in shifts:
        started.append(sender.send(gram_land.at[me], gram_land.at[me], shift))

    hessian_product(h, ext, counts, kinds, work, types)

    many_y, many_z = -1 in {dy for dy, _ in planes}, -1 in wider
    back = {0: work[:, : atoms + 2 * pair]}
    for dz in pick_z:
        part = one_side(work[:, atoms + 2 * pair :], dz, many_z, early)
        back[dz] = select_dot(part, pick_z[dz], ((1,), (1,)))
    terms = {(0, dz): x[:, : atoms + pair] for dz, x in back.items()}
    for dy, dz in pick_y:
        part = one_side(back[dz][:, atoms + pair :], dy, many_y, early)
        terms[dy, dz] = select_dot(part, pick_y[dy, dz], ((1,), (1,)))
    arriving = []
    for at, (dy, dz) in reversed(list(enumerate(planes))):
        back_raw[at] = terms[dy, dz][:, :atoms]
        back_face[at] = terms[dy, dz][:, atoms:]
        for dx, _, land in faces:
            arriving.append(sender.send(back_face.at[at], land.at[at], (-dx, dy, dz)))
        if at:
            arriving.append(sender.send(back_raw.at[at], raw_back.at[at], (0, dy, dz)))

    for copy in started:
        copy.wait_recv()
    total = gram_land[0]
    for other in range(1, groups[0][1]):
        total = total + gram_land[other]
    base = groups[0][1]
    for members, count, shifts in groups[1:]:
        me = base + place_in(members)
        gram_land[me] = total
        started = [sender.send(gram_land.at[me], gram_land.at[me], shift) for shift in shifts]
        for copy in started:
            copy.wait_recv()
        total = gram_land[base]
        for other in range(1, count):
            total = total + gram_land[base + other]
        base += count
    gram = jnp.concatenate([total[:, r : r + rows] for r in range(0, rows * rows // 8, rows)], axis=0) / entries

    for copy in arriving:
        copy.wait_recv()
    own = back_raw[0]
    low, up = low_back[0], up_back[0]
    for at in range(1, len(planes)):
        own = own + raw_back[at]
        low = low + low_back[at]
        up = up + up_back[at]
    own = own + select_dot(jnp.where(early, up, low), pick_x, ((1,), (1,)))
    hv = jnp.concatenate([own[c : c + 1, :] for c in range(3)], axis=1)
    stack[stored : stored + 1, :] = hv
    sums = dot_full(jnp.broadcast_to(hv, (8, 3 * atoms)), stack[...], ((1,), (1,)))
    sums = jnp.concatenate([sums[0:1], jnp.zeros((1, row_tile.shape[1] - rows), F32)], axis=1)
    base = 0
    for members, count, shifts in groups:
        me = base + place_in(members)
        row_land[me] = sums
        started = [sender.send(row_land.at[me], row_land.at[me], shift) for shift in shifts]
        for copy in started:
            copy.wait_recv()
        sums = row_land[base]
        for other in range(1, count):
            sums = sums + row_land[base + other]
        base += count
    for copy in sender.started:
        copy.wait_send()
    assert sender.used == copies
    lane = lax.broadcasted_iota(jnp.int32, (1, rows), 1)
    sums = sums[:, :rows] / entries
    kept = jnp.where(lane < stored, sums, 0.0)
    both = jnp.concatenate([gram, stack[...]], axis=1)
    mixed = dot_full(jnp.broadcast_to(kept, (8, rows)), both, ((1,), (0,)))[0:1]
    plain = sums[:, stored : stored + 1]
    cross = jnp.sum(mixed[:, :rows] * kept - 2.0 * kept * kept, axis=1, keepdims=True)
    norm = jnp.sqrt(plain + cross + 1e-06)
    norm_ref[...] = norm
    corr_ref[...] = sums[:, :stored]
    for c in range(3):
        part = slice(c * atoms, (c + 1) * atoms)
        next_ref[c] = (hv[:, part] - mixed[:, rows:][:, part]) / norm


def on_device(positions, basis, neighbours, used_count, kinds, map_x, map_y, map_z,
              table, fit_w1, fit_b1, fit_w2, fit_b2, fit_out):
    atoms = positions.shape[-1]
    width = neighbours.shape[-1]
    stored = basis.shape[0]
    types, levels, m1 = table.shape
    m2 = fit_w1.shape[0] // m1
    pair = 2 * map_x.shape[-1]
    ext = atoms + 3 * pair
    args = [
        positions.reshape(3, 1, atoms),
        basis.reshape(stored, 3, 1, atoms),
        neighbours.reshape(atoms, width),
        used_count.reshape(1, atoms),
        kinds.reshape(1, atoms),
        map_x.reshape(2, -1),
        map_y.reshape(2, -1),
        map_z.reshape(2, -1),
        table,
        fit_w1.T,
        fit_w2,
        fit_b1[None],
        fit_b2[None],
        fit_out[None],
    ]
    rows = (stored + 8) // 8 * 8
    planes = len(plane_offsets())
    groups = reduction_groups()
    slots = sum(count for _, count, _ in groups)
    copies = 2 * (3 * planes - 1) + 2 * sum(len(shifts) for _, _, shifts in groups)
    hvp = hvp_shapes(atoms, width, types, levels, m1, m2, fit_w2.shape[0], ext)
    any_space = pl.BlockSpec(memory_space=pl.ANY)
    vmem = pl.BlockSpec(memory_space=pltpu.VMEM)
    tile = pltpu.VMEM((planes, 8, pair), F32)
    next_vector, correlations, norm = pl.pallas_call(
        functools.partial(lanczos_kernel, inputs=len(args), copies=copies, names=tuple(hvp)),
        out_shape=(
            jax.ShapeDtypeStruct((3, 1, atoms), F32),
            jax.ShapeDtypeStruct((1, stored), F32),
            jax.ShapeDtypeStruct((1, 1), F32),
        ),
        in_specs=[any_space] * len(args),
        out_specs=(vmem,) * 3,
        scratch_shapes=[pltpu.VMEM(x.shape, x.dtype) for x in args] + [
            pltpu.SemaphoreType.DMA((len(args),)),
            pltpu.SemaphoreType.DMA((copies,)),
            pltpu.SemaphoreType.DMA((copies,)),
            pltpu.VMEM((8, ext), F32),
            pltpu.VMEM((8, ext), F32),
            pltpu.VMEM((8, pair), F32),
            pltpu.VMEM((8, pair), F32),
            tile, tile, tile, tile, tile, tile, tile, tile,
            pltpu.VMEM((rows, 3 * atoms), F32),
            pltpu.VMEM((8, rows * rows // 8), F32),
            pltpu.VMEM((slots, 8, rows * rows // 8), F32),
            pltpu.VMEM((1, 128), F32),
            pltpu.VMEM((slots, 1, 128), F32),
        ] + [pltpu.VMEM(shape, dtype) for shape, dtype in hvp.values()],
        compiler_params=pltpu.CompilerParams(
            collective_id=0, has_side_effects=True, vmem_limit_bytes=60 << 20
        ),
        name="lanczos",
    )(*args)
    return next_vector.reshape(positions.shape), correlations.reshape(stored), norm.reshape(())


def solution(mesh):
    placed = (
        P(None, "gx", "gy", "gz", None),
        P(None, None, "gx", "gy", "gz", None),
        P("gx", "gy", "gz", None, None),
        P("gx", "gy", "gz", None),
        P("gx", "gy", "gz", None),
        P("gx", "gy", "gz", None, None),
        P("gx", "gy", "gz", None, None),
        P("gx", "gy", "gz", None, None),
        P(),
        P(),
        P(),
        P(),
        P(),
        P(),
    )
    return jax.shard_map(
        on_device,
        mesh=mesh,
        in_specs=placed,
        out_specs=(P(None, "gx", "gy", "gz", None), P(), P()),
        check_vma=False,
    )
```

```python
import functools

import jax
import jax.numpy as jnp
from jax import lax
from jax.experimental import pallas as pl
from jax.experimental.pallas import tpu as pltpu
from jax.sharding import PartitionSpec as P

F32, BF16 = jnp.float32, jnp.bfloat16
HIGHEST = lax.Precision.HIGHEST
CHUNK = 8
DIGIT = 64


def split(x):
    high = x.astype(BF16)
    return high, (x - high.astype(F32)).astype(BF16)


def left_parts(x):
    high, low = split(x)
    return jnp.concatenate([high, low, high], axis=1)


def right_parts(x):
    high, low = split(x)
    return jnp.concatenate([high, high, low], axis=0)


def matmul(a, b):
    return lax.dot_general(a, b, (((1,), (0,)), ((), ())), preferred_element_type=F32)


def dot_full(a, b, dims):
    return lax.dot_general(a, b, (dims, ((), ())), precision=HIGHEST, preferred_element_type=F32)


def padded(x, rows, columns):
    if columns > x.shape[1]:
        x = jnp.concatenate([x, jnp.zeros((x.shape[0], columns - x.shape[1]), x.dtype)], axis=1)
    if rows > x.shape[0]:
        x = jnp.concatenate([x, jnp.zeros((rows - x.shape[0], x.shape[1]), x.dtype)], axis=0)
    return x


def up_to(n, step):
    return (n + step - 1) // step * step


def hvp_shapes(atoms, width, types, levels, m1, m2, fit, ext):
    fit_wide, m1_wide = up_to(fit, 128), up_to(m1, 128)
    low = levels * m2
    return dict(
        idt=((width, atoms), jnp.int32),
        onehot=((width // CHUNK, DIGIT, CHUNK * atoms), BF16),
        in_bank=((ext // DIGIT, width, atoms), F32),
        w1_rows=((fit_wide // 128, m1_wide * m2, 128), F32),
        w1_low=((fit_wide // 128, types * low, 128), F32),
        low_right=((types * fit, 3 * low), BF16),
        low_left=((types * low, 3 * fit_wide), BF16),
        w2_right=((fit, 3 * fit_wide), BF16),
        w2_left=((fit, 3 * fit_wide), BF16),
        columns=((fit, 8), F32),
        lead_up=((types * m2, 3 * levels), BF16),
        lead_down=((types * levels, 3 * m2), BF16),
        dv=((6, width + CHUNK, atoms), F32),
        radial=((5, width + CHUNK, atoms), F32),
        mix=((9, width + CHUNK, atoms), F32),
        gauss=((levels, 3, width + CHUNK, atoms), F32),
        pooled=((8, levels, atoms), F32),
        product=((low, 2 * atoms), F32),
        pulled=((low, 2 * atoms), F32),
        gp=((levels, 8 * atoms), F32),
        forces=((width * 8, atoms), F32),
    )


def prepare_matrices(h, table_ref, w1_ref, w2_ref, b1_ref, b2_ref, fo_ref):
    types, levels, m1 = table_ref.shape
    fit, m2 = w1_ref.shape[0], w1_ref.shape[1] // m1
    halves, rows, _ = h.w1_rows.shape
    m1_wide, low = rows // m2, levels * m2
    turned = padded(w1_ref[...], halves * 128, 0).T
    tables = jnp.concatenate([padded(table_ref[t], 0, m1_wide) for t in range(types)], axis=0)
    tables = left_parts(tables)
    for half in range(halves):
        h.w1_rows[half, : m1 * m2, :] = turned[:, half * 128 : (half + 1) * 128]
        h.w1_rows[half, m1 * m2 :, :] = jnp.zeros((rows - m1 * m2, 128), F32)
    for n in range(m2):
        part = [h.w1_rows[half, pl.ds(n, m1_wide, stride=m2), :] for half in range(halves)]
        out = matmul(tables, right_parts(jnp.concatenate(part, axis=1)))
        for half in range(halves):
            h.w1_low[half, pl.ds(n, types * levels, stride=m2), :] = out[:, half * 128 : (half + 1) * 128]
    for t in range(types):
        at = slice(t * low, (t + 1) * low)
        mine = jnp.concatenate([h.w1_low[half, at, :] for half in range(halves)], axis=1)
        h.low_left[at, :] = left_parts(mine)
        h.low_right[t * fit : (t + 1) * fit, :] = left_parts(mine.T[:fit])
    w2 = padded(w2_ref[...], halves * 128, halves * 128)
    h.w2_left[...] = left_parts(w2[:fit])
    h.w2_right[...] = left_parts(w2.T[:fit])
    lines = jnp.concatenate([b1_ref[...], b2_ref[...], fo_ref[...], jnp.zeros((5, fit), F32)], axis=0)
    h.columns[...] = dot_full(lines, identity(8), ((0,), (0,)))
    for t in range(types):
        first = table_ref[t][:, :m2]
        h.lead_down[t * levels : (t + 1) * levels, :] = left_parts(first)
        h.lead_up[t * m2 : (t + 1) * m2, :] = left_parts(dot_full(first, identity(levels), ((0,), (0,))))
    h.forces[...] = jnp.zeros_like(h.forces)


def identity(n):
    same = lax.broadcasted_iota(jnp.int32, (n, n), 0) == lax.broadcasted_iota(jnp.int32, (n, n), 1)
    return jnp.where(same, 1.0, 0.0).astype(F32)


def prepare_scatter(h, ids_ref):
    width, atoms = h.idt.shape
    h.idt[...] = ids_ref[...].T
    bank = jnp.right_shift(h.idt[...], DIGIT.bit_length() - 1)
    for b in range(h.in_bank.shape[0]):
        h.in_bank[b] = jnp.where(bank == b, 1.0, 0.0).astype(F32)
    column = lax.broadcasted_iota(jnp.int32, (DIGIT, atoms), 0)

    def one(c, carry):
        digit = jnp.bitwise_and(h.idt[pl.ds(pl.multiple_of(c * CHUNK, CHUNK), CHUNK), :], DIGIT - 1)
        for r in range(CHUNK):
            hit = jnp.where(digit[r : r + 1, :] == column, 1.0, 0.0)
            h.onehot[c, :, r * atoms : (r + 1) * atoms] = hit.astype(BF16)
        return carry

    lax.fori_loop(0, width // CHUNK, one, 0)


def pair_terms(h, ext_ref, counts):
    width, atoms = h.idt.shape
    levels = h.gauss.shape[0]
    banks = ext_ref.shape[1] // 128
    top = float(levels - 1)

    def one(c, carry):
        first = pl.multiple_of(c * CHUNK, CHUNK)
        here = pl.ds(first, CHUNK)
        idx = h.idt[here, :]
        lane = jnp.bitwise_and(idx, 127)
        bank = jnp.right_shift(idx, 7)
        fields = []
        for f in range(6):
            got = None
            for b in range(banks):
                row = jnp.broadcast_to(ext_ref[f : f + 1, b * 128 : (b + 1) * 128], (CHUNK, 128))
                part = jnp.take_along_axis(row, lane, axis=1, mode="promise_in_bounds")
                got = part if got is None else jnp.where(bank == b, part, got)
            got = got - ext_ref[f : f + 1, :atoms]
            h.dv[f, here, :] = got
            fields.append(got)
        d, v = fields[:3], fields[3:]
        slot = lax.broadcasted_iota(jnp.int32, (CHUNK, atoms), 0) + first
        q = d[0] * d[0] + d[1] * d[1] + d[2] * d[2]
        qd = 2.0 * (d[0] * v[0] + d[1] * v[1] + d[2] * v[2])
        w = 1.0 / (q + 0.01)
        decay = jnp.where(slot < counts, jnp.exp(-q), 0.0)
        s = decay * jnp.sqrt(w)
        u = decay * w
        s_q = -s * (1.0 + 0.5 * w)
        u_q = -u * (1.0 + w)
        shrink = 1.0 / (1.0 + s)
        for at, value in enumerate((qd, w, s, u, shrink)):
            h.radial[at, here, :] = value
        step = s_q * qd
        for at, value in enumerate(
            [-2.0 * top * shrink * shrink * step]
            + [s] + [u * e for e in d]
            + [step] + [u_q * qd * d[e] + u * v[e] for e in range(3)]
        ):
            h.mix[at, here, :] = value
        scaled = s * shrink * top
        for k in range(levels):
            y = scaled - float(k)
            phi = jnp.exp(-(y * y))
            psi = y * phi
            h.gauss[k, 0, here, :] = phi
            h.gauss[k, 1, here, :] = psi
            h.gauss[k, 2, here, :] = y * psi
        return carry

    lax.fori_loop(0, width // CHUNK, one, 0, unroll=8)


def pooled_terms(h):
    width, atoms = h.idt.shape
    levels = h.gauss.shape[0]
    together = 4
    zero = jnp.zeros((CHUNK, atoms), F32)
    for k0 in range(0, levels, together):

        def one(c, acc):
            here = slice(c * CHUNK, (c + 1) * CHUNK)
            slope = h.mix[0, here, :]
            r = [h.mix[1 + a, here, :] for a in range(4)]
            dr = [h.mix[5 + a, here, :] for a in range(4)]
            out = []
            for k in range(together):
                phi = h.gauss[k0 + k, 0, here, :]
                psi = h.gauss[k0 + k, 1, here, :] * slope
                out += [acc[8 * k + a] + phi * r[a] for a in range(4)]
                out += [acc[8 * k + 4 + a] + (phi * dr[a] + psi * r[a]) for a in range(4)]
            return tuple(out)

        acc = (zero,) * (8 * together)
        for c in range(width // CHUNK):
            acc = one(c, acc)
        for k in range(together):
            for a in range(8):
                h.pooled[a, k0 + k : k0 + k + 1, :] = jnp.sum(acc[8 * k + a], axis=0, keepdims=True) / width


def of_kind(kinds, rows):
    types = len(kinds)
    step = rows.shape[0] // types
    out = rows[:step]
    for t in range(1, types):
        out = jnp.where(kinds[t], rows[t * step : (t + 1) * step], out)
    return out


def lanes_of(x, count, atoms):
    return [x[:, a * atoms : (a + 1) * atoms] for a in range(count)]


def fitting_net(h, kinds_ref, types):
    fit = h.columns.shape[0]
    fit_wide = h.w2_left.shape[1] // 3
    levels = h.pooled.shape[1]
    m2 = h.lead_up.shape[0] // types
    width, atoms = h.idt.shape
    kinds2 = jnp.concatenate([kinds_ref[...]] * 2, axis=1)
    kinds8 = jnp.concatenate([kinds2] * 4, axis=1)
    kinds2 = [kinds2 == t for t in range(types)]
    kinds8 = [kinds8 == t for t in range(types)]
    pooled = jnp.concatenate([h.pooled[a] for a in range(8)], axis=1)
    lead = lanes_of(of_kind(kinds8, matmul(h.lead_up[...], right_parts(pooled))), 8, atoms)
    for k in range(levels):
        rows = [h.pooled[a, k : k + 1, :] for a in range(8)]
        plain = rows[0] * lead[0]
        moved = rows[4] * lead[0] + rows[0] * lead[4]
        for a in range(1, 4):
            plain += rows[a] * lead[a]
            moved += rows[4 + a] * lead[a] + rows[a] * lead[4 + a]
        h.product[k * m2 : (k + 1) * m2, :atoms] = plain
        h.product[k * m2 : (k + 1) * m2, atoms:] = moved
    z1 = of_kind(kinds2, matmul(h.low_right[...], right_parts(h.product[...])))
    b1, b2, fo = h.columns[:, 0:1], h.columns[:, 1:2], h.columns[:, 2:3]
    h1 = jnp.tanh(z1[:, :atoms] + b1)
    gate1 = 1.0 - h1 * h1
    dh1 = gate1 * z1[:, atoms:]
    z2 = matmul(h.w2_right[...], right_parts(padded(jnp.concatenate([h1, dh1], axis=1), fit_wide, 0)))
    t2 = jnp.tanh(z2[:, :atoms] + b2)
    gate2 = 1.0 - t2 * t2
    dt2 = gate2 * z2[:, atoms:]
    gz2 = jnp.concatenate([fo * gate2, fo * (-2.0 * t2 * dt2)], axis=1)
    gh = matmul(h.w2_left[...], right_parts(padded(gz2, fit_wide, 0)))
    gh1 = gh[:, :atoms] + fo
    gz1 = jnp.concatenate([gh1 * gate1, gh[:, atoms:] * gate1 - 2.0 * gh1 * h1 * dh1], axis=1)
    h.pulled[...] = of_kind(kinds2, matmul(h.low_left[...], right_parts(padded(gz1, fit_wide, 0))))
    acc = [jnp.zeros((m2, atoms), F32) for _ in range(8)]
    for k in range(levels):
        g = h.pulled[k * m2 : (k + 1) * m2, :atoms]
        dg = h.pulled[k * m2 : (k + 1) * m2, atoms:]
        rows = [h.pooled[a, k : k + 1, :] for a in range(8)]
        for a in range(4):
            straight = jnp.sum(g * lead[a], axis=0, keepdims=True)
            turned = jnp.sum(dg * lead[a] + g * lead[4 + a], axis=0, keepdims=True)
            h.gp[k : k + 1, a * atoms : (a + 1) * atoms] = straight
            h.gp[k : k + 1, (4 + a) * atoms : (5 + a) * atoms] = turned
            acc[a] = acc[a] + g * rows[a]
            acc[4 + a] = acc[4 + a] + (dg * rows[a] + g * rows[4 + a])
    across = of_kind(kinds8, matmul(h.lead_down[...], right_parts(jnp.concatenate(acc, axis=1))))
    h.gp[...] = (h.gp[...] + across) / width


def pair_forces(h, out_ref):
    width, atoms = h.idt.shape
    levels = h.gauss.shape[0]
    banks = h.in_bank.shape[0]
    top = float(levels - 1)

    def force_of(c, centre):
        first = pl.multiple_of(c * CHUNK, CHUNK)
        here = pl.ds(first, CHUNK)
        zero = jnp.zeros((CHUNK, atoms), F32)
        s0, s1, s2, e0, e1 = ([zero] * 4 for _ in range(5))
        for k in range(levels):
            phi, psi, chi = (h.gauss[k, p, here, :] for p in range(3))
            for a in range(4):
                g = h.gp[k : k + 1, a * atoms : (a + 1) * atoms]
                gd = h.gp[k : k + 1, (4 + a) * atoms : (5 + a) * atoms]
                s0[a] = s0[a] + g * phi
                s1[a] = s1[a] + g * psi
                s2[a] = s2[a] + g * chi
                e0[a] = e0[a] + gd * phi
                e1[a] = e1[a] + gd * psi
        d = [h.dv[f, here, :] for f in range(3)]
        v = [h.dv[f, here, :] for f in range(3, 6)]
        qd, w, s, u, shrink = (h.radial[at, here, :] for at in range(5))
        s_q = -s * (1.0 + 0.5 * w)
        u_q = -u * (1.0 + w)
        t_s = shrink * shrink
        t_q = t_s * s_q
        s_qq = -s_q * (1.0 + 0.5 * w) + 0.5 * s * w * w
        u_qq = -u_q * (1.0 + w) + u * w * w
        t_qq = -2.0 * t_s * shrink * s_q * s_q + t_s * s_qq
        step = t_q * qd
        val = s0
        val_t = [-2.0 * top * e for e in s1]
        val_tt = [top * top * (4.0 * s2[a] - 2.0 * s0[a]) for a in range(4)]
        dval = [e0[a] + val_t[a] * step for a in range(4)]
        dval_t = [-2.0 * top * e1[a] + val_tt[a] * step for a in range(4)]
        big = val[1] * d[0] + val[2] * d[1] + val[3] * d[2]
        big_t = val_t[1] * d[0] + val_t[2] * d[1] + val_t[3] * d[2]
        dbig = sum(dval[1 + e] * d[e] + val[1 + e] * v[e] for e in range(3))
        dbig_t = sum(dval_t[1 + e] * d[e] + val_t[1 + e] * v[e] for e in range(3))
        flow = val_t[0] * s + big_t * u
        kern = t_q * flow + val[0] * s_q + big * u_q
        dkern = (
            t_q * (dval_t[0] * s + dbig_t * u)
            + dval[0] * s_q
            + dbig * u_q
            + qd * (t_qq * flow + t_q * (val_t[0] * s_q + big_t * u_q) + val[0] * s_qq + big * u_qq)
        )
        du = u_q * qd
        out = []
        for e in range(3):
            force = 2.0 * (v[e] * kern + d[e] * dkern) + du * val[1 + e] + u * dval[1 + e]
            high = force.astype(BF16).astype(F32)
            h.forces[pl.ds(first * 8 + e, CHUNK, stride=8), :] = high
            h.forces[pl.ds(first * 8 + 3 + e, CHUNK, stride=8), :] = force - high
            out.append(centre[e] - force)
        return tuple(out)

    zero = jnp.zeros((CHUNK, atoms), F32)
    centre = lax.fori_loop(0, width // CHUNK, force_of, (zero,) * 3)

    together = width // 2

    def scatter(c, acc):
        lefts = []
        for r in range(together):
            n = c * together + r
            part = h.forces[pl.ds(pl.multiple_of(n * 8, 8), 8), :]
            lefts.append(
                jnp.concatenate([part * h.in_bank[b, pl.ds(n, 1), :] for b in range(banks)], axis=0).astype(BF16)
            )
        right = jnp.concatenate([h.onehot[c * (together // CHUNK) + j] for j in range(together // CHUNK)], axis=1)
        return acc + lax.dot_general(
            jnp.concatenate(lefts, axis=1), right, (((1,), (1,)), ((), ())), preferred_element_type=F32
        )

    acc = lax.fori_loop(0, width // together, scatter, jnp.zeros((8 * banks, DIGIT), F32))
    per = 128 // DIGIT
    for b in range(0, banks, per):
        part = jnp.concatenate([acc[8 * j : 8 * j + 8] for j in range(b, b + per)], axis=1)
        out_ref[:, b * DIGIT : (b + per) * DIGIT] = part + jnp.concatenate([part[3:], part[:3]], axis=0)
    for e in range(3):
        out_ref[e : e + 1, :atoms] += jnp.sum(centre[e], axis=0, keepdims=True)


def hessian_product(h, ext_ref, counts_ref, kinds_ref, out_ref, types):
    pair_terms(h, ext_ref, counts_ref[...])
    pooled_terms(h)
    fitting_net(h, kinds_ref, types)
    pair_forces(h, out_ref)


class Scratch:
    def __init__(self, names, refs):
        for name, ref in zip(names, refs, strict=True):
            setattr(self, name, ref)


AXES = ("gx", "gy", "gz")
MESH = pl.DeviceIdType.MESH
GROUP_LIMIT = 32


def sizes_of():
    return [lax.axis_size(axis) for axis in AXES]


def plane_offsets():
    def along(size):
        return (0, 1) if size == 2 else (0, 1, -1)

    _, ny, nz = sizes_of()
    return [(dy, dz) for dz in along(nz) for dy in along(ny)]


def device_at(shift):
    return {
        axis: lax.rem(lax.axis_index(axis) + (step + peers) % peers, peers)
        for axis, step, peers in zip(AXES, shift, sizes_of())
    }


def reduction_groups():
    sizes = sizes_of()
    groups = []
    for at in range(3):
        if groups and groups[-1][1] * sizes[at] <= GROUP_LIMIT:
            groups[-1] = (groups[-1][0] + [at], groups[-1][1] * sizes[at])
        else:
            groups.append(([at], sizes[at]))
    out = []
    for members, count in groups:
        shifts = [[0, 0, 0]]
        for at in members:
            shifts = [s[:at] + [step] + s[at + 1 :] for s in shifts for step in range(sizes[at])]
        out.append((members, count, [tuple(s) for s in shifts if any(s)]))
    return out


def place_in(members):
    sizes = sizes_of()
    me = 0
    for at in members:
        me = me * sizes[at] + lax.axis_index(AXES[at])
    return me


def three_parts(x):
    high = x.astype(BF16)
    rest = x - high.astype(F32)
    middle = rest.astype(BF16)
    low = (rest - middle.astype(F32)).astype(BF16)
    return jnp.concatenate([high.astype(F32), middle.astype(F32), low.astype(F32)], axis=0).astype(BF16)


def select_dot(x, onehot, dims):
    n = x.shape[0]
    out = lax.dot_general(three_parts(x), onehot, (dims, ((), ())), preferred_element_type=F32)
    return (out[:n] + out[n : 2 * n]) + out[2 * n :]


def chosen_columns(map_row, columns):
    rows = lax.broadcasted_iota(jnp.int32, (columns, map_row.shape[1]), 0).astype(F32)
    return jnp.where(rows == map_row, 1.0, 0.0).astype(BF16)


def sides(parts, early):
    if -1 in parts:
        return jnp.where(early, parts[-1], parts[1])
    return parts[1]


def one_side(x, step, distinct, early):
    if not distinct:
        return x
    return jnp.where(early, x, 0.0) if step == -1 else jnp.where(early, 0.0, x)


class Round:
    def __init__(self, sems, at, landed):
        self.sems, self.at, self.landed = sems, at, landed

    def copy(self, source, target, shift):
        return pltpu.make_async_remote_copy(
            src_ref=source,
            dst_ref=target,
            send_sem=self.sems.at[self.at, 0],
            recv_sem=self.sems.at[self.at, 1],
            device_id=device_at(shift),
            device_id_type=MESH,
        )

    def send(self, source, target, shift):
        self.shift = shift
        self.copy(source, target, shift).start()

    def all_of_them(self):
        return self.copy(self.landed, self.landed, self.shift)


def lanczos_kernel(*refs, inputs, names):
    hbm, (next_ref, corr_ref, norm_ref) = refs[:inputs], refs[inputs : inputs + 3]
    local = refs[inputs + 3 : 2 * inputs + 3]
    (load_sem, round_sem, ext, work, mine, face, landed, back_raw, back_face, returned, stack, gram_land, row_land, *hvp_scratch) = refs[2 * inputs + 3 :]
    places, basis, ids, counts, kinds, map_x, map_y, map_z, table, w1, w2, b1, b2, fo = local
    h = Scratch(names, hvp_scratch)
    types = table.shape[0]
    atoms = places.shape[2]
    stored = basis.shape[0]
    rows = stack.shape[0]
    pair = 2 * map_x.shape[1]
    sizes = sizes_of()
    entries = 3 * atoms * sizes[0] * sizes[1] * sizes[2]
    planes = plane_offsets()
    groups = reduction_groups()
    count = len(planes)

    partners = set()
    for dy, dz in planes:
        for dx in (-1, 0, 1):
            partners.add(tuple(step % peers for step, peers in zip((dx, dy, dz), sizes)))
    for _, _, shifts in groups:
        partners.update(shifts)
    partners = sorted(partners - {(0, 0, 0)})
    opposite = {tuple(-step % peers for step, peers in zip(shift, sizes)) for shift in partners}
    assert opposite == set(partners)
    barrier = pltpu.get_barrier_semaphore()
    for shift in partners:
        pl.semaphore_signal(barrier, inc=1, device_id=device_at(shift), device_id_type=MESH)
    loads = [pltpu.make_async_copy(a, b, load_sem.at[at]) for at, (a, b) in enumerate(zip(hbm, local))]
    for at in (0, 1, 5, 6, 7, 2, 3, 4, 8, 9, 10, 11, 12, 13):
        loads[at].start()
    early = lax.broadcasted_iota(jnp.int32, (8, pair), 1) < pair // 2
    line = lax.broadcasted_iota(jnp.int32, (8, pair), 0)
    for at in (0, 1, 5, 6, 7):
        loads[at].wait()
    for c in range(3):
        mine[c : c + 1, :] = places[c]
        mine[3 + c : 4 + c, :] = basis[stored - 1, c]
    map_rows = [jnp.concatenate([m[1:2, :], m[0:1, :]], axis=1).astype(F32) for m in (map_x, map_y, map_z)]
    mine[6:7, :] = map_rows[1]
    mine[7:8, :] = map_rows[2]
    pick_x = chosen_columns(map_rows[0], atoms)
    face[...] = select_dot(mine[...], pick_x, ((1,), (0,)))
    pl.semaphore_wait(barrier, len(partners))

    halo = Round(round_sem, 0, landed)
    for at, (dy, dz) in reversed(list(enumerate(planes))):
        halo.send(face, landed.at[at], (1, -dy, -dz))
        halo.send(face, landed.at[count + at], (-1, -dy, -dz))
        if at:
            halo.send(mine, landed.at[2 * count + at - 1], (0, -dy, -dz))

    stack[rows - 8 :, :] = jnp.zeros((8, 3 * atoms), F32)
    for k in range(stored):
        for c in range(3):
            stack[k : k + 1, c * atoms : (c + 1) * atoms] = basis[k, c]
    gram = dot_full(stack[...], stack[...], ((1,), (1,)))
    gram = jnp.concatenate([gram[r : r + 8] for r in range(0, rows, 8)], axis=1)
    for at in (2, 3, 4, 8, 9, 10, 11, 12, 13):
        loads[at].wait()
    prepare_scatter(h, ids)
    prepare_matrices(h, table, w1, w2, b1, b2, fo)
    halo.all_of_them().wait_recv()

    def shifted(x, row):
        return x + jnp.where(line == row, jnp.where(early, -1.0, 1.0), 0.0)

    raw = {plane: mine[...] if at == 0 else landed[2 * count + at - 1] for at, plane in enumerate(planes)}
    wide = {
        plane: jnp.concatenate([raw[plane], shifted(jnp.where(early, landed[at], landed[count + at]), 0)], axis=1)
        for at, plane in enumerate(planes)
    }
    pick_y, pick_z, wider = {}, {}, {}
    for dz in sorted({dz for _, dz in planes}):
        got = {}
        for dy in (1, -1):
            if (dy, dz) in raw:
                pick_y[dy, dz] = chosen_columns(raw[dy, dz][6:7, :], atoms + pair)
                got[dy] = select_dot(wide[dy, dz], pick_y[dy, dz], ((1,), (0,)))
        wider[dz] = jnp.concatenate([wide[0, dz], shifted(sides(got, early), 1)], axis=1)
    got = {}
    for dz in (1, -1):
        if dz in wider:
            pick_z[dz] = chosen_columns(raw[0, dz][7:8, :], atoms + 2 * pair)
            got[dz] = select_dot(wider[dz], pick_z[dz], ((1,), (0,)))
    ext[:, : atoms + 2 * pair] = wider[0]
    ext[:, atoms + 2 * pair :] = shifted(sides(got, early), 2)

    def gather_from(group, kind, tiles, base, value):
        members, size, shifts = groups[group]
        me = base + place_in(members)
        tiles[me] = value
        around = Round(round_sem, 2 + 2 * group + kind, tiles.at[pl.ds(base, size - 1)])
        for shift in shifts:
            around.send(tiles.at[me], tiles.at[me], shift)
        return around

    def added(tiles, base, size):
        total = tiles[base]
        for other in range(1, size):
            total = total + tiles[base + other]
        return total

    rounds = [halo, gather_from(0, 0, gram_land, 0, gram)]

    hessian_product(h, ext, counts, kinds, work, types)

    many_y, many_z = -1 in {dy for dy, _ in planes}, -1 in wider
    back = {0: work[:, : atoms + 2 * pair]}
    for dz in pick_z:
        part = one_side(work[:, atoms + 2 * pair :], dz, many_z, early)
        back[dz] = select_dot(part, pick_z[dz], ((1,), (1,)))
    terms = {(0, dz): x[:, : atoms + pair] for dz, x in back.items()}
    for dy, dz in pick_y:
        part = one_side(back[dz][:, atoms + pair :], dy, many_y, early)
        terms[dy, dz] = select_dot(part, pick_y[dy, dz], ((1,), (1,)))
    back_round = Round(round_sem, 1, returned)
    for at, (dy, dz) in reversed(list(enumerate(planes))):
        back_raw[at] = terms[dy, dz][:, :atoms]
        back_face[at] = terms[dy, dz][:, atoms:]
        back_round.send(back_face.at[at], returned.at[at], (-1, dy, dz))
        back_round.send(back_face.at[at], returned.at[count + at], (1, dy, dz))
        if at:
            back_round.send(back_raw.at[at], returned.at[2 * count + at - 1], (0, dy, dz))

    rounds[-1].all_of_them().wait_recv()
    total = added(gram_land, 0, groups[0][1])
    base = groups[0][1]
    for group in range(1, len(groups)):
        rounds.append(gather_from(group, 0, gram_land, base, total))
        rounds[-1].all_of_them().wait_recv()
        total = added(gram_land, base, groups[group][1])
        base += groups[group][1]
    rounds.append(back_round)
    gram = jnp.concatenate([total[:, r : r + rows] for r in range(0, rows * rows // 8, rows)], axis=0) / entries

    back_round.all_of_them().wait_recv()
    own, up, low = back_raw[0], returned[0], returned[count]
    for at in range(1, count):
        own = own + returned[2 * count + at - 1]
        up = up + returned[at]
        low = low + returned[count + at]
    own = own + select_dot(jnp.where(early, up, low), pick_x, ((1,), (1,)))
    hv = jnp.concatenate([own[c : c + 1, :] for c in range(3)], axis=1)
    stack[stored : stored + 1, :] = hv
    sums = dot_full(jnp.broadcast_to(hv, (8, 3 * atoms)), stack[...], ((1,), (1,)))
    sums = jnp.concatenate([sums[0:1], jnp.zeros((1, row_land.shape[2] - rows), F32)], axis=1)
    base = 0
    for group in range(len(groups)):
        rounds.append(gather_from(group, 1, row_land, base, sums))
        rounds[-1].all_of_them().wait_recv()
        sums = added(row_land, base, groups[group][1])
        base += groups[group][1]
    for around in rounds:
        around.all_of_them().wait_send()
    lane = lax.broadcasted_iota(jnp.int32, (1, rows), 1)
    sums = sums[:, :rows] / entries
    kept = jnp.where(lane < stored, sums, 0.0)
    both = jnp.concatenate([gram, stack[...]], axis=1)
    mixed = dot_full(jnp.broadcast_to(kept, (8, rows)), both, ((1,), (0,)))[0:1]
    plain = sums[:, stored : stored + 1]
    cross = jnp.sum(mixed[:, :rows] * kept - 2.0 * kept * kept, axis=1, keepdims=True)
    norm = jnp.sqrt(plain + cross + 1e-06)
    norm_ref[...] = norm
    corr_ref[...] = sums[:, :stored]
    for c in range(3):
        part = slice(c * atoms, (c + 1) * atoms)
        next_ref[c] = (hv[:, part] - mixed[:, rows:][:, part]) / norm


def on_device(positions, basis, neighbours, used_count, kinds, map_x, map_y, map_z,
              table, fit_w1, fit_b1, fit_w2, fit_b2, fit_out):
    atoms = positions.shape[-1]
    width = neighbours.shape[-1]
    stored = basis.shape[0]
    types, levels, m1 = table.shape
    m2 = fit_w1.shape[0] // m1
    pair = 2 * map_x.shape[-1]
    ext = atoms + 3 * pair
    args = [
        positions.reshape(3, 1, atoms),
        basis.reshape(stored, 3, 1, atoms),
        neighbours.reshape(atoms, width),
        used_count.reshape(1, atoms),
        kinds.reshape(1, atoms),
        map_x.reshape(2, -1),
        map_y.reshape(2, -1),
        map_z.reshape(2, -1),
        table,
        fit_w1.T,
        fit_w2,
        fit_b1[None],
        fit_b2[None],
        fit_out[None],
    ]
    rows = (stored + 8) // 8 * 8
    planes = len(plane_offsets())
    groups = reduction_groups()
    slots = sum(count for _, count, _ in groups)
    hvp = hvp_shapes(atoms, width, types, levels, m1, m2, fit_w2.shape[0], ext)
    any_space = pl.BlockSpec(memory_space=pl.ANY)
    vmem = pl.BlockSpec(memory_space=pltpu.VMEM)
    tiles = pltpu.VMEM((planes, 8, pair), F32)
    arrivals = pltpu.VMEM((3 * planes - 1, 8, pair), F32)
    next_vector, correlations, norm = pl.pallas_call(
        functools.partial(lanczos_kernel, inputs=len(args), names=tuple(hvp)),
        out_shape=(
            jax.ShapeDtypeStruct((3, 1, atoms), F32),
            jax.ShapeDtypeStruct((1, stored), F32),
            jax.ShapeDtypeStruct((1, 1), F32),
        ),
        in_specs=[any_space] * len(args),
        out_specs=(vmem,) * 3,
        scratch_shapes=[pltpu.VMEM(x.shape, x.dtype) for x in args] + [
            pltpu.SemaphoreType.DMA((len(args),)),
            pltpu.SemaphoreType.DMA((2 + 2 * len(groups), 2)),
            pltpu.VMEM((8, ext), F32),
            pltpu.VMEM((8, ext), F32),
            pltpu.VMEM((8, pair), F32),
            pltpu.VMEM((8, pair), F32),
            arrivals,
            tiles,
            tiles,
            arrivals,
            pltpu.VMEM((rows, 3 * atoms), F32),
            pltpu.VMEM((slots, 8, rows * rows // 8), F32),
            pltpu.VMEM((slots, 1, 128), F32),
        ] + [pltpu.VMEM(shape, dtype) for shape, dtype in hvp.values()],
        compiler_params=pltpu.CompilerParams(
            collective_id=0, has_side_effects=True, vmem_limit_bytes=60 << 20
        ),
        name="lanczos",
    )(*args)
    return next_vector.reshape(positions.shape), correlations.reshape(stored), norm.reshape(())


def solution(mesh):
    placed = (
        P(None, "gx", "gy", "gz", None),
        P(None, None, "gx", "gy", "gz", None),
        P("gx", "gy", "gz", None, None),
        P("gx", "gy", "gz", None),
        P("gx", "gy", "gz", None),
        P("gx", "gy", "gz", None, None),
        P("gx", "gy", "gz", None, None),
        P("gx", "gy", "gz", None, None),
        P(),
        P(),
        P(),
        P(),
        P(),
        P(),
    )
    return jax.shard_map(
        on_device,
        mesh=mesh,
        in_specs=placed,
        out_specs=(P(None, "gx", "gy", "gz", None), P(), P()),
        check_vma=False,
    )
```

```python
import functools

import jax
import jax.numpy as jnp
from jax import lax
from jax.experimental import pallas as pl
from jax.experimental.pallas import tpu as pltpu
from jax.sharding import PartitionSpec as P

F32, BF16 = jnp.float32, jnp.bfloat16
HIGHEST = lax.Precision.HIGHEST
CHUNK = 8
DIGIT = 64


def split(x):
    high = x.astype(BF16)
    return high, (x - high.astype(F32)).astype(BF16)


def left_parts(x):
    high, low = split(x)
    return jnp.concatenate([high, low, high], axis=1)


def right_parts(x):
    high, low = split(x)
    return jnp.concatenate([high, high, low], axis=0)


def matmul(a, b):
    return lax.dot_general(a, b, (((1,), (0,)), ((), ())), preferred_element_type=F32)


def dot_full(a, b, dims):
    return lax.dot_general(a, b, (dims, ((), ())), precision=HIGHEST, preferred_element_type=F32)


def padded(x, rows, columns):
    if columns > x.shape[1]:
        x = jnp.concatenate([x, jnp.zeros((x.shape[0], columns - x.shape[1]), x.dtype)], axis=1)
    if rows > x.shape[0]:
        x = jnp.concatenate([x, jnp.zeros((rows - x.shape[0], x.shape[1]), x.dtype)], axis=0)
    return x


def up_to(n, step):
    return (n + step - 1) // step * step


def hvp_shapes(atoms, width, types, levels, m1, m2, fit, ext):
    fit_wide, m1_wide = up_to(fit, 128), up_to(m1, 128)
    low = levels * m2
    return dict(
        idt=((width, atoms), jnp.int32),
        onehot=((width // CHUNK, DIGIT, CHUNK * atoms), BF16),
        in_bank=((ext // DIGIT, width, atoms), F32),
        w1_rows=((fit_wide // 128, m1_wide * m2, 128), F32),
        w1_low=((fit_wide // 128, types * low, 128), F32),
        low_right=((types * fit, 3 * low), BF16),
        low_left=((types * low, 3 * fit_wide), BF16),
        w2_right=((fit, 3 * fit_wide), BF16),
        w2_left=((fit, 3 * fit_wide), BF16),
        columns=((fit, 8), F32),
        lead_up=((types * m2, 3 * levels), BF16),
        lead_down=((types * levels, 3 * m2), BF16),
        dv=((6, width + CHUNK, atoms), F32),
        radial=((5, width + CHUNK, atoms), F32),
        mix=((9, width + CHUNK, atoms), F32),
        gauss=((levels, 3, width + CHUNK, atoms), F32),
        pooled=((8, levels, atoms), F32),
        product=((low, 2 * atoms), F32),
        pulled=((low, 2 * atoms), F32),
        gp=((levels, 8 * atoms), F32),
        forces=((width * 8, atoms), F32),
    )


def prepare_matrices(h, table_ref, w1_ref, w2_ref, b1_ref, b2_ref, fo_ref):
    types, levels, m1 = table_ref.shape
    fit, m2 = w1_ref.shape[0], w1_ref.shape[1] // m1
    halves, rows, _ = h.w1_rows.shape
    m1_wide, low = rows // m2, levels * m2
    turned = padded(w1_ref[...], halves * 128, 0).T
    tables = jnp.concatenate([padded(table_ref[t], 0, m1_wide) for t in range(types)], axis=0)
    tables = left_parts(tables)
    for half in range(halves):
        h.w1_rows[half, : m1 * m2, :] = turned[:, half * 128 : (half + 1) * 128]
        h.w1_rows[half, m1 * m2 :, :] = jnp.zeros((rows - m1 * m2, 128), F32)
    for n in range(m2):
        part = [h.w1_rows[half, pl.ds(n, m1_wide, stride=m2), :] for half in range(halves)]
        out = matmul(tables, right_parts(jnp.concatenate(part, axis=1)))
        for half in range(halves):
            h.w1_low[half, pl.ds(n, types * levels, stride=m2), :] = out[:, half * 128 : (half + 1) * 128]
    for t in range(types):
        at = slice(t * low, (t + 1) * low)
        mine = jnp.concatenate([h.w1_low[half, at, :] for half in range(halves)], axis=1)
        h.low_left[at, :] = left_parts(mine)
        h.low_right[t * fit : (t + 1) * fit, :] = left_parts(mine.T[:fit])
    w2 = padded(w2_ref[...], halves * 128, halves * 128)
    h.w2_left[...] = left_parts(w2[:fit])
    h.w2_right[...] = left_parts(w2.T[:fit])
    lines = jnp.concatenate([b1_ref[...], b2_ref[...], fo_ref[...], jnp.zeros((5, fit), F32)], axis=0)
    h.columns[...] = dot_full(lines, identity(8), ((0,), (0,)))
    for t in range(types):
        first = table_ref[t][:, :m2]
        h.lead_down[t * levels : (t + 1) * levels, :] = left_parts(first)
        h.lead_up[t * m2 : (t + 1) * m2, :] = left_parts(dot_full(first, identity(levels), ((0,), (0,))))
    h.forces[...] = jnp.zeros_like(h.forces)


def identity(n):
    same = lax.broadcasted_iota(jnp.int32, (n, n), 0) == lax.broadcasted_iota(jnp.int32, (n, n), 1)
    return jnp.where(same, 1.0, 0.0).astype(F32)


def prepare_scatter(h, ids_ref):
    width, atoms = h.idt.shape
    h.idt[...] = ids_ref[...].T
    bank = jnp.right_shift(h.idt[...], DIGIT.bit_length() - 1)
    for b in range(h.in_bank.shape[0]):
        h.in_bank[b] = jnp.where(bank == b, 1.0, 0.0).astype(F32)
    column = lax.broadcasted_iota(jnp.int32, (DIGIT, atoms), 0)

    def one(c, carry):
        digit = jnp.bitwise_and(h.idt[pl.ds(pl.multiple_of(c * CHUNK, CHUNK), CHUNK), :], DIGIT - 1)
        for r in range(CHUNK):
            hit = jnp.where(digit[r : r + 1, :] == column, 1.0, 0.0)
            h.onehot[c, :, r * atoms : (r + 1) * atoms] = hit.astype(BF16)
        return carry

    lax.fori_loop(0, width // CHUNK, one, 0)


def pair_terms(h, ext_ref, counts):
    width, atoms = h.idt.shape
    levels = h.gauss.shape[0]
    banks = ext_ref.shape[1] // 128
    top = float(levels - 1)

    def one(c, carry):
        first = pl.multiple_of(c * CHUNK, CHUNK)
        here = pl.ds(first, CHUNK)
        idx = h.idt[here, :]
        lane = jnp.bitwise_and(idx, 127)
        bank = jnp.right_shift(idx, 7)
        fields = []
        for f in range(6):
            got = None
            for b in range(banks):
                row = jnp.broadcast_to(ext_ref[f : f + 1, b * 128 : (b + 1) * 128], (CHUNK, 128))
                part = jnp.take_along_axis(row, lane, axis=1, mode="promise_in_bounds")
                got = part if got is None else jnp.where(bank == b, part, got)
            got = got - ext_ref[f : f + 1, :atoms]
            h.dv[f, here, :] = got
            fields.append(got)
        d, v = fields[:3], fields[3:]
        slot = lax.broadcasted_iota(jnp.int32, (CHUNK, atoms), 0) + first
        q = d[0] * d[0] + d[1] * d[1] + d[2] * d[2]
        qd = 2.0 * (d[0] * v[0] + d[1] * v[1] + d[2] * v[2])
        w = 1.0 / (q + 0.01)
        decay = jnp.where(slot < counts, jnp.exp(-q), 0.0)
        s = decay * jnp.sqrt(w)
        u = decay * w
        s_q = -s * (1.0 + 0.5 * w)
        u_q = -u * (1.0 + w)
        shrink = 1.0 / (1.0 + s)
        for at, value in enumerate((qd, w, s, u, shrink)):
            h.radial[at, here, :] = value
        step = s_q * qd
        for at, value in enumerate(
            [-2.0 * top * shrink * shrink * step]
            + [s] + [u * e for e in d]
            + [step] + [u_q * qd * d[e] + u * v[e] for e in range(3)]
        ):
            h.mix[at, here, :] = value
        scaled = s * shrink * top
        for k in range(levels):
            y = scaled - float(k)
            phi = jnp.exp(-(y * y))
            psi = y * phi
            h.gauss[k, 0, here, :] = phi
            h.gauss[k, 1, here, :] = psi
            h.gauss[k, 2, here, :] = y * psi
        return carry

    lax.fori_loop(0, width // CHUNK, one, 0, unroll=8)


def pooled_terms(h):
    width, atoms = h.idt.shape
    levels = h.gauss.shape[0]
    together = 4
    zero = jnp.zeros((CHUNK, atoms), F32)
    for k0 in range(0, levels, together):

        def one(c, acc):
            here = slice(c * CHUNK, (c + 1) * CHUNK)
            slope = h.mix[0, here, :]
            r = [h.mix[1 + a, here, :] for a in range(4)]
            dr = [h.mix[5 + a, here, :] for a in range(4)]
            out = []
            for k in range(together):
                phi = h.gauss[k0 + k, 0, here, :]
                psi = h.gauss[k0 + k, 1, here, :] * slope
                out += [acc[8 * k + a] + phi * r[a] for a in range(4)]
                out += [acc[8 * k + 4 + a] + (phi * dr[a] + psi * r[a]) for a in range(4)]
            return tuple(out)

        acc = (zero,) * (8 * together)
        for c in range(width // CHUNK):
            acc = one(c, acc)
        for k in range(together):
            for a in range(8):
                h.pooled[a, k0 + k : k0 + k + 1, :] = jnp.sum(acc[8 * k + a], axis=0, keepdims=True) / width


def of_kind(kinds, rows):
    types = len(kinds)
    step = rows.shape[0] // types
    out = rows[:step]
    for t in range(1, types):
        out = jnp.where(kinds[t], rows[t * step : (t + 1) * step], out)
    return out


def lanes_of(x, count, atoms):
    return [x[:, a * atoms : (a + 1) * atoms] for a in range(count)]


def fitting_net(h, kinds_ref, types):
    fit = h.columns.shape[0]
    fit_wide = h.w2_left.shape[1] // 3
    levels = h.pooled.shape[1]
    m2 = h.lead_up.shape[0] // types
    width, atoms = h.idt.shape
    kinds2 = jnp.concatenate([kinds_ref[...]] * 2, axis=1)
    kinds8 = jnp.concatenate([kinds2] * 4, axis=1)
    kinds2 = [kinds2 == t for t in range(types)]
    kinds8 = [kinds8 == t for t in range(types)]
    pooled = jnp.concatenate([h.pooled[a] for a in range(8)], axis=1)
    lead = lanes_of(of_kind(kinds8, matmul(h.lead_up[...], right_parts(pooled))), 8, atoms)
    for k in range(levels):
        rows = [h.pooled[a, k : k + 1, :] for a in range(8)]
        plain = rows[0] * lead[0]
        moved = rows[4] * lead[0] + rows[0] * lead[4]
        for a in range(1, 4):
            plain += rows[a] * lead[a]
            moved += rows[4 + a] * lead[a] + rows[a] * lead[4 + a]
        h.product[k * m2 : (k + 1) * m2, :atoms] = plain
        h.product[k * m2 : (k + 1) * m2, atoms:] = moved
    z1 = of_kind(kinds2, matmul(h.low_right[...], right_parts(h.product[...])))
    b1, b2, fo = h.columns[:, 0:1], h.columns[:, 1:2], h.columns[:, 2:3]
    h1 = jnp.tanh(z1[:, :atoms] + b1)
    gate1 = 1.0 - h1 * h1
    dh1 = gate1 * z1[:, atoms:]
    z2 = matmul(h.w2_right[...], right_parts(padded(jnp.concatenate([h1, dh1], axis=1), fit_wide, 0)))
    t2 = jnp.tanh(z2[:, :atoms] + b2)
    gate2 = 1.0 - t2 * t2
    dt2 = gate2 * z2[:, atoms:]
    gz2 = jnp.concatenate([fo * gate2, fo * (-2.0 * t2 * dt2)], axis=1)
    gh = matmul(h.w2_left[...], right_parts(padded(gz2, fit_wide, 0)))
    gh1 = gh[:, :atoms] + fo
    gz1 = jnp.concatenate([gh1 * gate1, gh[:, atoms:] * gate1 - 2.0 * gh1 * h1 * dh1], axis=1)
    h.pulled[...] = of_kind(kinds2, matmul(h.low_left[...], right_parts(padded(gz1, fit_wide, 0))))
    acc = [jnp.zeros((m2, atoms), F32) for _ in range(8)]
    for k in range(levels):
        g = h.pulled[k * m2 : (k + 1) * m2, :atoms]
        dg = h.pulled[k * m2 : (k + 1) * m2, atoms:]
        rows = [h.pooled[a, k : k + 1, :] for a in range(8)]
        for a in range(4):
            straight = jnp.sum(g * lead[a], axis=0, keepdims=True)
            turned = jnp.sum(dg * lead[a] + g * lead[4 + a], axis=0, keepdims=True)
            h.gp[k : k + 1, a * atoms : (a + 1) * atoms] = straight
            h.gp[k : k + 1, (4 + a) * atoms : (5 + a) * atoms] = turned
            acc[a] = acc[a] + g * rows[a]
            acc[4 + a] = acc[4 + a] + (dg * rows[a] + g * rows[4 + a])
    across = of_kind(kinds8, matmul(h.lead_down[...], right_parts(jnp.concatenate(acc, axis=1))))
    h.gp[...] = (h.gp[...] + across) / width


def pair_forces(h, out_ref):
    width, atoms = h.idt.shape
    levels = h.gauss.shape[0]
    banks = h.in_bank.shape[0]
    top = float(levels - 1)

    def force_of(c, centre):
        first = pl.multiple_of(c * CHUNK, CHUNK)
        here = pl.ds(first, CHUNK)
        zero = jnp.zeros((CHUNK, atoms), F32)
        s0, s1, s2, e0, e1 = ([zero] * 4 for _ in range(5))
        for k in range(levels):
            phi, psi, chi = (h.gauss[k, p, here, :] for p in range(3))
            for a in range(4):
                g = h.gp[k : k + 1, a * atoms : (a + 1) * atoms]
                gd = h.gp[k : k + 1, (4 + a) * atoms : (5 + a) * atoms]
                s0[a] = s0[a] + g * phi
                s1[a] = s1[a] + g * psi
                s2[a] = s2[a] + g * chi
                e0[a] = e0[a] + gd * phi
                e1[a] = e1[a] + gd * psi
        d = [h.dv[f, here, :] for f in range(3)]
        v = [h.dv[f, here, :] for f in range(3, 6)]
        qd, w, s, u, shrink = (h.radial[at, here, :] for at in range(5))
        s_q = -s * (1.0 + 0.5 * w)
        u_q = -u * (1.0 + w)
        t_s = shrink * shrink
        t_q = t_s * s_q
        s_qq = -s_q * (1.0 + 0.5 * w) + 0.5 * s * w * w
        u_qq = -u_q * (1.0 + w) + u * w * w
        t_qq = -2.0 * t_s * shrink * s_q * s_q + t_s * s_qq
        step = t_q * qd
        val = s0
        val_t = [-2.0 * top * e for e in s1]
        val_tt = [top * top * (4.0 * s2[a] - 2.0 * s0[a]) for a in range(4)]
        dval = [e0[a] + val_t[a] * step for a in range(4)]
        dval_t = [-2.0 * top * e1[a] + val_tt[a] * step for a in range(4)]
        big = val[1] * d[0] + val[2] * d[1] + val[3] * d[2]
        big_t = val_t[1] * d[0] + val_t[2] * d[1] + val_t[3] * d[2]
        dbig = sum(dval[1 + e] * d[e] + val[1 + e] * v[e] for e in range(3))
        dbig_t = sum(dval_t[1 + e] * d[e] + val_t[1 + e] * v[e] for e in range(3))
        flow = val_t[0] * s + big_t * u
        kern = t_q * flow + val[0] * s_q + big * u_q
        dkern = (
            t_q * (dval_t[0] * s + dbig_t * u)
            + dval[0] * s_q
            + dbig * u_q
            + qd * (t_qq * flow + t_q * (val_t[0] * s_q + big_t * u_q) + val[0] * s_qq + big * u_qq)
        )
        du = u_q * qd
        out = []
        for e in range(3):
            force = 2.0 * (v[e] * kern + d[e] * dkern) + du * val[1 + e] + u * dval[1 + e]
            high = force.astype(BF16).astype(F32)
            h.forces[pl.ds(first * 8 + e, CHUNK, stride=8), :] = high
            h.forces[pl.ds(first * 8 + 3 + e, CHUNK, stride=8), :] = force - high
            out.append(centre[e] - force)
        return tuple(out)

    zero = jnp.zeros((CHUNK, atoms), F32)
    centre = lax.fori_loop(0, width // CHUNK, force_of, (zero,) * 3)

    together = width // 2

    def scatter(c, acc):
        lefts = []
        for r in range(together):
            n = c * together + r
            part = h.forces[pl.ds(pl.multiple_of(n * 8, 8), 8), :]
            lefts.append(
                jnp.concatenate([part * h.in_bank[b, pl.ds(n, 1), :] for b in range(banks)], axis=0).astype(BF16)
            )
        right = jnp.concatenate([h.onehot[c * (together // CHUNK) + j] for j in range(together // CHUNK)], axis=1)
        return acc + lax.dot_general(
            jnp.concatenate(lefts, axis=1), right, (((1,), (1,)), ((), ())), preferred_element_type=F32
        )

    acc = lax.fori_loop(0, width // together, scatter, jnp.zeros((8 * banks, DIGIT), F32))
    per = 128 // DIGIT
    for b in range(0, banks, per):
        part = jnp.concatenate([acc[8 * j : 8 * j + 8] for j in range(b, b + per)], axis=1)
        out_ref[:, b * DIGIT : (b + per) * DIGIT] = part + jnp.concatenate([part[3:], part[:3]], axis=0)
    for e in range(3):
        out_ref[e : e + 1, :atoms] += jnp.sum(centre[e], axis=0, keepdims=True)


def hessian_product(h, ext_ref, counts_ref, kinds_ref, out_ref, types):
    pair_terms(h, ext_ref, counts_ref[...])
    pooled_terms(h)
    fitting_net(h, kinds_ref, types)
    pair_forces(h, out_ref)


class Scratch:
    def __init__(self, names, refs):
        for name, ref in zip(names, refs, strict=True):
            setattr(self, name, ref)


AXES = ("gx", "gy", "gz")
MESH = pl.DeviceIdType.MESH
GROUP_LIMIT = 32


def sizes_of():
    return [lax.axis_size(axis) for axis in AXES]


def plane_offsets():
    def along(size):
        return (0, 1) if size == 2 else (0, 1, -1)

    _, ny, nz = sizes_of()
    return [(dy, dz) for dz in along(nz) for dy in along(ny)]


def device_at(shift):
    return {
        axis: lax.rem(lax.axis_index(axis) + (step + peers) % peers, peers)
        for axis, step, peers in zip(AXES, shift, sizes_of())
    }


def reduction_groups():
    sizes = sizes_of()
    groups = []
    for at in range(3):
        if groups and groups[-1][1] * sizes[at] <= GROUP_LIMIT:
            groups[-1] = (groups[-1][0] + [at], groups[-1][1] * sizes[at])
        else:
            groups.append(([at], sizes[at]))
    out = []
    for members, count in groups:
        shifts = [[0, 0, 0]]
        for at in members:
            shifts = [s[:at] + [step] + s[at + 1 :] for s in shifts for step in range(sizes[at])]
        out.append((members, count, [tuple(s) for s in shifts if any(s)]))
    return out


def place_in(members):
    sizes = sizes_of()
    me = 0
    for at in members:
        me = me * sizes[at] + lax.axis_index(AXES[at])
    return me


def three_parts(x):
    high = x.astype(BF16)
    rest = x - high.astype(F32)
    middle = rest.astype(BF16)
    low = (rest - middle.astype(F32)).astype(BF16)
    return jnp.concatenate([high.astype(F32), middle.astype(F32), low.astype(F32)], axis=0).astype(BF16)


def select_dot(x, onehot, dims):
    n = x.shape[0]
    out = lax.dot_general(three_parts(x), onehot, (dims, ((), ())), preferred_element_type=F32)
    return (out[:n] + out[n : 2 * n]) + out[2 * n :]


def chosen_columns(map_row, columns):
    rows = lax.broadcasted_iota(jnp.int32, (columns, map_row.shape[1]), 0).astype(F32)
    return jnp.where(rows == map_row, 1.0, 0.0).astype(BF16)


def sides(parts, early):
    if -1 in parts:
        return jnp.where(early, parts[-1], parts[1])
    return parts[1]


def one_side(x, step, distinct, early):
    if not distinct:
        return x
    return jnp.where(early, x, 0.0) if step == -1 else jnp.where(early, 0.0, x)


class Round:
    def __init__(self, sems, at, landed):
        self.sems, self.at, self.landed = sems, at, landed

    def copy(self, source, target, shift):
        return pltpu.make_async_remote_copy(
            src_ref=source,
            dst_ref=target,
            send_sem=self.sems.at[self.at, 0],
            recv_sem=self.sems.at[self.at, 1],
            device_id=device_at(shift),
            device_id_type=MESH,
        )

    def send(self, source, target, shift):
        self.shift = shift
        self.copy(source, target, shift).start()

    def all_of_them(self):
        return self.copy(self.landed, self.landed, self.shift)


def lanczos_kernel(*refs, inputs, names):
    hbm, (next_ref, corr_ref, norm_ref) = refs[:inputs], refs[inputs : inputs + 3]
    local = refs[inputs + 3 : 2 * inputs + 3]
    (load_sem, round_sem, ext, work, mine, face, landed, back_raw, back_face, returned, stack, gram_land, row_land, *hvp_scratch) = refs[2 * inputs + 3 :]
    places, basis, ids, counts, kinds, map_x, map_y, map_z, table, w1, w2, b1, b2, fo = local
    h = Scratch(names, hvp_scratch)
    types = table.shape[0]
    atoms = places.shape[2]
    stored = basis.shape[0]
    rows = stack.shape[0]
    pair = 2 * map_x.shape[1]
    sizes = sizes_of()
    entries = 3 * atoms * sizes[0] * sizes[1] * sizes[2]
    planes = plane_offsets()
    groups = reduction_groups()
    count = len(planes)

    partners = set()
    for dy, dz in planes:
        for dx in (-1, 0, 1):
            partners.add(tuple(step % peers for step, peers in zip((dx, dy, dz), sizes)))
    for _, _, shifts in groups:
        partners.update(shifts)
    partners = sorted(partners - {(0, 0, 0)})
    opposite = {tuple(-step % peers for step, peers in zip(shift, sizes)) for shift in partners}
    assert opposite == set(partners)
    barrier = pltpu.get_barrier_semaphore()
    for shift in partners:
        pl.semaphore_signal(barrier, inc=1, device_id=device_at(shift), device_id_type=MESH)
    loads = [pltpu.make_async_copy(a, b, load_sem.at[at]) for at, (a, b) in enumerate(zip(hbm, local))]
    for at in (0, 1, 5, 6, 7, 2, 3, 4, 8, 9, 10, 11, 12, 13):
        loads[at].start()
    early = lax.broadcasted_iota(jnp.int32, (8, pair), 1) < pair // 2
    line = lax.broadcasted_iota(jnp.int32, (8, pair), 0)
    for at in (0, 1, 5, 6, 7):
        loads[at].wait()
    for c in range(3):
        mine[c : c + 1, :] = places[c]
        mine[3 + c : 4 + c, :] = basis[stored - 1, c]
    map_rows = [jnp.concatenate([m[1:2, :], m[0:1, :]], axis=1).astype(F32) for m in (map_x, map_y, map_z)]
    mine[6:7, :] = map_rows[1]
    mine[7:8, :] = map_rows[2]
    pick_x = chosen_columns(map_rows[0], atoms)
    face[...] = select_dot(mine[...], pick_x, ((1,), (0,)))
    pl.semaphore_wait(barrier, len(partners))

    halo = Round(round_sem, 0, landed)
    for at, (dy, dz) in reversed(list(enumerate(planes))):
        halo.send(face, landed.at[at], (1, -dy, -dz))
        halo.send(face, landed.at[count + at], (-1, -dy, -dz))
        if at:
            halo.send(mine, landed.at[2 * count + at - 1], (0, -dy, -dz))

    stack[rows - 8 :, :] = jnp.zeros((8, 3 * atoms), F32)
    for k in range(stored):
        for c in range(3):
            stack[k : k + 1, c * atoms : (c + 1) * atoms] = basis[k, c]
    gram = dot_full(stack[...], stack[...], ((1,), (1,)))
    gram = jnp.concatenate([gram[r : r + 8] for r in range(0, rows, 8)], axis=1)
    for at in (2, 3, 4, 8, 9, 10, 11, 12, 13):
        loads[at].wait()
    prepare_scatter(h, ids)
    prepare_matrices(h, table, w1, w2, b1, b2, fo)
    halo.all_of_them().wait_recv()

    def shifted(x, row):
        return x + jnp.where(line == row, jnp.where(early, -1.0, 1.0), 0.0)

    raw = {plane: mine[...] if at == 0 else landed[2 * count + at - 1] for at, plane in enumerate(planes)}
    wide = {
        plane: jnp.concatenate([raw[plane], shifted(jnp.where(early, landed[at], landed[count + at]), 0)], axis=1)
        for at, plane in enumerate(planes)
    }
    pick_y, pick_z, wider = {}, {}, {}
    for dz in sorted({dz for _, dz in planes}):
        got = {}
        for dy in (1, -1):
            if (dy, dz) in raw:
                pick_y[dy, dz] = chosen_columns(raw[dy, dz][6:7, :], atoms + pair)
                got[dy] = select_dot(wide[dy, dz], pick_y[dy, dz], ((1,), (0,)))
        wider[dz] = jnp.concatenate([wide[0, dz], shifted(sides(got, early), 1)], axis=1)
    got = {}
    for dz in (1, -1):
        if dz in wider:
            pick_z[dz] = chosen_columns(raw[0, dz][7:8, :], atoms + 2 * pair)
            got[dz] = select_dot(wider[dz], pick_z[dz], ((1,), (0,)))
    ext[:, : atoms + 2 * pair] = wider[0]
    ext[:, atoms + 2 * pair :] = shifted(sides(got, early), 2)

    def gather_from(group, kind, tiles, base, value):
        members, size, shifts = groups[group]
        me = base + place_in(members)
        tiles[me] = value
        around = Round(round_sem, 2 + 2 * group + kind, tiles.at[pl.ds(base, size - 1)])
        for shift in shifts:
            around.send(tiles.at[me], tiles.at[me], shift)
        return around

    def added(tiles, base, size):
        total = tiles[base]
        for other in range(1, size):
            total = total + tiles[base + other]
        return total

    rounds = [halo, gather_from(0, 0, gram_land, 0, gram)]

    hessian_product(h, ext, counts, kinds, work, types)

    many_y, many_z = -1 in {dy for dy, _ in planes}, -1 in wider
    back = {0: work[:, : atoms + 2 * pair]}
    for dz in pick_z:
        part = one_side(work[:, atoms + 2 * pair :], dz, many_z, early)
        back[dz] = select_dot(part, pick_z[dz], ((1,), (1,)))
    terms = {(0, dz): x[:, : atoms + pair] for dz, x in back.items()}
    for dy, dz in pick_y:
        part = one_side(back[dz][:, atoms + pair :], dy, many_y, early)
        terms[dy, dz] = select_dot(part, pick_y[dy, dz], ((1,), (1,)))
    back_round = Round(round_sem, 1, returned)
    for at, (dy, dz) in reversed(list(enumerate(planes))):
        back_raw[at] = terms[dy, dz][:, :atoms]
        back_face[at] = terms[dy, dz][:, atoms:]
        back_round.send(back_face.at[at], returned.at[at], (-1, dy, dz))
        back_round.send(back_face.at[at], returned.at[count + at], (1, dy, dz))
        if at:
            back_round.send(back_raw.at[at], returned.at[2 * count + at - 1], (0, dy, dz))

    rounds[-1].all_of_them().wait_recv()
    total = added(gram_land, 0, groups[0][1])
    base = groups[0][1]
    for group in range(1, len(groups)):
        rounds.append(gather_from(group, 0, gram_land, base, total))
        rounds[-1].all_of_them().wait_recv()
        total = added(gram_land, base, groups[group][1])
        base += groups[group][1]
    rounds.append(back_round)
    gram = jnp.concatenate([total[:, r : r + rows] for r in range(0, rows * rows // 8, rows)], axis=0) / entries

    back_round.all_of_them().wait_recv()
    own, up, low = back_raw[0], returned[0], returned[count]
    for at in range(1, count):
        own = own + returned[2 * count + at - 1]
        up = up + returned[at]
        low = low + returned[count + at]
    own = own + select_dot(jnp.where(early, up, low), pick_x, ((1,), (1,)))
    hv = jnp.concatenate([own[c : c + 1, :] for c in range(3)], axis=1)
    stack[stored : stored + 1, :] = hv
    sums = dot_full(jnp.broadcast_to(hv, (8, 3 * atoms)), stack[...], ((1,), (1,)))
    sums = jnp.concatenate([sums[0:1], jnp.zeros((1, row_land.shape[2] - rows), F32)], axis=1)
    base = 0
    for group in range(len(groups)):
        rounds.append(gather_from(group, 1, row_land, base, sums))
        rounds[-1].all_of_them().wait_recv()
        sums = added(row_land, base, groups[group][1])
        base += groups[group][1]
    for around in rounds:
        around.all_of_them().wait_send()
    lane = lax.broadcasted_iota(jnp.int32, (1, rows), 1)
    sums = sums[:, :rows] / entries
    kept = jnp.where(lane < stored, sums, 0.0)
    both = jnp.concatenate([gram, stack[...]], axis=1)
    mixed = dot_full(jnp.broadcast_to(kept, (8, rows)), both, ((1,), (0,)))[0:1]
    plain = sums[:, stored : stored + 1]
    cross = jnp.sum(mixed[:, :rows] * kept - 2.0 * kept * kept, axis=1, keepdims=True)
    norm = jnp.sqrt(plain + cross + 1e-06)
    norm_ref[...] = norm
    corr_ref[...] = sums[:, :stored]
    for c in range(3):
        part = slice(c * atoms, (c + 1) * atoms)
        next_ref[c] = (hv[:, part] - mixed[:, rows:][:, part]) / norm


def hand_over(*refs):
    count = (len(refs) - 1) // 2
    sems = refs[-1]
    copies = [pltpu.make_async_copy(refs[at], refs[count + at], sems.at[at]) for at in range(count)]
    for copy in copies:
        copy.start()
    for copy in copies:
        copy.wait()


def on_device(positions, basis, neighbours, used_count, kinds, map_x, map_y, map_z,
              table, fit_w1, fit_b1, fit_w2, fit_b2, fit_out):
    atoms = positions.shape[-1]
    width = neighbours.shape[-1]
    stored = basis.shape[0]
    types, levels, m1 = table.shape
    m2 = fit_w1.shape[0] // m1
    pair = 2 * map_x.shape[-1]
    ext = atoms + 3 * pair
    args = [
        positions.reshape(3, 1, atoms),
        basis.reshape(stored, 3, 1, atoms),
        neighbours.reshape(atoms, width),
        used_count.reshape(1, atoms),
        kinds.reshape(1, atoms),
        map_x.reshape(2, -1),
        map_y.reshape(2, -1),
        map_z.reshape(2, -1),
        table,
        fit_w1.T,
        fit_w2,
        fit_b1[None],
        fit_b2[None],
        fit_out[None],
    ]
    rows = (stored + 8) // 8 * 8
    planes = len(plane_offsets())
    groups = reduction_groups()
    slots = sum(count for _, count, _ in groups)
    hvp = hvp_shapes(atoms, width, types, levels, m1, m2, fit_w2.shape[0], ext)
    any_space = pl.BlockSpec(memory_space=pl.ANY)
    vmem = pl.BlockSpec(memory_space=pltpu.VMEM)
    tiles = pltpu.VMEM((planes, 8, pair), F32)
    arrivals = pltpu.VMEM((3 * planes - 1, 8, pair), F32)
    results = pl.pallas_call(
        functools.partial(lanczos_kernel, inputs=len(args), names=tuple(hvp)),
        out_shape=(
            jax.ShapeDtypeStruct((3, 1, atoms), F32),
            jax.ShapeDtypeStruct((1, stored), F32),
            jax.ShapeDtypeStruct((1, 1), F32),
        ),
        in_specs=[any_space] * len(args),
        out_specs=(vmem,) * 3,
        scratch_shapes=[pltpu.VMEM(x.shape, x.dtype) for x in args] + [
            pltpu.SemaphoreType.DMA((len(args),)),
            pltpu.SemaphoreType.DMA((2 + 2 * len(groups), 2)),
            pltpu.VMEM((8, ext), F32),
            pltpu.VMEM((8, ext), F32),
            pltpu.VMEM((8, pair), F32),
            pltpu.VMEM((8, pair), F32),
            arrivals,
            tiles,
            tiles,
            arrivals,
            pltpu.VMEM((rows, 3 * atoms), F32),
            pltpu.VMEM((slots, 8, rows * rows // 8), F32),
            pltpu.VMEM((slots, 1, 128), F32),
        ] + [pltpu.VMEM(shape, dtype) for shape, dtype in hvp.values()],
        compiler_params=pltpu.CompilerParams(
            collective_id=0, has_side_effects=True, vmem_limit_bytes=60 << 20
        ),
        name="lanczos",
    )(*args)
    results = pl.pallas_call(
        hand_over,
        out_shape=tuple(jax.ShapeDtypeStruct(x.shape, x.dtype) for x in results),
        in_specs=[any_space] * 3,
        out_specs=(any_space,) * 3,
        scratch_shapes=[pltpu.SemaphoreType.DMA((3,))],
        name="hand_over",
    )(*results)
    next_vector, correlations, norm = results
    return next_vector.reshape(positions.shape), correlations.reshape(stored), norm.reshape(())


def solution(mesh):
    placed = (
        P(None, "gx", "gy", "gz", None),
        P(None, None, "gx", "gy", "gz", None),
        P("gx", "gy", "gz", None, None),
        P("gx", "gy", "gz", None),
        P("gx", "gy", "gz", None),
        P("gx", "gy", "gz", None, None),
        P("gx", "gy", "gz", None, None),
        P("gx", "gy", "gz", None, None),
        P(),
        P(),
        P(),
        P(),
        P(),
        P(),
    )
    return jax.shard_map(
        on_device,
        mesh=mesh,
        in_specs=placed,
        out_specs=(P(None, "gx", "gy", "gz", None), P(), P()),
        check_vma=False,
    )
```

```python
import functools

import jax
import jax.numpy as jnp
from jax import lax
from jax.experimental import pallas as pl
from jax.experimental.pallas import tpu as pltpu
from jax.sharding import PartitionSpec as P

F32, BF16 = jnp.float32, jnp.bfloat16
HIGHEST = lax.Precision.HIGHEST
CHUNK = 8
DIGIT = 64


def split(x):
    high = x.astype(BF16)
    return high, (x - high.astype(F32)).astype(BF16)


def left_parts(x):
    high, low = split(x)
    return jnp.concatenate([high, low, high], axis=1)


def right_parts(x):
    high, low = split(x)
    return jnp.concatenate([high, high, low], axis=0)


def matmul(a, b):
    return lax.dot_general(a, b, (((1,), (0,)), ((), ())), preferred_element_type=F32)


def dot_full(a, b, dims):
    return lax.dot_general(a, b, (dims, ((), ())), precision=HIGHEST, preferred_element_type=F32)


def padded(x, rows, columns):
    if columns > x.shape[1]:
        x = jnp.concatenate([x, jnp.zeros((x.shape[0], columns - x.shape[1]), x.dtype)], axis=1)
    if rows > x.shape[0]:
        x = jnp.concatenate([x, jnp.zeros((rows - x.shape[0], x.shape[1]), x.dtype)], axis=0)
    return x


def up_to(n, step):
    return (n + step - 1) // step * step


def hvp_shapes(atoms, width, types, levels, m1, m2, fit, ext):
    fit_wide, m1_wide = up_to(fit, 128), up_to(m1, 128)
    low = levels * m2
    return dict(
        idt=((width, atoms), jnp.int32),
        onehot=((width // CHUNK, DIGIT, CHUNK * atoms), BF16),
        in_bank=((width, ext // DIGIT, atoms), F32),
        w1_rows=((fit_wide // 128, m1_wide * m2, 128), F32),
        w1_low=((fit_wide // 128, types * low, 128), F32),
        low_right=((types * fit, 3 * low), BF16),
        low_left=((types * low, 3 * fit_wide), BF16),
        w2_right=((fit, 3 * fit_wide), BF16),
        w2_left=((fit, 3 * fit_wide), BF16),
        columns=((fit, 8), F32),
        lead_up=((types * m2, 3 * levels), BF16),
        lead_down=((types * levels, 3 * m2), BF16),
        dv=((6, width + CHUNK, atoms), F32),
        radial=((5, width + CHUNK, atoms), F32),
        mix=((9, width + CHUNK, atoms), F32),
        gauss=((levels, 3, width + CHUNK, atoms), F32),
        pooled=((8, levels, atoms), F32),
        product=((low, 2 * atoms), F32),
        pulled=((low, 2 * atoms), F32),
        gp=((levels, 8 * atoms), F32),
        forces=((6, width + CHUNK, atoms), F32),
    )


def prepare_matrices(h, table_ref, w1_ref, w2_ref, b1_ref, b2_ref, fo_ref):
    types, levels, m1 = table_ref.shape
    fit, m2 = w1_ref.shape[0], w1_ref.shape[1] // m1
    halves, rows, _ = h.w1_rows.shape
    m1_wide, low = rows // m2, levels * m2
    turned = padded(w1_ref[...], halves * 128, 0).T
    tables = jnp.concatenate([padded(table_ref[t], 0, m1_wide) for t in range(types)], axis=0)
    tables = left_parts(tables)
    for half in range(halves):
        h.w1_rows[half, : m1 * m2, :] = turned[:, half * 128 : (half + 1) * 128]
        h.w1_rows[half, m1 * m2 :, :] = jnp.zeros((rows - m1 * m2, 128), F32)
    for n in range(m2):
        part = [h.w1_rows[half, pl.ds(n, m1_wide, stride=m2), :] for half in range(halves)]
        out = matmul(tables, right_parts(jnp.concatenate(part, axis=1)))
        for half in range(halves):
            h.w1_low[half, pl.ds(n, types * levels, stride=m2), :] = out[:, half * 128 : (half + 1) * 128]
    for t in range(types):
        at = slice(t * low, (t + 1) * low)
        mine = jnp.concatenate([h.w1_low[half, at, :] for half in range(halves)], axis=1)
        h.low_left[at, :] = left_parts(mine)
        h.low_right[t * fit : (t + 1) * fit, :] = left_parts(mine.T[:fit])
    w2 = padded(w2_ref[...], halves * 128, halves * 128)
    h.w2_left[...] = left_parts(w2[:fit])
    h.w2_right[...] = left_parts(w2.T[:fit])
    lines = jnp.concatenate([b1_ref[...], b2_ref[...], fo_ref[...], jnp.zeros((5, fit), F32)], axis=0)
    h.columns[...] = dot_full(lines, identity(8), ((0,), (0,)))
    for t in range(types):
        first = table_ref[t][:, :m2]
        h.lead_down[t * levels : (t + 1) * levels, :] = left_parts(first)
        h.lead_up[t * m2 : (t + 1) * m2, :] = left_parts(dot_full(first, identity(levels), ((0,), (0,))))


def identity(n):
    same = lax.broadcasted_iota(jnp.int32, (n, n), 0) == lax.broadcasted_iota(jnp.int32, (n, n), 1)
    return jnp.where(same, 1.0, 0.0).astype(F32)


def prepare_scatter(h, ids_ref):
    width, atoms = h.idt.shape
    h.idt[...] = ids_ref[...].T
    group = lax.broadcasted_iota(jnp.int32, h.in_bank.shape[1:], 0)
    column = lax.broadcasted_iota(jnp.int32, (DIGIT, atoms), 0)

    def one(c, carry):
        idx = h.idt[pl.ds(pl.multiple_of(c * CHUNK, CHUNK), CHUNK), :]
        digit = jnp.bitwise_and(idx, DIGIT - 1)
        bank = jnp.right_shift(idx, DIGIT.bit_length() - 1)
        for r in range(CHUNK):
            h.in_bank[c * CHUNK + r] = jnp.where(bank[r : r + 1, :] == group, 1.0, 0.0).astype(F32)
            hit = jnp.where(digit[r : r + 1, :] == column, 1.0, 0.0)
            h.onehot[c, :, r * atoms : (r + 1) * atoms] = hit.astype(BF16)
        return carry

    lax.fori_loop(0, width // CHUNK, one, 0)


def pair_terms(h, ext_ref, counts):
    width, atoms = h.idt.shape
    levels = h.gauss.shape[0]
    banks = ext_ref.shape[1] // 128
    top = float(levels - 1)

    def one(c, carry):
        first = pl.multiple_of(c * CHUNK, CHUNK)
        here = pl.ds(first, CHUNK)
        idx = h.idt[here, :]
        lane = jnp.bitwise_and(idx, 127)
        bank = jnp.right_shift(idx, 7)
        fields = []
        for f in range(6):
            got = None
            for b in range(banks):
                row = jnp.broadcast_to(ext_ref[f : f + 1, b * 128 : (b + 1) * 128], (CHUNK, 128))
                part = jnp.take_along_axis(row, lane, axis=1, mode="promise_in_bounds")
                got = part if got is None else jnp.where(bank == b, part, got)
            got = got - ext_ref[f : f + 1, :atoms]
            h.dv[f, here, :] = got
            fields.append(got)
        d, v = fields[:3], fields[3:]
        slot = lax.broadcasted_iota(jnp.int32, (CHUNK, atoms), 0) + first
        q = d[0] * d[0] + d[1] * d[1] + d[2] * d[2]
        qd = 2.0 * (d[0] * v[0] + d[1] * v[1] + d[2] * v[2])
        w = 1.0 / (q + 0.01)
        decay = jnp.where(slot < counts, jnp.exp(-q), 0.0)
        s = decay * jnp.sqrt(w)
        u = decay * w
        s_q = -s * (1.0 + 0.5 * w)
        u_q = -u * (1.0 + w)
        shrink = 1.0 / (1.0 + s)
        for at, value in enumerate((qd, w, s, u, shrink)):
            h.radial[at, here, :] = value
        step = s_q * qd
        for at, value in enumerate(
            [-2.0 * top * shrink * shrink * step]
            + [s] + [u * e for e in d]
            + [step] + [u_q * qd * d[e] + u * v[e] for e in range(3)]
        ):
            h.mix[at, here, :] = value
        scaled = s * shrink * top
        for k in range(levels):
            y = scaled - float(k)
            phi = jnp.exp(-(y * y))
            psi = y * phi
            h.gauss[k, 0, here, :] = phi
            h.gauss[k, 1, here, :] = psi
            h.gauss[k, 2, here, :] = y * psi
        return carry

    lax.fori_loop(0, width // CHUNK, one, 0, unroll=8)


def pooled_terms(h):
    width, atoms = h.idt.shape
    levels = h.gauss.shape[0]
    together = 4
    zero = jnp.zeros((CHUNK, atoms), F32)
    for k0 in range(0, levels, together):

        def one(c, acc):
            here = slice(c * CHUNK, (c + 1) * CHUNK)
            slope = h.mix[0, here, :]
            r = [h.mix[1 + a, here, :] for a in range(4)]
            dr = [h.mix[5 + a, here, :] for a in range(4)]
            out = []
            for k in range(together):
                phi = h.gauss[k0 + k, 0, here, :]
                psi = h.gauss[k0 + k, 1, here, :] * slope
                out += [acc[8 * k + a] + phi * r[a] for a in range(4)]
                out += [acc[8 * k + 4 + a] + (phi * dr[a] + psi * r[a]) for a in range(4)]
            return tuple(out)

        acc = (zero,) * (8 * together)
        for c in range(width // CHUNK):
            acc = one(c, acc)
        for k in range(together):
            for a in range(8):
                h.pooled[a, k0 + k : k0 + k + 1, :] = jnp.sum(acc[8 * k + a], axis=0, keepdims=True) / width


def of_kind(kinds, rows):
    types = len(kinds)
    step = rows.shape[0] // types
    out = rows[:step]
    for t in range(1, types):
        out = jnp.where(kinds[t], rows[t * step : (t + 1) * step], out)
    return out


def lanes_of(x, count, atoms):
    return [x[:, a * atoms : (a + 1) * atoms] for a in range(count)]


def fitting_net(h, kinds_ref, types):
    fit = h.columns.shape[0]
    fit_wide = h.w2_left.shape[1] // 3
    levels = h.pooled.shape[1]
    m2 = h.lead_up.shape[0] // types
    width, atoms = h.idt.shape
    kinds2 = jnp.concatenate([kinds_ref[...]] * 2, axis=1)
    kinds8 = jnp.concatenate([kinds2] * 4, axis=1)
    kinds2 = [kinds2 == t for t in range(types)]
    kinds8 = [kinds8 == t for t in range(types)]
    pooled = jnp.concatenate([h.pooled[a] for a in range(8)], axis=1)
    lead = lanes_of(of_kind(kinds8, matmul(h.lead_up[...], right_parts(pooled))), 8, atoms)
    for k in range(levels):
        rows = [h.pooled[a, k : k + 1, :] for a in range(8)]
        plain = rows[0] * lead[0]
        moved = rows[4] * lead[0] + rows[0] * lead[4]
        for a in range(1, 4):
            plain += rows[a] * lead[a]
            moved += rows[4 + a] * lead[a] + rows[a] * lead[4 + a]
        h.product[k * m2 : (k + 1) * m2, :atoms] = plain
        h.product[k * m2 : (k + 1) * m2, atoms:] = moved
    z1 = of_kind(kinds2, matmul(h.low_right[...], right_parts(h.product[...])))
    b1, b2, fo = h.columns[:, 0:1], h.columns[:, 1:2], h.columns[:, 2:3]
    h1 = jnp.tanh(z1[:, :atoms] + b1)
    gate1 = 1.0 - h1 * h1
    dh1 = gate1 * z1[:, atoms:]
    z2 = matmul(h.w2_right[...], right_parts(padded(jnp.concatenate([h1, dh1], axis=1), fit_wide, 0)))
    t2 = jnp.tanh(z2[:, :atoms] + b2)
    gate2 = 1.0 - t2 * t2
    dt2 = gate2 * z2[:, atoms:]
    gz2 = jnp.concatenate([fo * gate2, fo * (-2.0 * t2 * dt2)], axis=1)
    gh = matmul(h.w2_left[...], right_parts(padded(gz2, fit_wide, 0)))
    gh1 = gh[:, :atoms] + fo
    gz1 = jnp.concatenate([gh1 * gate1, gh[:, atoms:] * gate1 - 2.0 * gh1 * h1 * dh1], axis=1)
    h.pulled[...] = of_kind(kinds2, matmul(h.low_left[...], right_parts(padded(gz1, fit_wide, 0))))
    acc = [jnp.zeros((m2, atoms), F32) for _ in range(8)]
    for k in range(levels):
        g = h.pulled[k * m2 : (k + 1) * m2, :atoms]
        dg = h.pulled[k * m2 : (k + 1) * m2, atoms:]
        rows = [h.pooled[a, k : k + 1, :] for a in range(8)]
        for a in range(4):
            straight = jnp.sum(g * lead[a], axis=0, keepdims=True)
            turned = jnp.sum(dg * lead[a] + g * lead[4 + a], axis=0, keepdims=True)
            h.gp[k : k + 1, a * atoms : (a + 1) * atoms] = straight
            h.gp[k : k + 1, (4 + a) * atoms : (5 + a) * atoms] = turned
            acc[a] = acc[a] + g * rows[a]
            acc[4 + a] = acc[4 + a] + (dg * rows[a] + g * rows[4 + a])
    across = of_kind(kinds8, matmul(h.lead_down[...], right_parts(jnp.concatenate(acc, axis=1))))
    h.gp[...] = (h.gp[...] + across) / width


def pair_forces(h, out_ref):
    width, atoms = h.idt.shape
    levels = h.gauss.shape[0]
    banks = h.in_bank.shape[1]
    top = float(levels - 1)

    def force_of(c, centre):
        first = pl.multiple_of(c * CHUNK, CHUNK)
        here = pl.ds(first, CHUNK)
        zero = jnp.zeros((CHUNK, atoms), F32)
        s0, s1, s2, e0, e1 = ([zero] * 4 for _ in range(5))
        for k in range(levels):
            phi, psi, chi = (h.gauss[k, p, here, :] for p in range(3))
            for a in range(4):
                g = h.gp[k : k + 1, a * atoms : (a + 1) * atoms]
                gd = h.gp[k : k + 1, (4 + a) * atoms : (5 + a) * atoms]
                s0[a] = s0[a] + g * phi
                s1[a] = s1[a] + g * psi
                s2[a] = s2[a] + g * chi
                e0[a] = e0[a] + gd * phi
                e1[a] = e1[a] + gd * psi
        d = [h.dv[f, here, :] for f in range(3)]
        v = [h.dv[f, here, :] for f in range(3, 6)]
        qd, w, s, u, shrink = (h.radial[at, here, :] for at in range(5))
        s_q = -s * (1.0 + 0.5 * w)
        u_q = -u * (1.0 + w)
        t_s = shrink * shrink
        t_q = t_s * s_q
        s_qq = -s_q * (1.0 + 0.5 * w) + 0.5 * s * w * w
        u_qq = -u_q * (1.0 + w) + u * w * w
        t_qq = -2.0 * t_s * shrink * s_q * s_q + t_s * s_qq
        step = t_q * qd
        val = s0
        val_t = [-2.0 * top * e for e in s1]
        val_tt = [top * top * (4.0 * s2[a] - 2.0 * s0[a]) for a in range(4)]
        dval = [e0[a] + val_t[a] * step for a in range(4)]
        dval_t = [-2.0 * top * e1[a] + val_tt[a] * step for a in range(4)]
        big = val[1] * d[0] + val[2] * d[1] + val[3] * d[2]
        big_t = val_t[1] * d[0] + val_t[2] * d[1] + val_t[3] * d[2]
        dbig = sum(dval[1 + e] * d[e] + val[1 + e] * v[e] for e in range(3))
        dbig_t = sum(dval_t[1 + e] * d[e] + val_t[1 + e] * v[e] for e in range(3))
        flow = val_t[0] * s + big_t * u
        kern = t_q * flow + val[0] * s_q + big * u_q
        dkern = (
            t_q * (dval_t[0] * s + dbig_t * u)
            + dval[0] * s_q
            + dbig * u_q
            + qd * (t_qq * flow + t_q * (val_t[0] * s_q + big_t * u_q) + val[0] * s_qq + big * u_qq)
        )
        du = u_q * qd
        out = []
        for e in range(3):
            force = 2.0 * (v[e] * kern + d[e] * dkern) + du * val[1 + e] + u * dval[1 + e]
            high = force.astype(BF16).astype(F32)
            h.forces[e, here, :] = high
            h.forces[3 + e, here, :] = force - high
            out.append(centre[e] - force)
        return tuple(out)

    zero = jnp.zeros((CHUNK, atoms), F32)
    def scatter(first, chunks):
        lefts = []
        for n in range(first * CHUNK, (first + chunks) * CHUNK):
            mine = h.in_bank[n]
            lefts.append(jnp.concatenate([h.forces[e, n : n + 1, :] * mine for e in range(6)], axis=0).astype(BF16))
        right = jnp.concatenate([h.onehot[first + j] for j in range(chunks)], axis=1)
        return lax.dot_general(
            jnp.concatenate(lefts, axis=1), right, (((1,), (1,)), ((), ())), preferred_element_type=F32
        )

    chunks = width // CHUNK
    centre = (zero,) * 3
    acc = None
    for piece in range(4):
        if piece:
            part = scatter((piece - 1) * chunks // 4, chunks // 4)
            acc = part if acc is None else acc + part
        for c in range(piece * chunks // 4, (piece + 1) * chunks // 4):
            centre = force_of(c, centre)
    acc = acc + scatter(3 * chunks // 4, chunks // 4)
    per = 128 // DIGIT
    out_ref[3:, :] = jnp.zeros((out_ref.shape[0] - 3, out_ref.shape[1]), F32)
    for e in range(3):
        part = acc[banks * e : banks * (e + 1)] + acc[banks * (3 + e) : banks * (4 + e)]
        for b in range(0, banks, per):
            row = jnp.concatenate([part[j : j + 1] for j in range(b, b + per)], axis=1)
            if b == 0:
                row = row + jnp.sum(centre[e], axis=0, keepdims=True)
            out_ref[e : e + 1, b * DIGIT : (b + per) * DIGIT] = row


def hessian_product(h, ext_ref, counts_ref, kinds_ref, out_ref, types):
    pair_terms(h, ext_ref, counts_ref[...])
    pooled_terms(h)
    fitting_net(h, kinds_ref, types)
    pair_forces(h, out_ref)


class Scratch:
    def __init__(self, names, refs):
        for name, ref in zip(names, refs, strict=True):
            setattr(self, name, ref)


AXES = ("gx", "gy", "gz")
MESH = pl.DeviceIdType.MESH
GROUP_LIMIT = 32


def sizes_of():
    return [lax.axis_size(axis) for axis in AXES]


def plane_offsets():
    def along(size):
        return (0, 1) if size == 2 else (0, 1, -1)

    _, ny, nz = sizes_of()
    return [(dy, dz) for dz in along(nz) for dy in along(ny)]


class Grid:
    def __init__(self):
        self.sizes = sizes_of()
        self.along = []
        for axis, peers in zip(AXES, self.sizes):
            me = lax.axis_index(axis)
            self.along.append([me] + [lax.rem(me + step, peers) for step in range(1, peers)])

    def device(self, shift):
        return {
            axis: row[step % peers] for axis, row, step, peers in zip(AXES, self.along, shift, self.sizes)
        }


def reduction_groups():
    sizes = sizes_of()
    groups = []
    for at in range(3):
        if groups and groups[-1][1] * sizes[at] <= GROUP_LIMIT:
            groups[-1] = (groups[-1][0] + [at], groups[-1][1] * sizes[at])
        else:
            groups.append(([at], sizes[at]))
    out = []
    for members, count in groups:
        shifts = [[0, 0, 0]]
        for at in members:
            shifts = [s[:at] + [step] + s[at + 1 :] for s in shifts for step in range(sizes[at])]
        out.append((members, count, [tuple(s) for s in shifts if any(s)]))
    return out


def place_in(members):
    sizes = sizes_of()
    me = 0
    for at in members:
        me = me * sizes[at] + lax.axis_index(AXES[at])
    return me


def three_parts(x):
    high = x.astype(BF16)
    rest = x - high.astype(F32)
    middle = rest.astype(BF16)
    low = (rest - middle.astype(F32)).astype(BF16)
    return jnp.concatenate([high.astype(F32), middle.astype(F32), low.astype(F32)], axis=0).astype(BF16)


def select_dot(x, onehot, dims):
    n = x.shape[0]
    out = lax.dot_general(three_parts(x), onehot, (dims, ((), ())), preferred_element_type=F32)
    return (out[:n] + out[n : 2 * n]) + out[2 * n :]


def chosen_columns(map_row, columns):
    rows = lax.broadcasted_iota(jnp.int32, (columns, map_row.shape[1]), 0).astype(F32)
    return jnp.where(rows == map_row, 1.0, 0.0).astype(BF16)


def sides(parts, early):
    if -1 in parts:
        return jnp.where(early, parts[-1], parts[1])
    return parts[1]


def one_side(x, step, distinct, early):
    if not distinct:
        return x
    return jnp.where(early, x, 0.0) if step == -1 else jnp.where(early, 0.0, x)


class Round:
    def __init__(self, grid, sems, at, landed):
        self.grid, self.sems, self.at, self.landed = grid, sems, at, landed

    def copy(self, source, target, shift):
        return pltpu.make_async_remote_copy(
            src_ref=source,
            dst_ref=target,
            send_sem=self.sems.at[self.at, 0],
            recv_sem=self.sems.at[self.at, 1],
            device_id=self.grid.device(shift),
            device_id_type=MESH,
        )

    def send(self, source, target, shift):
        self.shift = shift
        self.copy(source, target, shift).start()

    def all_of_them(self):
        return self.copy(self.landed, self.landed, self.shift)


def lanczos_kernel(*refs, inputs, names):
    hbm, (next_ref, corr_ref, norm_ref) = refs[:inputs], refs[inputs : inputs + 3]
    local = refs[inputs + 3 : 2 * inputs + 3]
    (load_sem, round_sem, ext, work, mine, face, landed, back_raw, back_face, returned, stack, mixed_right, gram_land, row_land, *hvp_scratch) = refs[2 * inputs + 3 :]
    places, basis, ids, counts, kinds, map_x, map_y, map_z, table, w1, w2, b1, b2, fo = local
    h = Scratch(names, hvp_scratch)
    types = table.shape[0]
    atoms = places.shape[2]
    stored = basis.shape[0]
    rows = stack.shape[0]
    pair = 2 * map_x.shape[1]
    grid = Grid()
    sizes = grid.sizes
    entries = 3 * atoms * sizes[0] * sizes[1] * sizes[2]
    planes = plane_offsets()
    groups = reduction_groups()
    count = len(planes)

    partners = set()
    for dy, dz in planes:
        for dx in (-1, 0, 1):
            partners.add(tuple(step % peers for step, peers in zip((dx, dy, dz), sizes)))
    for _, _, shifts in groups:
        partners.update(shifts)
    partners = sorted(partners - {(0, 0, 0)})
    opposite = {tuple(-step % peers for step, peers in zip(shift, sizes)) for shift in partners}
    assert opposite == set(partners)
    barrier = pltpu.get_barrier_semaphore()
    for shift in partners:
        pl.semaphore_signal(barrier, inc=1, device_id=grid.device(shift), device_id_type=MESH)
    loads = [pltpu.make_async_copy(a, b, load_sem.at[at]) for at, (a, b) in enumerate(zip(hbm, local))]
    for at in (0, 1, 5, 6, 7, 2, 3, 4, 8, 9, 10, 11, 12, 13):
        loads[at].start()
    early = lax.broadcasted_iota(jnp.int32, (8, pair), 1) < pair // 2
    line = lax.broadcasted_iota(jnp.int32, (8, pair), 0)
    for at in (0, 1, 5, 6, 7):
        loads[at].wait()
    for c in range(3):
        mine[c : c + 1, :] = places[c]
        mine[3 + c : 4 + c, :] = basis[stored - 1, c]
    map_rows = [jnp.concatenate([m[1:2, :], m[0:1, :]], axis=1).astype(F32) for m in (map_x, map_y, map_z)]
    mine[6:7, :] = map_rows[1]
    mine[7:8, :] = map_rows[2]
    pick_x = chosen_columns(map_rows[0], atoms)
    face[...] = select_dot(mine[...], pick_x, ((1,), (0,)))
    pl.semaphore_wait(barrier, len(partners))

    halo = Round(grid, round_sem, 0, landed)
    for at, (dy, dz) in reversed(list(enumerate(planes))):
        halo.send(face, landed.at[at], (1, -dy, -dz))
        halo.send(face, landed.at[count + at], (-1, -dy, -dz))
        if at:
            halo.send(mine, landed.at[2 * count + at - 1], (0, -dy, -dz))

    stack[rows - 8 :, :] = jnp.zeros((8, 3 * atoms), F32)
    for k in range(stored):
        for c in range(3):
            stack[k : k + 1, c * atoms : (c + 1) * atoms] = basis[k, c]
    gram = dot_full(stack[...], stack[...], ((1,), (1,)))
    gram = jnp.concatenate([gram[r : r + 8] for r in range(0, rows, 8)], axis=1)
    for at in (2, 3, 4, 8, 9, 10, 11, 12, 13):
        loads[at].wait()
    prepare_scatter(h, ids)
    prepare_matrices(h, table, w1, w2, b1, b2, fo)
    halo.all_of_them().wait_recv()

    def shifted(x, row):
        return x + jnp.where(line == row, jnp.where(early, -1.0, 1.0), 0.0)

    raw = {plane: mine[...] if at == 0 else landed[2 * count + at - 1] for at, plane in enumerate(planes)}
    wide = {
        plane: jnp.concatenate([raw[plane], shifted(jnp.where(early, landed[at], landed[count + at]), 0)], axis=1)
        for at, plane in enumerate(planes)
    }
    pick_y, pick_z, wider = {}, {}, {}
    for dz in sorted({dz for _, dz in planes}):
        got = {}
        for dy in (1, -1):
            if (dy, dz) in raw:
                pick_y[dy, dz] = chosen_columns(raw[dy, dz][6:7, :], atoms + pair)
                got[dy] = select_dot(wide[dy, dz], pick_y[dy, dz], ((1,), (0,)))
        wider[dz] = jnp.concatenate([wide[0, dz], shifted(sides(got, early), 1)], axis=1)
    got = {}
    for dz in (1, -1):
        if dz in wider:
            pick_z[dz] = chosen_columns(raw[0, dz][7:8, :], atoms + 2 * pair)
            got[dz] = select_dot(wider[dz], pick_z[dz], ((1,), (0,)))
    ext[:, : atoms + 2 * pair] = wider[0]
    ext[:, atoms + 2 * pair :] = shifted(sides(got, early), 2)

    def gather_from(group, kind, tiles, base, value):
        members, size, shifts = groups[group]
        me = base + place_in(members)
        tiles[me] = value
        around = Round(grid, round_sem, 2 + 2 * group + kind, tiles.at[pl.ds(base, size - 1)])
        for shift in shifts:
            around.send(tiles.at[me], tiles.at[me], shift)
        return around

    def added(tiles, base, size):
        terms = [tiles[base + at] for at in range(size)]
        while len(terms) > 1:
            terms = [sum(terms[at : at + 2][1:], terms[at]) for at in range(0, len(terms), 2)]
        return terms[0]

    rounds = [halo, gather_from(0, 0, gram_land, 0, gram)]

    hessian_product(h, ext, counts, kinds, work, types)

    many_y, many_z = -1 in {dy for dy, _ in planes}, -1 in wider
    back = {0: work[:, : atoms + 2 * pair]}
    for dz in pick_z:
        part = one_side(work[:, atoms + 2 * pair :], dz, many_z, early)
        back[dz] = select_dot(part, pick_z[dz], ((1,), (1,)))
    terms = {(0, dz): x[:, : atoms + pair] for dz, x in back.items()}
    for dy, dz in pick_y:
        part = one_side(back[dz][:, atoms + pair :], dy, many_y, early)
        terms[dy, dz] = select_dot(part, pick_y[dy, dz], ((1,), (1,)))
    back_round = Round(grid, round_sem, 1, returned)
    for at, (dy, dz) in reversed(list(enumerate(planes))):
        back_raw[at] = terms[dy, dz][:, :atoms]
        back_face[at] = terms[dy, dz][:, atoms:]
        back_round.send(back_face.at[at], returned.at[at], (-1, dy, dz))
        back_round.send(back_face.at[at], returned.at[count + at], (1, dy, dz))
        if at:
            back_round.send(back_raw.at[at], returned.at[2 * count + at - 1], (0, dy, dz))

    rounds[-1].all_of_them().wait_recv()
    total = added(gram_land, 0, groups[0][1])
    base = groups[0][1]
    for group in range(1, len(groups)):
        rounds.append(gather_from(group, 0, gram_land, base, total))
        rounds[-1].all_of_them().wait_recv()
        total = added(gram_land, base, groups[group][1])
        base += groups[group][1]
    rounds.append(back_round)
    gram = jnp.concatenate([total[:, r : r + rows] for r in range(0, rows * rows // 8, rows)], axis=0) / entries

    high, low = split(stack[...])
    stack_right = jnp.concatenate([high, high, low], axis=1)
    mixed_right[...] = right_parts(jnp.concatenate([padded(gram, 0, 128), stack[...]], axis=1))
    back_round.all_of_them().wait_recv()
    own, up, low = back_raw[0], returned[0], returned[count]
    for at in range(1, count):
        own = own + returned[2 * count + at - 1]
        up = up + returned[at]
        low = low + returned[count + at]
    own = own + select_dot(jnp.where(early, up, low), pick_x, ((1,), (1,)))
    hv = jnp.concatenate([own[c : c + 1, :] for c in range(3)], axis=1)
    sums = lax.dot_general(
        left_parts(jnp.broadcast_to(hv, (8, 3 * atoms))), stack_right, (((1,), (1,)), ((), ())), preferred_element_type=F32
    )
    lane = lax.broadcasted_iota(jnp.int32, (1, row_land.shape[2]), 1)
    sums = jnp.concatenate([sums[0:1], jnp.zeros((1, row_land.shape[2] - rows), F32)], axis=1)
    sums = jnp.where(lane == stored, jnp.sum(hv * hv, axis=1, keepdims=True), sums)
    base = 0
    for group in range(len(groups)):
        rounds.append(gather_from(group, 1, row_land, base, sums))
        rounds[-1].all_of_them().wait_recv()
        sums = added(row_land, base, groups[group][1])
        base += groups[group][1]
    for around in rounds:
        around.all_of_them().wait_send()
    sums = sums[:, :rows] / entries
    kept = jnp.where(lane[:, :rows] < stored, sums, 0.0)
    mixed = matmul(left_parts(jnp.broadcast_to(kept, (8, rows))), mixed_right[...])[0:1]
    plain = sums[:, stored : stored + 1]
    cross = jnp.sum(mixed[:, :rows] * kept - 2.0 * kept * kept, axis=1, keepdims=True)
    norm = jnp.sqrt(plain + cross + 1e-06)
    norm_ref[...] = norm
    corr_ref[...] = sums[:, :stored]
    for c in range(3):
        part = slice(c * atoms, (c + 1) * atoms)
        next_ref[c] = (hv[:, part] - mixed[:, 128:][:, part]) / norm


def hand_over(*refs):
    count = (len(refs) - 1) // 2
    sems = refs[-1]
    copies = [pltpu.make_async_copy(refs[at], refs[count + at], sems.at[at]) for at in range(count)]
    for copy in copies:
        copy.start()
    for copy in copies:
        copy.wait()


def on_device(positions, basis, neighbours, used_count, kinds, map_x, map_y, map_z,
              table, fit_w1, fit_b1, fit_w2, fit_b2, fit_out):
    atoms = positions.shape[-1]
    width = neighbours.shape[-1]
    stored = basis.shape[0]
    types, levels, m1 = table.shape
    m2 = fit_w1.shape[0] // m1
    pair = 2 * map_x.shape[-1]
    ext = atoms + 3 * pair
    args = [
        positions.reshape(3, 1, atoms),
        basis.reshape(stored, 3, 1, atoms),
        neighbours.reshape(atoms, width),
        used_count.reshape(1, atoms),
        kinds.reshape(1, atoms),
        map_x.reshape(2, -1),
        map_y.reshape(2, -1),
        map_z.reshape(2, -1),
        table,
        fit_w1.T,
        fit_w2,
        fit_b1[None],
        fit_b2[None],
        fit_out[None],
    ]
    rows = (stored + 8) // 8 * 8
    planes = len(plane_offsets())
    groups = reduction_groups()
    slots = sum(count for _, count, _ in groups)
    hvp = hvp_shapes(atoms, width, types, levels, m1, m2, fit_w2.shape[0], ext)
    any_space = pl.BlockSpec(memory_space=pl.ANY)
    vmem = pl.BlockSpec(memory_space=pltpu.VMEM)
    tiles = pltpu.VMEM((planes, 8, pair), F32)
    arrivals = pltpu.VMEM((3 * planes - 1, 8, pair), F32)
    results = pl.pallas_call(
        functools.partial(lanczos_kernel, inputs=len(args), names=tuple(hvp)),
        out_shape=(
            jax.ShapeDtypeStruct((3, 1, atoms), F32),
            jax.ShapeDtypeStruct((1, stored), F32),
            jax.ShapeDtypeStruct((1, 1), F32),
        ),
        in_specs=[any_space] * len(args),
        out_specs=(vmem,) * 3,
        scratch_shapes=[pltpu.VMEM(x.shape, x.dtype) for x in args] + [
            pltpu.SemaphoreType.DMA((len(args),)),
            pltpu.SemaphoreType.DMA((2 + 2 * len(groups), 2)),
            pltpu.VMEM((8, ext), F32),
            pltpu.VMEM((8, ext), F32),
            pltpu.VMEM((8, pair), F32),
            pltpu.VMEM((8, pair), F32),
            arrivals,
            tiles,
            tiles,
            arrivals,
            pltpu.VMEM((rows, 3 * atoms), F32),
            pltpu.VMEM((3 * rows, 128 + 3 * atoms), BF16),
            pltpu.VMEM((slots, 8, rows * rows // 8), F32),
            pltpu.VMEM((slots, 1, 128), F32),
        ] + [pltpu.VMEM(shape, dtype) for shape, dtype in hvp.values()],
        compiler_params=pltpu.CompilerParams(
            collective_id=0, has_side_effects=True, vmem_limit_bytes=60 << 20
        ),
        name="lanczos",
    )(*args)
    results = pl.pallas_call(
        hand_over,
        out_shape=tuple(jax.ShapeDtypeStruct(x.shape, x.dtype) for x in results),
        in_specs=[any_space] * 3,
        out_specs=(any_space,) * 3,
        scratch_shapes=[pltpu.SemaphoreType.DMA((3,))],
        name="hand_over",
    )(*results)
    next_vector, correlations, norm = results
    return next_vector.reshape(positions.shape), correlations.reshape(stored), norm.reshape(())


def solution(mesh):
    placed = (
        P(None, "gx", "gy", "gz", None),
        P(None, None, "gx", "gy", "gz", None),
        P("gx", "gy", "gz", None, None),
        P("gx", "gy", "gz", None),
        P("gx", "gy", "gz", None),
        P("gx", "gy", "gz", None, None),
        P("gx", "gy", "gz", None, None),
        P("gx", "gy", "gz", None, None),
        P(),
        P(),
        P(),
        P(),
        P(),
        P(),
    )
    return jax.shard_map(
        on_device,
        mesh=mesh,
        in_specs=placed,
        out_specs=(P(None, "gx", "gy", "gz", None), P(), P()),
        check_vma=False,
    )
```

```python
import functools

import jax
import jax.numpy as jnp
from jax import lax
from jax.experimental import pallas as pl
from jax.experimental.pallas import tpu as pltpu
from jax.sharding import PartitionSpec as P

F32, BF16 = jnp.float32, jnp.bfloat16
HIGHEST = lax.Precision.HIGHEST
CHUNK = 8
DIGIT = 64


def split(x):
    high = x.astype(BF16)
    return high, (x - high.astype(F32)).astype(BF16)


def left_parts(x):
    high, low = split(x)
    return jnp.concatenate([high, low, high], axis=1)


def right_parts(x):
    high, low = split(x)
    return jnp.concatenate([high, high, low], axis=0)


def matmul(a, b):
    return lax.dot_general(a, b, (((1,), (0,)), ((), ())), preferred_element_type=F32)


def dot_full(a, b, dims):
    return lax.dot_general(a, b, (dims, ((), ())), precision=HIGHEST, preferred_element_type=F32)


def padded(x, rows, columns):
    if columns > x.shape[1]:
        x = jnp.concatenate([x, jnp.zeros((x.shape[0], columns - x.shape[1]), x.dtype)], axis=1)
    if rows > x.shape[0]:
        x = jnp.concatenate([x, jnp.zeros((rows - x.shape[0], x.shape[1]), x.dtype)], axis=0)
    return x


def up_to(n, step):
    return (n + step - 1) // step * step


def hvp_shapes(atoms, width, types, levels, m1, m2, fit, ext):
    fit_wide, m1_wide = up_to(fit, 128), up_to(m1, 128)
    low = levels * m2
    return dict(
        idt=((width, atoms), jnp.int32),
        onehot=((width // CHUNK, DIGIT, CHUNK * atoms), BF16),
        in_bank=((width, ext // DIGIT, atoms), F32),
        w1_rows=((fit_wide // 128, m1_wide * m2, 128), F32),
        w1_low=((fit_wide // 128, types * low, 128), F32),
        low_right=((types * fit, 3 * low), BF16),
        low_left=((types * low, 3 * fit_wide), BF16),
        w2_right=((fit, 3 * fit_wide), BF16),
        w2_left=((fit, 3 * fit_wide), BF16),
        columns=((fit, 8), F32),
        lead_up=((types * m2, 3 * levels), BF16),
        lead_down=((types * levels, 3 * m2), BF16),
        dv=((6, width + CHUNK, atoms), F32),
        radial=((5, width + CHUNK, atoms), F32),
        mix=((9, width + CHUNK, atoms), F32),
        gauss=((levels, 3, width + CHUNK, atoms), F32),
        pooled=((8, levels, atoms), F32),
        product=((low, 2 * atoms), F32),
        pulled=((low, 2 * atoms), F32),
        gp=((levels, 8 * atoms), F32),
        forces=((6, width + CHUNK, atoms), F32),
    )


def prepare_matrices(h, table_ref, w1_ref, w2_ref, b1_ref, b2_ref, fo_ref):
    types, levels, m1 = table_ref.shape
    fit, m2 = w1_ref.shape[0], w1_ref.shape[1] // m1
    halves, rows, _ = h.w1_rows.shape
    m1_wide, low = rows // m2, levels * m2
    turned = padded(w1_ref[...], halves * 128, 0).T
    tables = jnp.concatenate([padded(table_ref[t], 0, m1_wide) for t in range(types)], axis=0)
    tables = left_parts(tables)
    for half in range(halves):
        h.w1_rows[half, : m1 * m2, :] = turned[:, half * 128 : (half + 1) * 128]
        h.w1_rows[half, m1 * m2 :, :] = jnp.zeros((rows - m1 * m2, 128), F32)
    for n in range(m2):
        part = [h.w1_rows[half, pl.ds(n, m1_wide, stride=m2), :] for half in range(halves)]
        out = matmul(tables, right_parts(jnp.concatenate(part, axis=1)))
        for half in range(halves):
            h.w1_low[half, pl.ds(n, types * levels, stride=m2), :] = out[:, half * 128 : (half + 1) * 128]
    for t in range(types):
        at = slice(t * low, (t + 1) * low)
        mine = jnp.concatenate([h.w1_low[half, at, :] for half in range(halves)], axis=1)
        h.low_left[at, :] = left_parts(mine)
        h.low_right[t * fit : (t + 1) * fit, :] = left_parts(mine.T[:fit])
    w2 = padded(w2_ref[...], halves * 128, halves * 128)
    h.w2_left[...] = left_parts(w2[:fit])
    h.w2_right[...] = left_parts(w2.T[:fit])
    lines = jnp.concatenate([b1_ref[...], b2_ref[...], fo_ref[...], jnp.zeros((5, fit), F32)], axis=0)
    h.columns[...] = dot_full(lines, identity(8), ((0,), (0,)))
    for t in range(types):
        first = table_ref[t][:, :m2]
        h.lead_down[t * levels : (t + 1) * levels, :] = left_parts(first)
        h.lead_up[t * m2 : (t + 1) * m2, :] = left_parts(dot_full(first, identity(levels), ((0,), (0,))))


def identity(n):
    same = lax.broadcasted_iota(jnp.int32, (n, n), 0) == lax.broadcasted_iota(jnp.int32, (n, n), 1)
    return jnp.where(same, 1.0, 0.0).astype(F32)


def prepare_scatter(h, ids_ref):
    width, atoms = h.idt.shape
    h.idt[...] = ids_ref[...].T
    group = lax.broadcasted_iota(jnp.int32, h.in_bank.shape[1:], 0)
    column = lax.broadcasted_iota(jnp.int32, (DIGIT, atoms), 0)

    def one(c, carry):
        idx = h.idt[pl.ds(pl.multiple_of(c * CHUNK, CHUNK), CHUNK), :]
        digit = jnp.bitwise_and(idx, DIGIT - 1)
        bank = jnp.right_shift(idx, DIGIT.bit_length() - 1)
        for r in range(CHUNK):
            h.in_bank[c * CHUNK + r] = jnp.where(bank[r : r + 1, :] == group, 1.0, 0.0).astype(F32)
            hit = jnp.where(digit[r : r + 1, :] == column, 1.0, 0.0)
            h.onehot[c, :, r * atoms : (r + 1) * atoms] = hit.astype(BF16)
        return carry

    lax.fori_loop(0, width // CHUNK, one, 0)


def pair_terms(h, ext_ref, counts):
    width, atoms = h.idt.shape
    levels = h.gauss.shape[0]
    banks = ext_ref.shape[1] // 128
    top = float(levels - 1)

    def one(c, carry):
        first = pl.multiple_of(c * CHUNK, CHUNK)
        here = pl.ds(first, CHUNK)
        idx = h.idt[here, :]
        lane = jnp.bitwise_and(idx, 127)
        bank = jnp.right_shift(idx, 7)
        fields = []
        for f in range(6):
            got = None
            for b in range(banks):
                row = jnp.broadcast_to(ext_ref[f : f + 1, b * 128 : (b + 1) * 128], (CHUNK, 128))
                part = jnp.take_along_axis(row, lane, axis=1, mode="promise_in_bounds")
                got = part if got is None else jnp.where(bank == b, part, got)
            got = got - ext_ref[f : f + 1, :atoms]
            h.dv[f, here, :] = got
            fields.append(got)
        d, v = fields[:3], fields[3:]
        slot = lax.broadcasted_iota(jnp.int32, (CHUNK, atoms), 0) + first
        q = d[0] * d[0] + d[1] * d[1] + d[2] * d[2]
        qd = 2.0 * (d[0] * v[0] + d[1] * v[1] + d[2] * v[2])
        w = 1.0 / (q + 0.01)
        decay = jnp.where(slot < counts, jnp.exp(-q), 0.0)
        s = decay * jnp.sqrt(w)
        u = decay * w
        s_q = -s * (1.0 + 0.5 * w)
        u_q = -u * (1.0 + w)
        shrink = 1.0 / (1.0 + s)
        for at, value in enumerate((qd, w, s, u, shrink)):
            h.radial[at, here, :] = value
        step = s_q * qd
        for at, value in enumerate(
            [-2.0 * top * shrink * shrink * step]
            + [s] + [u * e for e in d]
            + [step] + [u_q * qd * d[e] + u * v[e] for e in range(3)]
        ):
            h.mix[at, here, :] = value
        scaled = s * shrink * top
        for k in range(levels):
            y = scaled - float(k)
            phi = jnp.exp(-(y * y))
            psi = y * phi
            h.gauss[k, 0, here, :] = phi
            h.gauss[k, 1, here, :] = psi
            h.gauss[k, 2, here, :] = y * psi
        return carry

    lax.fori_loop(0, width // CHUNK, one, 0, unroll=8)


def pooled_terms(h):
    width, atoms = h.idt.shape
    levels = h.gauss.shape[0]
    together = 2
    zero = jnp.zeros((CHUNK, atoms), F32)
    for k0 in range(0, levels, together):

        def one(c, acc):
            here = slice(c * CHUNK, (c + 1) * CHUNK)
            slope = h.mix[0, here, :]
            r = [h.mix[1 + a, here, :] for a in range(4)]
            dr = [h.mix[5 + a, here, :] for a in range(4)]
            out = []
            for k in range(together):
                phi = h.gauss[k0 + k, 0, here, :]
                psi = h.gauss[k0 + k, 1, here, :] * slope
                out += [acc[8 * k + a] + phi * r[a] for a in range(4)]
                out += [acc[8 * k + 4 + a] + (phi * dr[a] + psi * r[a]) for a in range(4)]
            return tuple(out)

        acc = (zero,) * (8 * together)
        for c in range(width // CHUNK):
            acc = one(c, acc)
        for k in range(together):
            for a in range(8):
                h.pooled[a, k0 + k : k0 + k + 1, :] = jnp.sum(acc[8 * k + a], axis=0, keepdims=True) / width


def of_kind(kinds, rows):
    types = len(kinds)
    step = rows.shape[0] // types
    out = rows[:step]
    for t in range(1, types):
        out = jnp.where(kinds[t], rows[t * step : (t + 1) * step], out)
    return out


def lanes_of(x, count, atoms):
    return [x[:, a * atoms : (a + 1) * atoms] for a in range(count)]


def fitting_net(h, kinds_ref, types):
    fit = h.columns.shape[0]
    fit_wide = h.w2_left.shape[1] // 3
    levels = h.pooled.shape[1]
    m2 = h.lead_up.shape[0] // types
    width, atoms = h.idt.shape
    kinds2 = jnp.concatenate([kinds_ref[...]] * 2, axis=1)
    kinds8 = jnp.concatenate([kinds2] * 4, axis=1)
    kinds2 = [kinds2 == t for t in range(types)]
    kinds8 = [kinds8 == t for t in range(types)]
    pooled = jnp.concatenate([h.pooled[a] for a in range(8)], axis=1)
    lead = lanes_of(of_kind(kinds8, matmul(h.lead_up[...], right_parts(pooled))), 8, atoms)
    for k in range(levels):
        rows = [h.pooled[a, k : k + 1, :] for a in range(8)]
        plain = rows[0] * lead[0]
        moved = rows[4] * lead[0] + rows[0] * lead[4]
        for a in range(1, 4):
            plain += rows[a] * lead[a]
            moved += rows[4 + a] * lead[a] + rows[a] * lead[4 + a]
        h.product[k * m2 : (k + 1) * m2, :atoms] = plain
        h.product[k * m2 : (k + 1) * m2, atoms:] = moved
    z1 = of_kind(kinds2, matmul(h.low_right[...], right_parts(h.product[...])))
    b1, b2, fo = h.columns[:, 0:1], h.columns[:, 1:2], h.columns[:, 2:3]
    h1 = jnp.tanh(z1[:, :atoms] + b1)
    gate1 = 1.0 - h1 * h1
    dh1 = gate1 * z1[:, atoms:]
    z2 = matmul(h.w2_right[...], right_parts(padded(jnp.concatenate([h1, dh1], axis=1), fit_wide, 0)))
    t2 = jnp.tanh(z2[:, :atoms] + b2)
    gate2 = 1.0 - t2 * t2
    dt2 = gate2 * z2[:, atoms:]
    gz2 = jnp.concatenate([fo * gate2, fo * (-2.0 * t2 * dt2)], axis=1)
    gh = matmul(h.w2_left[...], right_parts(padded(gz2, fit_wide, 0)))
    gh1 = gh[:, :atoms] + fo
    gz1 = jnp.concatenate([gh1 * gate1, gh[:, atoms:] * gate1 - 2.0 * gh1 * h1 * dh1], axis=1)
    h.pulled[...] = of_kind(kinds2, matmul(h.low_left[...], right_parts(padded(gz1, fit_wide, 0))))
    acc = [jnp.zeros((m2, atoms), F32) for _ in range(8)]
    for k in range(levels):
        g = h.pulled[k * m2 : (k + 1) * m2, :atoms]
        dg = h.pulled[k * m2 : (k + 1) * m2, atoms:]
        rows = [h.pooled[a, k : k + 1, :] for a in range(8)]
        for a in range(4):
            straight = jnp.sum(g * lead[a], axis=0, keepdims=True)
            turned = jnp.sum(dg * lead[a] + g * lead[4 + a], axis=0, keepdims=True)
            h.gp[k : k + 1, a * atoms : (a + 1) * atoms] = straight
            h.gp[k : k + 1, (4 + a) * atoms : (5 + a) * atoms] = turned
            acc[a] = acc[a] + g * rows[a]
            acc[4 + a] = acc[4 + a] + (dg * rows[a] + g * rows[4 + a])
    across = of_kind(kinds8, matmul(h.lead_down[...], right_parts(jnp.concatenate(acc, axis=1))))
    h.gp[...] = (h.gp[...] + across) / width


def pair_forces(h, out_ref):
    width, atoms = h.idt.shape
    levels = h.gauss.shape[0]
    banks = h.in_bank.shape[1]
    top = float(levels - 1)

    def force_of(c, centre):
        first = pl.multiple_of(c * CHUNK, CHUNK)
        here = pl.ds(first, CHUNK)
        zero = jnp.zeros((CHUNK, atoms), F32)
        s0, s1, s2, e0, e1 = ([zero] * 4 for _ in range(5))
        for k in range(levels):
            phi, psi, chi = (h.gauss[k, p, here, :] for p in range(3))
            for a in range(4):
                g = h.gp[k : k + 1, a * atoms : (a + 1) * atoms]
                gd = h.gp[k : k + 1, (4 + a) * atoms : (5 + a) * atoms]
                s0[a] = s0[a] + g * phi
                s1[a] = s1[a] + g * psi
                s2[a] = s2[a] + g * chi
                e0[a] = e0[a] + gd * phi
                e1[a] = e1[a] + gd * psi
        d = [h.dv[f, here, :] for f in range(3)]
        v = [h.dv[f, here, :] for f in range(3, 6)]
        qd, w, s, u, shrink = (h.radial[at, here, :] for at in range(5))
        s_q = -s * (1.0 + 0.5 * w)
        u_q = -u * (1.0 + w)
        t_s = shrink * shrink
        t_q = t_s * s_q
        s_qq = -s_q * (1.0 + 0.5 * w) + 0.5 * s * w * w
        u_qq = -u_q * (1.0 + w) + u * w * w
        t_qq = -2.0 * t_s * shrink * s_q * s_q + t_s * s_qq
        step = t_q * qd
        val = s0
        val_t = [-2.0 * top * e for e in s1]
        val_tt = [top * top * (4.0 * s2[a] - 2.0 * s0[a]) for a in range(4)]
        dval = [e0[a] + val_t[a] * step for a in range(4)]
        dval_t = [-2.0 * top * e1[a] + val_tt[a] * step for a in range(4)]
        big = val[1] * d[0] + val[2] * d[1] + val[3] * d[2]
        big_t = val_t[1] * d[0] + val_t[2] * d[1] + val_t[3] * d[2]
        dbig = sum(dval[1 + e] * d[e] + val[1 + e] * v[e] for e in range(3))
        dbig_t = sum(dval_t[1 + e] * d[e] + val_t[1 + e] * v[e] for e in range(3))
        flow = val_t[0] * s + big_t * u
        kern = t_q * flow + val[0] * s_q + big * u_q
        dkern = (
            t_q * (dval_t[0] * s + dbig_t * u)
            + dval[0] * s_q
            + dbig * u_q
            + qd * (t_qq * flow + t_q * (val_t[0] * s_q + big_t * u_q) + val[0] * s_qq + big * u_qq)
        )
        du = u_q * qd
        out = []
        for e in range(3):
            force = 2.0 * (v[e] * kern + d[e] * dkern) + du * val[1 + e] + u * dval[1 + e]
            high = force.astype(BF16).astype(F32)
            h.forces[e, here, :] = high
            h.forces[3 + e, here, :] = force - high
            out.append(centre[e] - force)
        return tuple(out)

    zero = jnp.zeros((CHUNK, atoms), F32)
    def scatter(first, chunks):
        lefts = []
        for n in range(first * CHUNK, (first + chunks) * CHUNK):
            mine = h.in_bank[n]
            lefts.append(jnp.concatenate([h.forces[e, n : n + 1, :] * mine for e in range(6)], axis=0).astype(BF16))
        right = jnp.concatenate([h.onehot[first + j] for j in range(chunks)], axis=1)
        return lax.dot_general(
            jnp.concatenate(lefts, axis=1), right, (((1,), (1,)), ((), ())), preferred_element_type=F32
        )

    chunks = width // CHUNK
    centre = (zero,) * 3
    acc = None
    for piece in range(4):
        if piece:
            part = scatter((piece - 1) * chunks // 4, chunks // 4)
            acc = part if acc is None else acc + part
        for c in range(piece * chunks // 4, (piece + 1) * chunks // 4):
            centre = force_of(c, centre)
    acc = acc + scatter(3 * chunks // 4, chunks // 4)
    per = 128 // DIGIT
    out_ref[3:, :] = jnp.zeros((out_ref.shape[0] - 3, out_ref.shape[1]), F32)
    for e in range(3):
        part = acc[banks * e : banks * (e + 1)] + acc[banks * (3 + e) : banks * (4 + e)]
        for b in range(0, banks, per):
            row = jnp.concatenate([part[j : j + 1] for j in range(b, b + per)], axis=1)
            if b == 0:
                row = row + jnp.sum(centre[e], axis=0, keepdims=True)
            out_ref[e : e + 1, b * DIGIT : (b + per) * DIGIT] = row


class Scratch:
    def __init__(self, names, refs):
        for name, ref in zip(names, refs, strict=True):
            setattr(self, name, ref)


AXES = ("gx", "gy", "gz")
MESH = pl.DeviceIdType.MESH
GROUP_LIMIT = 32


def sizes_of():
    return [lax.axis_size(axis) for axis in AXES]


def plane_offsets():
    def along(size):
        return (0, 1) if size == 2 else (0, 1, -1)

    _, ny, nz = sizes_of()
    return [(dy, dz) for dz in along(nz) for dy in along(ny)]


class Grid:
    def __init__(self):
        self.sizes = sizes_of()
        self.along = []
        for axis, peers in zip(AXES, self.sizes):
            me = lax.axis_index(axis)
            self.along.append([me] + [lax.rem(me + step, peers) for step in range(1, peers)])

    def device(self, shift):
        return {
            axis: row[step % peers] for axis, row, step, peers in zip(AXES, self.along, shift, self.sizes)
        }


def reduction_groups():
    sizes = sizes_of()
    groups = []
    for at in range(3):
        if groups and groups[-1][1] * sizes[at] <= GROUP_LIMIT:
            groups[-1] = (groups[-1][0] + [at], groups[-1][1] * sizes[at])
        else:
            groups.append(([at], sizes[at]))
    out = []
    for members, count in groups:
        shifts = [[0, 0, 0]]
        for at in members:
            shifts = [s[:at] + [step] + s[at + 1 :] for s in shifts for step in range(sizes[at])]
        out.append((members, count, [tuple(s) for s in shifts if any(s)]))
    return out


def place_in(members):
    sizes = sizes_of()
    me = 0
    for at in members:
        me = me * sizes[at] + lax.axis_index(AXES[at])
    return me


def three_parts(x):
    high = x.astype(BF16)
    rest = x - high.astype(F32)
    middle = rest.astype(BF16)
    low = (rest - middle.astype(F32)).astype(BF16)
    return jnp.concatenate([high.astype(F32), middle.astype(F32), low.astype(F32)], axis=0).astype(BF16)


def select_dot(x, onehot, dims):
    n = x.shape[0]
    out = lax.dot_general(three_parts(x), onehot, (dims, ((), ())), preferred_element_type=F32)
    return (out[:n] + out[n : 2 * n]) + out[2 * n :]


def chosen_columns(map_row, columns):
    rows = lax.broadcasted_iota(jnp.int32, (columns, map_row.shape[1]), 0).astype(F32)
    return jnp.where(rows == map_row, 1.0, 0.0).astype(BF16)


def sides(parts, early):
    if -1 in parts:
        return jnp.where(early, parts[-1], parts[1])
    return parts[1]


def one_side(x, step, distinct, early):
    if not distinct:
        return x
    return jnp.where(early, x, 0.0) if step == -1 else jnp.where(early, 0.0, x)


class Round:
    def __init__(self, grid, sems, at, landed):
        self.grid, self.sems, self.at, self.landed = grid, sems, at, landed

    def copy(self, source, target, shift):
        return pltpu.make_async_remote_copy(
            src_ref=source,
            dst_ref=target,
            send_sem=self.sems.at[self.at, 0],
            recv_sem=self.sems.at[self.at, 1],
            device_id=self.grid.device(shift),
            device_id_type=MESH,
        )

    def send(self, source, target, shift):
        self.shift = shift
        self.copy(source, target, shift).start()

    def all_of_them(self):
        return self.copy(self.landed, self.landed, self.shift)


def lanczos_kernel(*refs, inputs, names):
    hbm, (next_ref, corr_ref, norm_ref) = refs[:inputs], refs[inputs : inputs + 3]
    local = refs[inputs + 3 : 2 * inputs + 3]
    (load_sem, round_sem, ext, work, mine, face, landed, back_raw, back_face, returned, stack, mixed_right, gram_land, row_land, *hvp_scratch) = refs[2 * inputs + 3 :]
    places, basis, ids, counts, kinds, map_x, map_y, map_z, table, w1, w2, b1, b2, fo = local
    h = Scratch(names, hvp_scratch)
    types = table.shape[0]
    atoms = places.shape[2]
    stored = basis.shape[0]
    rows = stack.shape[0]
    pair = 2 * map_x.shape[1]
    grid = Grid()
    sizes = grid.sizes
    entries = 3 * atoms * sizes[0] * sizes[1] * sizes[2]
    planes = plane_offsets()
    groups = reduction_groups()
    count = len(planes)

    partners = set()
    for dy, dz in planes:
        for dx in (-1, 0, 1):
            partners.add(tuple(step % peers for step, peers in zip((dx, dy, dz), sizes)))
    for _, _, shifts in groups:
        partners.update(shifts)
    partners = sorted(partners - {(0, 0, 0)})
    opposite = {tuple(-step % peers for step, peers in zip(shift, sizes)) for shift in partners}
    assert opposite == set(partners)
    barrier = pltpu.get_barrier_semaphore()
    for shift in partners:
        pl.semaphore_signal(barrier, inc=1, device_id=grid.device(shift), device_id_type=MESH)
    loads = [pltpu.make_async_copy(a, b, load_sem.at[at]) for at, (a, b) in enumerate(zip(hbm, local))]
    for at in (0, 1, 5, 6, 7, 2, 3, 4, 8, 9, 10, 11, 12, 13):
        loads[at].start()
    early = lax.broadcasted_iota(jnp.int32, (8, pair), 1) < pair // 2
    line = lax.broadcasted_iota(jnp.int32, (8, pair), 0)
    for at in (0, 1, 5, 6, 7):
        loads[at].wait()
    for c in range(3):
        mine[c : c + 1, :] = places[c]
        mine[3 + c : 4 + c, :] = basis[stored - 1, c]
    map_rows = [jnp.concatenate([m[1:2, :], m[0:1, :]], axis=1).astype(F32) for m in (map_x, map_y, map_z)]
    mine[6:7, :] = map_rows[1]
    mine[7:8, :] = map_rows[2]
    pick_x = chosen_columns(map_rows[0], atoms)
    face[...] = select_dot(mine[...], pick_x, ((1,), (0,)))
    returned[...] = jnp.zeros_like(returned)
    pl.semaphore_wait(barrier, len(partners))

    halo = Round(grid, round_sem, 0, landed)
    for at, (dy, dz) in reversed(list(enumerate(planes))):
        halo.send(face, landed.at[at], (1, -dy, -dz))
        halo.send(face, landed.at[count + at], (-1, -dy, -dz))
        if at:
            halo.send(mine, landed.at[2 * count + at - 1], (0, -dy, -dz))

    stack[rows - 8 :, :] = jnp.zeros((8, 3 * atoms), F32)
    for k in range(stored):
        for c in range(3):
            stack[k : k + 1, c * atoms : (c + 1) * atoms] = basis[k, c]
    gram = dot_full(stack[...], stack[...], ((1,), (1,)))
    gram = jnp.concatenate([gram[r : r + 8] for r in range(0, rows, 8)], axis=1)
    for at in (2, 3, 4, 8, 9, 10, 11, 12, 13):
        loads[at].wait()
    prepare_scatter(h, ids)
    prepare_matrices(h, table, w1, w2, b1, b2, fo)
    halo.all_of_them().wait_recv()

    def shifted(x, row):
        return x + jnp.where(line == row, jnp.where(early, -1.0, 1.0), 0.0)

    raw = {plane: mine[...] if at == 0 else landed[2 * count + at - 1] for at, plane in enumerate(planes)}
    wide = {
        plane: jnp.concatenate([raw[plane], shifted(jnp.where(early, landed[at], landed[count + at]), 0)], axis=1)
        for at, plane in enumerate(planes)
    }
    pick_y, pick_z, wider = {}, {}, {}
    for dz in sorted({dz for _, dz in planes}):
        got = {}
        for dy in (1, -1):
            if (dy, dz) in raw:
                pick_y[dy, dz] = chosen_columns(raw[dy, dz][6:7, :], atoms + pair)
                got[dy] = select_dot(wide[dy, dz], pick_y[dy, dz], ((1,), (0,)))
        wider[dz] = jnp.concatenate([wide[0, dz], shifted(sides(got, early), 1)], axis=1)
    got = {}
    for dz in (1, -1):
        if dz in wider:
            pick_z[dz] = chosen_columns(raw[0, dz][7:8, :], atoms + 2 * pair)
            got[dz] = select_dot(wider[dz], pick_z[dz], ((1,), (0,)))
    ext[:, : atoms + 2 * pair] = wider[0]
    ext[:, atoms + 2 * pair :] = shifted(sides(got, early), 2)

    def gather_from(group, kind, tiles, base, value):
        members, size, shifts = groups[group]
        me = base + place_in(members)
        tiles[me] = value
        around = Round(grid, round_sem, 2 + 2 * group + kind, tiles.at[pl.ds(base, size - 1)])
        for shift in shifts:
            around.send(tiles.at[me], tiles.at[me], shift)
        return around

    def added(tiles, base, size):
        terms = [tiles[base + at] for at in range(size)]
        while len(terms) > 1:
            terms = [sum(terms[at : at + 2][1:], terms[at]) for at in range(0, len(terms), 2)]
        return terms[0]

    pair_terms(h, ext, counts[...])
    rounds = [halo, gather_from(0, 0, gram_land, 0, gram)]
    pooled_terms(h)
    fitting_net(h, kinds, types)
    pair_forces(h, work)

    many_y, many_z = -1 in {dy for dy, _ in planes}, -1 in wider
    back = {0: work[:, : atoms + 2 * pair]}
    for dz in pick_z:
        part = one_side(work[:, atoms + 2 * pair :], dz, many_z, early)
        back[dz] = select_dot(part, pick_z[dz], ((1,), (1,)))
    terms = {(0, dz): x[:, : atoms + pair] for dz, x in back.items()}
    for dy, dz in pick_y:
        part = one_side(back[dz][:, atoms + pair :], dy, many_y, early)
        terms[dy, dz] = select_dot(part, pick_y[dy, dz], ((1,), (1,)))
    lead = pl.ds(0, 3)
    back_round = Round(grid, round_sem, 1, returned.at[:, lead])
    for at, (dy, dz) in reversed(list(enumerate(planes))):
        back_raw[at] = terms[dy, dz][:, :atoms]
        back_face[at] = terms[dy, dz][:, atoms:]
        back_round.send(back_face.at[at, lead], returned.at[at, lead], (-1, dy, dz))
        back_round.send(back_face.at[at, lead], returned.at[count + at, lead], (1, dy, dz))
        if at:
            back_round.send(back_raw.at[at, lead], returned.at[2 * count + at - 1, lead], (0, dy, dz))

    rounds[-1].all_of_them().wait_recv()
    total = added(gram_land, 0, groups[0][1])
    base = groups[0][1]
    for group in range(1, len(groups)):
        rounds.append(gather_from(group, 0, gram_land, base, total))
        rounds[-1].all_of_them().wait_recv()
        total = added(gram_land, base, groups[group][1])
        base += groups[group][1]
    rounds.append(back_round)
    gram = jnp.concatenate([total[:, r : r + rows] for r in range(0, rows * rows // 8, rows)], axis=0) / entries

    high, low = split(stack[...])
    stack_right = jnp.concatenate([high, high, low], axis=1)
    mixed_right[...] = right_parts(jnp.concatenate([padded(gram, 0, 128), stack[...]], axis=1))
    back_round.all_of_them().wait_recv()
    own, up, low = back_raw[0], returned[0], returned[count]
    for at in range(1, count):
        own = own + returned[2 * count + at - 1]
        up = up + returned[at]
        low = low + returned[count + at]
    own = own + select_dot(jnp.where(early, up, low), pick_x, ((1,), (1,)))
    hv = jnp.concatenate([own[c : c + 1, :] for c in range(3)], axis=1)
    sums = lax.dot_general(
        left_parts(jnp.broadcast_to(hv, (8, 3 * atoms))), stack_right, (((1,), (1,)), ((), ())), preferred_element_type=F32
    )
    lane = lax.broadcasted_iota(jnp.int32, (1, row_land.shape[2]), 1)
    sums = jnp.concatenate([sums[0:1], jnp.zeros((1, row_land.shape[2] - rows), F32)], axis=1)
    sums = jnp.where(lane == stored, jnp.sum(hv * hv, axis=1, keepdims=True), sums)
    base = 0
    for group in range(len(groups)):
        rounds.append(gather_from(group, 1, row_land, base, sums))
        rounds[-1].all_of_them().wait_recv()
        sums = added(row_land, base, groups[group][1])
        base += groups[group][1]
    for around in rounds:
        around.all_of_them().wait_send()
    sums = sums[:, :rows] / entries
    kept = jnp.where(lane[:, :rows] < stored, sums, 0.0)
    mixed = matmul(left_parts(jnp.broadcast_to(kept, (8, rows))), mixed_right[...])[0:1]
    plain = sums[:, stored : stored + 1]
    cross = jnp.sum(mixed[:, :rows] * kept - 2.0 * kept * kept, axis=1, keepdims=True)
    norm = jnp.sqrt(plain + cross + 1e-06)
    norm_ref[...] = norm
    corr_ref[...] = sums[:, :stored]
    for c in range(3):
        part = slice(c * atoms, (c + 1) * atoms)
        next_ref[c] = (hv[:, part] - mixed[:, 128:][:, part]) / norm


def hand_over(*refs):
    count = (len(refs) - 1) // 2
    sems = refs[-1]
    copies = [pltpu.make_async_copy(refs[at], refs[count + at], sems.at[at]) for at in range(count)]
    for copy in copies:
        copy.start()
    for copy in copies:
        copy.wait()


def on_device(positions, basis, neighbours, used_count, kinds, map_x, map_y, map_z,
              table, fit_w1, fit_b1, fit_w2, fit_b2, fit_out):
    atoms = positions.shape[-1]
    width = neighbours.shape[-1]
    stored = basis.shape[0]
    types, levels, m1 = table.shape
    m2 = fit_w1.shape[0] // m1
    pair = 2 * map_x.shape[-1]
    ext = atoms + 3 * pair
    args = [
        positions.reshape(3, 1, atoms),
        basis.reshape(stored, 3, 1, atoms),
        neighbours.reshape(atoms, width),
        used_count.reshape(1, atoms),
        kinds.reshape(1, atoms),
        map_x.reshape(2, -1),
        map_y.reshape(2, -1),
        map_z.reshape(2, -1),
        table,
        fit_w1.T,
        fit_w2,
        fit_b1[None],
        fit_b2[None],
        fit_out[None],
    ]
    rows = (stored + 8) // 8 * 8
    planes = len(plane_offsets())
    groups = reduction_groups()
    slots = sum(count for _, count, _ in groups)
    hvp = hvp_shapes(atoms, width, types, levels, m1, m2, fit_w2.shape[0], ext)
    any_space = pl.BlockSpec(memory_space=pl.ANY)
    vmem = pl.BlockSpec(memory_space=pltpu.VMEM)
    tiles = pltpu.VMEM((planes, 8, pair), F32)
    arrivals = pltpu.VMEM((3 * planes - 1, 8, pair), F32)
    results = pl.pallas_call(
        functools.partial(lanczos_kernel, inputs=len(args), names=tuple(hvp)),
        out_shape=(
            jax.ShapeDtypeStruct((3, 1, atoms), F32),
            jax.ShapeDtypeStruct((1, stored), F32),
            jax.ShapeDtypeStruct((1, 1), F32),
        ),
        in_specs=[any_space] * len(args),
        out_specs=(vmem,) * 3,
        scratch_shapes=[pltpu.VMEM(x.shape, x.dtype) for x in args] + [
            pltpu.SemaphoreType.DMA((len(args),)),
            pltpu.SemaphoreType.DMA((2 + 2 * len(groups), 2)),
            pltpu.VMEM((8, ext), F32),
            pltpu.VMEM((8, ext), F32),
            pltpu.VMEM((8, pair), F32),
            pltpu.VMEM((8, pair), F32),
            arrivals,
            tiles,
            tiles,
            arrivals,
            pltpu.VMEM((rows, 3 * atoms), F32),
            pltpu.VMEM((3 * rows, 128 + 3 * atoms), BF16),
            pltpu.VMEM((slots, 8, rows * rows // 8), F32),
            pltpu.VMEM((slots, 1, 128), F32),
        ] + [pltpu.VMEM(shape, dtype) for shape, dtype in hvp.values()],
        compiler_params=pltpu.CompilerParams(
            collective_id=0, has_side_effects=True, vmem_limit_bytes=60 << 20
        ),
        name="lanczos",
    )(*args)
    results = pl.pallas_call(
        hand_over,
        out_shape=tuple(jax.ShapeDtypeStruct(x.shape, x.dtype) for x in results),
        in_specs=[any_space] * 3,
        out_specs=(any_space,) * 3,
        scratch_shapes=[pltpu.SemaphoreType.DMA((3,))],
        name="hand_over",
    )(*results)
    next_vector, correlations, norm = results
    return next_vector.reshape(positions.shape), correlations.reshape(stored), norm.reshape(())


def solution(mesh):
    placed = (
        P(None, "gx", "gy", "gz", None),
        P(None, None, "gx", "gy", "gz", None),
        P("gx", "gy", "gz", None, None),
        P("gx", "gy", "gz", None),
        P("gx", "gy", "gz", None),
        P("gx", "gy", "gz", None, None),
        P("gx", "gy", "gz", None, None),
        P("gx", "gy", "gz", None, None),
        P(),
        P(),
        P(),
        P(),
        P(),
        P(),
    )
    return jax.shard_map(
        on_device,
        mesh=mesh,
        in_specs=placed,
        out_specs=(P(None, "gx", "gy", "gz", None), P(), P()),
        check_vma=False,
    )
```

```python
import functools

import jax
import jax.numpy as jnp
from jax import lax
from jax.experimental import pallas as pl
from jax.experimental.pallas import tpu as pltpu
from jax.sharding import PartitionSpec as P

F32, BF16 = jnp.float32, jnp.bfloat16
HIGHEST = lax.Precision.HIGHEST
CHUNK = 8
DIGIT = 64


def split(x):
    high = x.astype(BF16)
    return high, (x - high.astype(F32)).astype(BF16)


def left_parts(x):
    high, low = split(x)
    return jnp.concatenate([high, low, high], axis=1)


def right_parts(x):
    high, low = split(x)
    return jnp.concatenate([high, high, low], axis=0)


def matmul(a, b):
    return lax.dot_general(a, b, (((1,), (0,)), ((), ())), preferred_element_type=F32)


def dot_full(a, b, dims):
    return lax.dot_general(a, b, (dims, ((), ())), precision=HIGHEST, preferred_element_type=F32)


def padded(x, rows, columns):
    if columns > x.shape[1]:
        x = jnp.concatenate([x, jnp.zeros((x.shape[0], columns - x.shape[1]), x.dtype)], axis=1)
    if rows > x.shape[0]:
        x = jnp.concatenate([x, jnp.zeros((rows - x.shape[0], x.shape[1]), x.dtype)], axis=0)
    return x


def up_to(n, step):
    return (n + step - 1) // step * step


def hvp_shapes(atoms, width, types, levels, m1, m2, fit, ext):
    fit_wide, m1_wide = up_to(fit, 128), up_to(m1, 128)
    low = levels * m2
    return dict(
        idt=((width, atoms), jnp.int32),
        onehot=((width // CHUNK, DIGIT, CHUNK * atoms), BF16),
        in_bank=((width, ext // DIGIT, atoms), F32),
        w1_rows=((fit_wide // 128, m1_wide * m2, 128), F32),
        w1_low=((fit_wide // 128, types * low, 128), F32),
        low_right=((types * fit, 3 * low), BF16),
        low_left=((types * low, 3 * fit_wide), BF16),
        w2_right=((fit, 3 * fit_wide), BF16),
        w2_left=((fit, 3 * fit_wide), BF16),
        columns=((fit, 8), F32),
        lead_up=((types * m2, 3 * levels), BF16),
        lead_down=((types * levels, 3 * m2), BF16),
        dv=((6, width + CHUNK, atoms), F32),
        radial=((5, width + CHUNK, atoms), F32),
        mix=((9, width + CHUNK, atoms), F32),
        gauss=((levels, 3, width + CHUNK, atoms), F32),
        pooled=((8, levels, atoms), F32),
        product=((low, 2 * atoms), F32),
        pulled=((low, 2 * atoms), F32),
        gp=((levels, 8 * atoms), F32),
        forces=((6, width + CHUNK, atoms), F32),
    )


def prepare_matrices(h, table_ref, w1_ref, w2_ref, b1_ref, b2_ref, fo_ref):
    types, levels, m1 = table_ref.shape
    fit, m2 = w1_ref.shape[0], w1_ref.shape[1] // m1
    halves, rows, _ = h.w1_rows.shape
    m1_wide, low = rows // m2, levels * m2
    turned = padded(w1_ref[...], halves * 128, 0).T
    tables = jnp.concatenate([padded(table_ref[t], 0, m1_wide) for t in range(types)], axis=0)
    tables = left_parts(tables)
    for half in range(halves):
        h.w1_rows[half, : m1 * m2, :] = turned[:, half * 128 : (half + 1) * 128]
        h.w1_rows[half, m1 * m2 :, :] = jnp.zeros((rows - m1 * m2, 128), F32)
    for n in range(m2):
        part = [h.w1_rows[half, pl.ds(n, m1_wide, stride=m2), :] for half in range(halves)]
        out = matmul(tables, right_parts(jnp.concatenate(part, axis=1)))
        for half in range(halves):
            h.w1_low[half, pl.ds(n, types * levels, stride=m2), :] = out[:, half * 128 : (half + 1) * 128]
    for t in range(types):
        at = slice(t * low, (t + 1) * low)
        mine = jnp.concatenate([h.w1_low[half, at, :] for half in range(halves)], axis=1)
        h.low_left[at, :] = left_parts(mine)
        h.low_right[t * fit : (t + 1) * fit, :] = left_parts(mine.T[:fit])
    w2 = padded(w2_ref[...], halves * 128, halves * 128)
    h.w2_left[...] = left_parts(w2[:fit])
    h.w2_right[...] = left_parts(w2.T[:fit])
    lines = jnp.concatenate([b1_ref[...], b2_ref[...], fo_ref[...], jnp.zeros((5, fit), F32)], axis=0)
    h.columns[...] = dot_full(lines, identity(8), ((0,), (0,)))
    for t in range(types):
        first = table_ref[t][:, :m2]
        h.lead_down[t * levels : (t + 1) * levels, :] = left_parts(first)
        h.lead_up[t * m2 : (t + 1) * m2, :] = left_parts(dot_full(first, identity(levels), ((0,), (0,))))


def identity(n):
    same = lax.broadcasted_iota(jnp.int32, (n, n), 0) == lax.broadcasted_iota(jnp.int32, (n, n), 1)
    return jnp.where(same, 1.0, 0.0).astype(F32)


def prepare_scatter(h, ids_ref):
    width, atoms = h.idt.shape
    h.idt[...] = ids_ref[...].T
    group = lax.broadcasted_iota(jnp.int32, h.in_bank.shape[1:], 0)
    column = lax.broadcasted_iota(jnp.int32, (DIGIT, atoms), 0)

    def one(c, carry):
        idx = h.idt[pl.ds(pl.multiple_of(c * CHUNK, CHUNK), CHUNK), :]
        digit = jnp.bitwise_and(idx, DIGIT - 1)
        bank = jnp.right_shift(idx, DIGIT.bit_length() - 1)
        for r in range(CHUNK):
            h.in_bank[c * CHUNK + r] = jnp.where(bank[r : r + 1, :] == group, 1.0, 0.0).astype(F32)
            hit = jnp.where(digit[r : r + 1, :] == column, 1.0, 0.0)
            h.onehot[c, :, r * atoms : (r + 1) * atoms] = hit.astype(BF16)
        return carry

    lax.fori_loop(0, width // CHUNK, one, 0)


def pair_terms(h, ext_ref, counts):
    width, atoms = h.idt.shape
    levels = h.gauss.shape[0]
    banks = ext_ref.shape[1] // 128
    top = float(levels - 1)

    def one(c, carry):
        first = pl.multiple_of(c * CHUNK, CHUNK)
        here = pl.ds(first, CHUNK)
        idx = h.idt[here, :]
        lane = jnp.bitwise_and(idx, 127)
        bank = jnp.right_shift(idx, 7)
        fields = []
        for f in range(6):
            got = None
            for b in range(banks):
                row = jnp.broadcast_to(ext_ref[f : f + 1, b * 128 : (b + 1) * 128], (CHUNK, 128))
                part = jnp.take_along_axis(row, lane, axis=1, mode="promise_in_bounds")
                got = part if got is None else jnp.where(bank == b, part, got)
            got = got - ext_ref[f : f + 1, :atoms]
            h.dv[f, here, :] = got
            fields.append(got)
        d, v = fields[:3], fields[3:]
        slot = lax.broadcasted_iota(jnp.int32, (CHUNK, atoms), 0) + first
        q = d[0] * d[0] + d[1] * d[1] + d[2] * d[2]
        qd = 2.0 * (d[0] * v[0] + d[1] * v[1] + d[2] * v[2])
        w = 1.0 / (q + 0.01)
        decay = jnp.where(slot < counts, jnp.exp(-q), 0.0)
        s = decay * jnp.sqrt(w)
        u = decay * w
        s_q = -s * (1.0 + 0.5 * w)
        u_q = -u * (1.0 + w)
        shrink = 1.0 / (1.0 + s)
        for at, value in enumerate((qd, w, s, u, shrink)):
            h.radial[at, here, :] = value
        step = s_q * qd
        for at, value in enumerate(
            [-2.0 * top * shrink * shrink * step]
            + [s] + [u * e for e in d]
            + [step] + [u_q * qd * d[e] + u * v[e] for e in range(3)]
        ):
            h.mix[at, here, :] = value
        scaled = s * shrink * top
        for k in range(levels):
            y = scaled - float(k)
            phi = jnp.exp(-(y * y))
            psi = y * phi
            h.gauss[k, 0, here, :] = phi
            h.gauss[k, 1, here, :] = psi
            h.gauss[k, 2, here, :] = y * psi
        return carry

    lax.fori_loop(0, width // CHUNK, one, 0, unroll=8)


def pooled_terms(h):
    width, atoms = h.idt.shape
    levels = h.gauss.shape[0]
    together = 2
    zero = jnp.zeros((CHUNK, atoms), F32)
    for k0 in range(0, levels, together):

        def one(c, acc):
            here = slice(c * CHUNK, (c + 1) * CHUNK)
            slope = h.mix[0, here, :]
            r = [h.mix[1 + a, here, :] for a in range(4)]
            dr = [h.mix[5 + a, here, :] for a in range(4)]
            out = []
            for k in range(together):
                phi = h.gauss[k0 + k, 0, here, :]
                psi = h.gauss[k0 + k, 1, here, :] * slope
                out += [acc[8 * k + a] + phi * r[a] for a in range(4)]
                out += [acc[8 * k + 4 + a] + (phi * dr[a] + psi * r[a]) for a in range(4)]
            return tuple(out)

        acc = (zero,) * (8 * together)
        for c in range(width // CHUNK):
            acc = one(c, acc)
        for k in range(together):
            for a in range(8):
                h.pooled[a, k0 + k : k0 + k + 1, :] = jnp.sum(acc[8 * k + a], axis=0, keepdims=True) / width


def of_kind(kinds, rows):
    types = len(kinds)
    step = rows.shape[0] // types
    out = rows[:step]
    for t in range(1, types):
        out = jnp.where(kinds[t], rows[t * step : (t + 1) * step], out)
    return out


def lanes_of(x, count, atoms):
    return [x[:, a * atoms : (a + 1) * atoms] for a in range(count)]


def fitting_net(h, kinds_ref, types):
    fit = h.columns.shape[0]
    fit_wide = h.w2_left.shape[1] // 3
    levels = h.pooled.shape[1]
    m2 = h.lead_up.shape[0] // types
    width, atoms = h.idt.shape
    kinds2 = jnp.concatenate([kinds_ref[...]] * 2, axis=1)
    kinds8 = jnp.concatenate([kinds2] * 4, axis=1)
    kinds2 = [kinds2 == t for t in range(types)]
    kinds8 = [kinds8 == t for t in range(types)]
    pooled = jnp.concatenate([h.pooled[a] for a in range(8)], axis=1)
    lead = lanes_of(of_kind(kinds8, matmul(h.lead_up[...], right_parts(pooled))), 8, atoms)
    for k in range(levels):
        rows = [h.pooled[a, k : k + 1, :] for a in range(8)]
        plain = rows[0] * lead[0]
        moved = rows[4] * lead[0] + rows[0] * lead[4]
        for a in range(1, 4):
            plain += rows[a] * lead[a]
            moved += rows[4 + a] * lead[a] + rows[a] * lead[4 + a]
        h.product[k * m2 : (k + 1) * m2, :atoms] = plain
        h.product[k * m2 : (k + 1) * m2, atoms:] = moved
    z1 = of_kind(kinds2, matmul(h.low_right[...], right_parts(h.product[...])))
    b1, b2, fo = h.columns[:, 0:1], h.columns[:, 1:2], h.columns[:, 2:3]
    h1 = jnp.tanh(z1[:, :atoms] + b1)
    gate1 = 1.0 - h1 * h1
    dh1 = gate1 * z1[:, atoms:]
    z2 = matmul(h.w2_right[...], right_parts(padded(jnp.concatenate([h1, dh1], axis=1), fit_wide, 0)))
    t2 = jnp.tanh(z2[:, :atoms] + b2)
    gate2 = 1.0 - t2 * t2
    dt2 = gate2 * z2[:, atoms:]
    gz2 = jnp.concatenate([fo * gate2, fo * (-2.0 * t2 * dt2)], axis=1)
    gh = matmul(h.w2_left[...], right_parts(padded(gz2, fit_wide, 0)))
    gh1 = gh[:, :atoms] + fo
    gz1 = jnp.concatenate([gh1 * gate1, gh[:, atoms:] * gate1 - 2.0 * gh1 * h1 * dh1], axis=1)
    h.pulled[...] = of_kind(kinds2, matmul(h.low_left[...], right_parts(padded(gz1, fit_wide, 0))))
    acc = [jnp.zeros((m2, atoms), F32) for _ in range(8)]
    for k in range(levels):
        g = h.pulled[k * m2 : (k + 1) * m2, :atoms]
        dg = h.pulled[k * m2 : (k + 1) * m2, atoms:]
        rows = [h.pooled[a, k : k + 1, :] for a in range(8)]
        for a in range(4):
            straight = jnp.sum(g * lead[a], axis=0, keepdims=True)
            turned = jnp.sum(dg * lead[a] + g * lead[4 + a], axis=0, keepdims=True)
            h.gp[k : k + 1, a * atoms : (a + 1) * atoms] = straight
            h.gp[k : k + 1, (4 + a) * atoms : (5 + a) * atoms] = turned
            acc[a] = acc[a] + g * rows[a]
            acc[4 + a] = acc[4 + a] + (dg * rows[a] + g * rows[4 + a])
    across = of_kind(kinds8, matmul(h.lead_down[...], right_parts(jnp.concatenate(acc, axis=1))))
    h.gp[...] = (h.gp[...] + across) / width


def pair_forces(h, out_ref):
    width, atoms = h.idt.shape
    levels = h.gauss.shape[0]
    banks = h.in_bank.shape[1]
    top = float(levels - 1)

    def force_of(c, centre):
        first = pl.multiple_of(c * CHUNK, CHUNK)
        here = pl.ds(first, CHUNK)
        zero = jnp.zeros((CHUNK, atoms), F32)
        s0, s1, s2, e0, e1 = ([zero] * 4 for _ in range(5))
        for k in range(levels):
            phi, psi, chi = (h.gauss[k, p, here, :] for p in range(3))
            for a in range(4):
                g = h.gp[k : k + 1, a * atoms : (a + 1) * atoms]
                gd = h.gp[k : k + 1, (4 + a) * atoms : (5 + a) * atoms]
                s0[a] = s0[a] + g * phi
                s1[a] = s1[a] + g * psi
                s2[a] = s2[a] + g * chi
                e0[a] = e0[a] + gd * phi
                e1[a] = e1[a] + gd * psi
        d = [h.dv[f, here, :] for f in range(3)]
        v = [h.dv[f, here, :] for f in range(3, 6)]
        qd, w, s, u, shrink = (h.radial[at, here, :] for at in range(5))
        s_q = -s * (1.0 + 0.5 * w)
        u_q = -u * (1.0 + w)
        t_s = shrink * shrink
        t_q = t_s * s_q
        s_qq = -s_q * (1.0 + 0.5 * w) + 0.5 * s * w * w
        u_qq = -u_q * (1.0 + w) + u * w * w
        t_qq = -2.0 * t_s * shrink * s_q * s_q + t_s * s_qq
        step = t_q * qd
        val = s0
        val_t = [-2.0 * top * e for e in s1]
        val_tt = [top * top * (4.0 * s2[a] - 2.0 * s0[a]) for a in range(4)]
        dval = [e0[a] + val_t[a] * step for a in range(4)]
        dval_t = [-2.0 * top * e1[a] + val_tt[a] * step for a in range(4)]
        big = val[1] * d[0] + val[2] * d[1] + val[3] * d[2]
        big_t = val_t[1] * d[0] + val_t[2] * d[1] + val_t[3] * d[2]
        dbig = sum(dval[1 + e] * d[e] + val[1 + e] * v[e] for e in range(3))
        dbig_t = sum(dval_t[1 + e] * d[e] + val_t[1 + e] * v[e] for e in range(3))
        flow = val_t[0] * s + big_t * u
        kern = t_q * flow + val[0] * s_q + big * u_q
        dkern = (
            t_q * (dval_t[0] * s + dbig_t * u)
            + dval[0] * s_q
            + dbig * u_q
            + qd * (t_qq * flow + t_q * (val_t[0] * s_q + big_t * u_q) + val[0] * s_qq + big * u_qq)
        )
        du = u_q * qd
        kern, dkern = 2.0 * kern, 2.0 * dkern
        out = []
        for e in range(3):
            force = v[e] * kern + d[e] * dkern + du * val[1 + e] + u * dval[1 + e]
            high = force.astype(BF16).astype(F32)
            h.forces[e, here, :] = high
            h.forces[3 + e, here, :] = force - high
            out.append(centre[e] - force)
        return tuple(out)

    zero = jnp.zeros((CHUNK, atoms), F32)
    def scatter(first, chunks):
        lefts = []
        for n in range(first * CHUNK, (first + chunks) * CHUNK):
            mine = h.in_bank[n]
            lefts.append(jnp.concatenate([h.forces[e, n : n + 1, :] * mine for e in range(6)], axis=0).astype(BF16))
        right = jnp.concatenate([h.onehot[first + j] for j in range(chunks)], axis=1)
        return lax.dot_general(
            jnp.concatenate(lefts, axis=1), right, (((1,), (1,)), ((), ())), preferred_element_type=F32
        )

    chunks = width // CHUNK
    centre = (zero,) * 3
    acc = None
    for piece in range(4):
        if piece:
            part = scatter((piece - 1) * chunks // 4, chunks // 4)
            acc = part if acc is None else acc + part
        for c in range(piece * chunks // 4, (piece + 1) * chunks // 4):
            centre = force_of(c, centre)
    acc = acc + scatter(3 * chunks // 4, chunks // 4)
    per = 128 // DIGIT
    out_ref[3:, :] = jnp.zeros((out_ref.shape[0] - 3, out_ref.shape[1]), F32)
    for e in range(3):
        part = acc[banks * e : banks * (e + 1)] + acc[banks * (3 + e) : banks * (4 + e)]
        for b in range(0, banks, per):
            row = jnp.concatenate([part[j : j + 1] for j in range(b, b + per)], axis=1)
            if b == 0:
                row = row + jnp.sum(centre[e], axis=0, keepdims=True)
            out_ref[e : e + 1, b * DIGIT : (b + per) * DIGIT] = row


class Scratch:
    def __init__(self, names, refs):
        for name, ref in zip(names, refs, strict=True):
            setattr(self, name, ref)


AXES = ("gx", "gy", "gz")
MESH = pl.DeviceIdType.MESH
GROUP_LIMIT = 32


def sizes_of():
    return [lax.axis_size(axis) for axis in AXES]


def plane_offsets():
    def along(size):
        return (0, 1) if size == 2 else (0, 1, -1)

    _, ny, nz = sizes_of()
    return [(dy, dz) for dz in along(nz) for dy in along(ny)]


class Grid:
    def __init__(self):
        self.sizes = sizes_of()
        self.along = []
        for axis, peers in zip(AXES, self.sizes):
            me = lax.axis_index(axis)
            self.along.append([me] + [lax.rem(me + step, peers) for step in range(1, peers)])

    def device(self, shift):
        return {
            axis: row[step % peers] for axis, row, step, peers in zip(AXES, self.along, shift, self.sizes)
        }


def reduction_groups():
    sizes = sizes_of()
    groups = []
    for at in range(3):
        if groups and groups[-1][1] * sizes[at] <= GROUP_LIMIT:
            groups[-1] = (groups[-1][0] + [at], groups[-1][1] * sizes[at])
        else:
            groups.append(([at], sizes[at]))
    out = []
    for members, count in groups:
        shifts = [[0, 0, 0]]
        for at in members:
            shifts = [s[:at] + [step] + s[at + 1 :] for s in shifts for step in range(sizes[at])]
        out.append((members, count, [tuple(s) for s in shifts if any(s)]))
    return out


def place_in(members):
    sizes = sizes_of()
    me = 0
    for at in members:
        me = me * sizes[at] + lax.axis_index(AXES[at])
    return me


def three_parts(x):
    high = x.astype(BF16)
    rest = x - high.astype(F32)
    middle = rest.astype(BF16)
    low = (rest - middle.astype(F32)).astype(BF16)
    return jnp.concatenate([high.astype(F32), middle.astype(F32), low.astype(F32)], axis=0).astype(BF16)


def select_dot(x, onehot, dims):
    n = x.shape[0]
    out = lax.dot_general(three_parts(x), onehot, (dims, ((), ())), preferred_element_type=F32)
    return (out[:n] + out[n : 2 * n]) + out[2 * n :]


def chosen_columns(map_row, columns):
    rows = lax.broadcasted_iota(jnp.int32, (columns, map_row.shape[1]), 0).astype(F32)
    return jnp.where(rows == map_row, 1.0, 0.0).astype(BF16)


def sides(parts, early):
    if -1 in parts:
        return jnp.where(early, parts[-1], parts[1])
    return parts[1]


def one_side(x, step, distinct, early):
    if not distinct:
        return x
    return jnp.where(early, x, 0.0) if step == -1 else jnp.where(early, 0.0, x)


class Round:
    def __init__(self, grid, sems, at, landed):
        self.grid, self.sems, self.at, self.landed = grid, sems, at, landed

    def copy(self, source, target, shift):
        return pltpu.make_async_remote_copy(
            src_ref=source,
            dst_ref=target,
            send_sem=self.sems.at[self.at, 0],
            recv_sem=self.sems.at[self.at, 1],
            device_id=self.grid.device(shift),
            device_id_type=MESH,
        )

    def send(self, source, target, shift):
        self.shift = shift
        self.copy(source, target, shift).start()

    def all_of_them(self):
        return self.copy(self.landed, self.landed, self.shift)


def lanczos_kernel(*refs, inputs, names):
    hbm, (next_ref, corr_ref, norm_ref) = refs[:inputs], refs[inputs : inputs + 3]
    local = refs[inputs + 3 : 2 * inputs + 3]
    (load_sem, round_sem, ext, work, mine, face, landed, back_raw, back_face, returned, stack, mixed_right, gram_land, row_land, *hvp_scratch) = refs[2 * inputs + 3 :]
    places, basis, ids, counts, kinds, map_x, map_y, map_z, table, w1, w2, b1, b2, fo = local
    h = Scratch(names, hvp_scratch)
    types = table.shape[0]
    atoms = places.shape[2]
    stored = basis.shape[0]
    rows = stack.shape[0]
    pair = 2 * map_x.shape[1]
    grid = Grid()
    sizes = grid.sizes
    entries = 3 * atoms * sizes[0] * sizes[1] * sizes[2]
    planes = plane_offsets()
    groups = reduction_groups()
    count = len(planes)

    partners = set()
    for dy, dz in planes:
        for dx in (-1, 0, 1):
            partners.add(tuple(step % peers for step, peers in zip((dx, dy, dz), sizes)))
    for _, _, shifts in groups:
        partners.update(shifts)
    partners = sorted(partners - {(0, 0, 0)}, key=lambda shift: (-sum(map(bool, shift[::2])), shift))
    opposite = {tuple(-step % peers for step, peers in zip(shift, sizes)) for shift in partners}
    assert opposite == set(partners)
    barrier = pltpu.get_barrier_semaphore()
    for shift in partners:
        pl.semaphore_signal(barrier, inc=1, device_id=grid.device(shift), device_id_type=MESH)
    loads = [pltpu.make_async_copy(a, b, load_sem.at[at]) for at, (a, b) in enumerate(zip(hbm, local))]
    for at in (0, 1, 5, 6, 7, 2, 3, 4, 8, 9, 10, 11, 12, 13):
        loads[at].start()
    early = lax.broadcasted_iota(jnp.int32, (8, pair), 1) < pair // 2
    line = lax.broadcasted_iota(jnp.int32, (8, pair), 0)
    for at in (0, 1, 5, 6, 7):
        loads[at].wait()
    for c in range(3):
        mine[c : c + 1, :] = places[c]
        mine[3 + c : 4 + c, :] = basis[stored - 1, c]
    map_rows = [jnp.concatenate([m[1:2, :], m[0:1, :]], axis=1).astype(F32) for m in (map_x, map_y, map_z)]
    mine[6:7, :] = map_rows[1]
    mine[7:8, :] = map_rows[2]
    pick_x = chosen_columns(map_rows[0], atoms)
    face[...] = select_dot(mine[...], pick_x, ((1,), (0,)))
    returned[...] = jnp.zeros_like(returned)
    pl.semaphore_wait(barrier, len(partners))

    halo = Round(grid, round_sem, 0, landed)
    for at, (dy, dz) in reversed(list(enumerate(planes))):
        halo.send(face, landed.at[at], (1, -dy, -dz))
        halo.send(face, landed.at[count + at], (-1, -dy, -dz))
        if at:
            halo.send(mine, landed.at[2 * count + at - 1], (0, -dy, -dz))

    stack[rows - 8 :, :] = jnp.zeros((8, 3 * atoms), F32)
    for k in range(stored):
        for c in range(3):
            stack[k : k + 1, c * atoms : (c + 1) * atoms] = basis[k, c]
    gram = dot_full(stack[...], stack[...], ((1,), (1,)))
    gram = jnp.concatenate([gram[r : r + 8] for r in range(0, rows, 8)], axis=1)
    for at in (2, 3, 4, 8, 9, 10, 11, 12, 13):
        loads[at].wait()
    prepare_scatter(h, ids)
    prepare_matrices(h, table, w1, w2, b1, b2, fo)
    halo.all_of_them().wait_recv()

    def shifted(x, row):
        return x + jnp.where(line == row, jnp.where(early, -1.0, 1.0), 0.0)

    raw = {plane: mine[...] if at == 0 else landed[2 * count + at - 1] for at, plane in enumerate(planes)}
    wide = {
        plane: jnp.concatenate([raw[plane], shifted(jnp.where(early, landed[at], landed[count + at]), 0)], axis=1)
        for at, plane in enumerate(planes)
    }
    pick_y, pick_z, wider = {}, {}, {}
    for dz in sorted({dz for _, dz in planes}):
        got = {}
        for dy in (1, -1):
            if (dy, dz) in raw:
                pick_y[dy, dz] = chosen_columns(raw[dy, dz][6:7, :], atoms + pair)
                got[dy] = select_dot(wide[dy, dz], pick_y[dy, dz], ((1,), (0,)))
        wider[dz] = jnp.concatenate([wide[0, dz], shifted(sides(got, early), 1)], axis=1)
    got = {}
    for dz in (1, -1):
        if dz in wider:
            pick_z[dz] = chosen_columns(raw[0, dz][7:8, :], atoms + 2 * pair)
            got[dz] = select_dot(wider[dz], pick_z[dz], ((1,), (0,)))
    ext[:, : atoms + 2 * pair] = wider[0]
    ext[:, atoms + 2 * pair :] = shifted(sides(got, early), 2)

    def gather_from(group, kind, tiles, base, value):
        members, size, shifts = groups[group]
        me = base + place_in(members)
        tiles[me] = value
        around = Round(grid, round_sem, 2 + 2 * group + kind, tiles.at[pl.ds(base, size - 1)])
        for shift in shifts:
            around.send(tiles.at[me], tiles.at[me], shift)
        return around

    def added(tiles, base, size):
        terms = [tiles[base + at] for at in range(size)]
        while len(terms) > 1:
            terms = [sum(terms[at : at + 2][1:], terms[at]) for at in range(0, len(terms), 2)]
        return terms[0]

    pair_terms(h, ext, counts[...])
    rounds = [halo, gather_from(0, 0, gram_land, 0, gram)]
    pooled_terms(h)
    fitting_net(h, kinds, types)
    pair_forces(h, work)

    many_y, many_z = -1 in {dy for dy, _ in planes}, -1 in wider
    back = {0: work[:, : atoms + 2 * pair]}
    for dz in pick_z:
        part = one_side(work[:, atoms + 2 * pair :], dz, many_z, early)
        back[dz] = select_dot(part, pick_z[dz], ((1,), (1,)))
    terms = {(0, dz): x[:, : atoms + pair] for dz, x in back.items()}
    for dy, dz in pick_y:
        part = one_side(back[dz][:, atoms + pair :], dy, many_y, early)
        terms[dy, dz] = select_dot(part, pick_y[dy, dz], ((1,), (1,)))
    lead = pl.ds(0, 3)
    back_round = Round(grid, round_sem, 1, returned.at[:, lead])
    for at, (dy, dz) in reversed(list(enumerate(planes))):
        back_raw[at] = terms[dy, dz][:, :atoms]
        back_face[at] = terms[dy, dz][:, atoms:]
        back_round.send(back_face.at[at, lead], returned.at[at, lead], (-1, dy, dz))
        back_round.send(back_face.at[at, lead], returned.at[count + at, lead], (1, dy, dz))
        if at:
            back_round.send(back_raw.at[at, lead], returned.at[2 * count + at - 1, lead], (0, dy, dz))

    rounds[-1].all_of_them().wait_recv()
    total = added(gram_land, 0, groups[0][1])
    base = groups[0][1]
    for group in range(1, len(groups)):
        rounds.append(gather_from(group, 0, gram_land, base, total))
        rounds[-1].all_of_them().wait_recv()
        total = added(gram_land, base, groups[group][1])
        base += groups[group][1]
    rounds.append(back_round)
    gram = jnp.concatenate([total[:, r : r + rows] for r in range(0, rows * rows // 8, rows)], axis=0) / entries

    high, low = split(stack[...])
    stack_right = jnp.concatenate([high, high, low], axis=1)
    mixed_right[...] = right_parts(jnp.concatenate([padded(gram, 0, 128), stack[...]], axis=1))
    back_round.all_of_them().wait_recv()
    own, up, low = back_raw[0], returned[0], returned[count]
    for at in range(1, count):
        own = own + returned[2 * count + at - 1]
        up = up + returned[at]
        low = low + returned[count + at]
    own = own + select_dot(jnp.where(early, up, low), pick_x, ((1,), (1,)))
    hv = jnp.concatenate([own[c : c + 1, :] for c in range(3)], axis=1)
    sums = lax.dot_general(
        left_parts(jnp.broadcast_to(hv, (8, 3 * atoms))), stack_right, (((1,), (1,)), ((), ())), preferred_element_type=F32
    )
    lane = lax.broadcasted_iota(jnp.int32, (1, row_land.shape[2]), 1)
    sums = jnp.concatenate([sums[0:1], jnp.zeros((1, row_land.shape[2] - rows), F32)], axis=1)
    sums = jnp.where(lane == stored, jnp.sum(hv * hv, axis=1, keepdims=True), sums)
    base = 0
    for group in range(len(groups)):
        rounds.append(gather_from(group, 1, row_land, base, sums))
        rounds[-1].all_of_them().wait_recv()
        sums = added(row_land, base, groups[group][1])
        base += groups[group][1]
    for around in rounds:
        around.all_of_them().wait_send()
    sums = sums[:, :rows] / entries
    kept = jnp.where(lane[:, :rows] < stored, sums, 0.0)
    mixed = matmul(left_parts(jnp.broadcast_to(kept, (8, rows))), mixed_right[...])[0:1]
    plain = sums[:, stored : stored + 1]
    cross = jnp.sum(mixed[:, :rows] * kept - 2.0 * kept * kept, axis=1, keepdims=True)
    norm = jnp.sqrt(plain + cross + 1e-06)
    norm_ref[...] = norm
    corr_ref[...] = sums[:, :stored]
    for c in range(3):
        part = slice(c * atoms, (c + 1) * atoms)
        next_ref[c] = (hv[:, part] - mixed[:, 128:][:, part]) / norm


def hand_over(*refs):
    count = (len(refs) - 1) // 2
    sems = refs[-1]
    copies = [pltpu.make_async_copy(refs[at], refs[count + at], sems.at[at]) for at in range(count)]
    for copy in copies:
        copy.start()
    for copy in copies:
        copy.wait()


def on_device(positions, basis, neighbours, used_count, kinds, map_x, map_y, map_z,
              table, fit_w1, fit_b1, fit_w2, fit_b2, fit_out):
    atoms = positions.shape[-1]
    width = neighbours.shape[-1]
    stored = basis.shape[0]
    types, levels, m1 = table.shape
    m2 = fit_w1.shape[0] // m1
    pair = 2 * map_x.shape[-1]
    ext = atoms + 3 * pair
    args = [
        positions.reshape(3, 1, atoms),
        basis.reshape(stored, 3, 1, atoms),
        neighbours.reshape(atoms, width),
        used_count.reshape(1, atoms),
        kinds.reshape(1, atoms),
        map_x.reshape(2, -1),
        map_y.reshape(2, -1),
        map_z.reshape(2, -1),
        table,
        fit_w1.T,
        fit_w2,
        fit_b1[None],
        fit_b2[None],
        fit_out[None],
    ]
    rows = (stored + 8) // 8 * 8
    planes = len(plane_offsets())
    groups = reduction_groups()
    slots = sum(count for _, count, _ in groups)
    hvp = hvp_shapes(atoms, width, types, levels, m1, m2, fit_w2.shape[0], ext)
    any_space = pl.BlockSpec(memory_space=pl.ANY)
    vmem = pl.BlockSpec(memory_space=pltpu.VMEM)
    tiles = pltpu.VMEM((planes, 8, pair), F32)
    arrivals = pltpu.VMEM((3 * planes - 1, 8, pair), F32)
    results = pl.pallas_call(
        functools.partial(lanczos_kernel, inputs=len(args), names=tuple(hvp)),
        out_shape=(
            jax.ShapeDtypeStruct((3, 1, atoms), F32),
            jax.ShapeDtypeStruct((1, stored), F32),
            jax.ShapeDtypeStruct((1, 1), F32),
        ),
        in_specs=[any_space] * len(args),
        out_specs=(vmem,) * 3,
        scratch_shapes=[pltpu.VMEM(x.shape, x.dtype) for x in args] + [
            pltpu.SemaphoreType.DMA((len(args),)),
            pltpu.SemaphoreType.DMA((2 + 2 * len(groups), 2)),
            pltpu.VMEM((8, ext), F32),
            pltpu.VMEM((8, ext), F32),
            pltpu.VMEM((8, pair), F32),
            pltpu.VMEM((8, pair), F32),
            arrivals,
            tiles,
            tiles,
            arrivals,
            pltpu.VMEM((rows, 3 * atoms), F32),
            pltpu.VMEM((3 * rows, 128 + 3 * atoms), BF16),
            pltpu.VMEM((slots, 8, rows * rows // 8), F32),
            pltpu.VMEM((slots, 1, 128), F32),
        ] + [pltpu.VMEM(shape, dtype) for shape, dtype in hvp.values()],
        compiler_params=pltpu.CompilerParams(
            collective_id=0, has_side_effects=True, vmem_limit_bytes=60 << 20
        ),
        name="lanczos",
    )(*args)
    results = pl.pallas_call(
        hand_over,
        out_shape=tuple(jax.ShapeDtypeStruct(x.shape, x.dtype) for x in results),
        in_specs=[any_space] * 3,
        out_specs=(any_space,) * 3,
        scratch_shapes=[pltpu.SemaphoreType.DMA((3,))],
        name="hand_over",
    )(*results)
    next_vector, correlations, norm = results
    return next_vector.reshape(positions.shape), correlations.reshape(stored), norm.reshape(())


def solution(mesh):
    placed = (
        P(None, "gx", "gy", "gz", None),
        P(None, None, "gx", "gy", "gz", None),
        P("gx", "gy", "gz", None, None),
        P("gx", "gy", "gz", None),
        P("gx", "gy", "gz", None),
        P("gx", "gy", "gz", None, None),
        P("gx", "gy", "gz", None, None),
        P("gx", "gy", "gz", None, None),
        P(),
        P(),
        P(),
        P(),
        P(),
        P(),
    )
    return jax.shard_map(
        on_device,
        mesh=mesh,
        in_specs=placed,
        out_specs=(P(None, "gx", "gy", "gz", None), P(), P()),
        check_vma=False,
    )
```
